128 devices in a mesh: tm: 32 (over x, y, core), batch: 4 (over z).
Axes of the slice: x: 4, y: 4, z: 4, core: 2. Of those that a mesh axis runs over, the one named last changes fastest.
Arguments:
- hidden_states: bfloat16 [4, 4096, 5120], P('batch', 'tm'), may hold values from -6 to 6
- gen_weight: bfloat16 [64, 5120], replicated, may hold values from -0.078125 to 0.078125
- noise_field: bfloat16 [4, 64, 4096], P('batch', None, 'tm'), may hold values from -6 to 6
- timesteps: int32 [4], P('batch'), may hold values from 200 to 999
- embed_real: bfloat16 [128, 5120], replicated, may hold values from -0.5 to 0.5
- time_real: bfloat16 [256, 3, 5120], P('tm'), may hold values from -0.375 to 0.375
- query_real: bfloat16 [5120, 4096], P(None, 'tm'), may hold values from -3 to 3
- key_real: bfloat16 [5120, 4096], P(None, 'tm'), may hold values from -3 to 3
- value_real: bfloat16 [5120, 4096], P(None, 'tm'), may hold values from -0.078125 to 0.078125
- out_real: bfloat16 [4096, 5120], P('tm'), may hold values from -0.09375 to 0.09375
- gain_real: float32 [2, 4096], P(None, 'tm'), may hold values from 0.25 to 3
- proj_real: bfloat16 [64, 5120], replicated, may hold values from -0.078125 to 0.078125
- embed_fake: bfloat16 [128, 5120], replicated, may hold values from -0.5 to 0.5
- time_fake: bfloat16 [256, 3, 5120], P('tm'), may hold values from -0.375 to 0.375
- query_fake: bfloat16 [5120, 4096], P(None, 'tm'), may hold values from -3 to 3
- key_fake: bfloat16 [5120, 4096], P(None, 'tm'), may hold values from -3 to 3
- value_fake: bfloat16 [5120, 4096], P(None, 'tm'), may hold values from -0.078125 to 0.078125
- out_fake: bfloat16 [4096, 5120], P('tm'), may hold values from -0.09375 to 0.09375
- gain_fake: float32 [2, 4096], P(None, 'tm'), may hold values from 0.25 to 3
- proj_fake: bfloat16 [64, 5120], replicated, may hold values from -0.078125 to 0.078125
Outputs:
- dmd_gradient: float32 [4, 64, 4096], P('batch', None, 'tm')
- weight_grad: float32 [64, 5120], replicated
The draws below stay inside these ranges and needn't reach their ends.
All inputs are finite; a program needn't handle non-finite values.
Results may differ from the reference program's by a relative error of at most 0.019.
Values may be sent and summed in bfloat16 or wider, within the bound.
A program may use at most 128 MiB of HBM per device.

```python
import math
import jax
import jax.numpy as jnp
from jax import lax

D = 5120
HD = 128
FREQ = 256
FTOK = 128
HEADS = 32
PATCH = 64
KIN = 128
TOKENS = 4096
SAMPLES = 4


def spiked_pair(key, salt_value):
    base_key = jax.random.fold_in(key, salt_value)
    key_one, key_two, key_three, key_four = jax.random.split(base_key, 4)
    proj_width = HEADS * HD
    query_draw = jax.random.normal(key_one, (D, proj_width), jnp.float32) / math.sqrt(D)
    key_draw = jax.random.normal(key_four, (D, proj_width), jnp.float32) / math.sqrt(D)
    return (jnp.clip(query_draw, -3.0, 3.0), jnp.clip(key_draw, -3.0, 3.0))


def draw_query_real(key, part):
    return spiked_pair(key, 11)[0].astype(jnp.bfloat16)


def draw_key_real(key, part):
    return spiked_pair(key, 11)[1].astype(jnp.bfloat16)


def draw_query_fake(key, part):
    return spiked_pair(key, 23)[0].astype(jnp.bfloat16)


def draw_key_fake(key, part):
    return spiked_pair(key, 23)[1].astype(jnp.bfloat16)


def touch_ends(drawn, key, smallest, largest):
    longest = drawn.shape.index(max(drawn.shape))
    spots = []
    for shift in (0, 1):
        where = [jax.random.randint(jax.random.fold_in(key, axis), (), 0, length) for axis, length in enumerate(drawn.shape)]
        where[longest] = (where[longest] + shift) % drawn.shape[longest]
        spots.append(tuple(where))
    return drawn.at[spots[0]].set(smallest).at[spots[1]].set(largest)


def level_of(key, extent, shards, low, top_value):
    def one(position, parts):
        steps = jax.random.uniform(jax.random.fold_in(jax.random.fold_in(key, 6), position), (parts,), jnp.float32, low / len(shards), top_value / len(shards))
        return jnp.repeat(jnp.exp(steps), extent[position] // parts).reshape((-1,) + (1,) * (len(extent) - position - 1))

    factor_of = one(*shards[0])
    for cut in shards[1:]:
        factor_of = factor_of * one(*cut)
    return factor_of


def scatter_about(rng, dims, deviation, most, cuts=(), kind=jnp.bfloat16):
    factor_of = level_of(rng, dims, cuts, -0.22, 0.18) if cuts else 1.0
    values = jax.random.normal(rng, dims, jnp.float32) * deviation * factor_of
    return jnp.minimum(jnp.maximum(values, -most), most).astype(kind)


def setup_inputs(seed: int = 0) -> dict:
    seeds = jax.random.split(jax.random.key(seed), 21)
    hidden_states = scatter_about(seeds[0], (SAMPLES, TOKENS, D), 1.0, 6.0, ((0, 4), (1, 32)))
    gen_weight = scatter_about(seeds[1], (PATCH, D), D ** -0.5, 0.078125)
    noise_field = scatter_about(seeds[2], (SAMPLES, PATCH, TOKENS), 1.0, 6.0, ((0, 4), (2, 32)))
    timesteps = touch_ends(jax.random.randint(seeds[3], (SAMPLES,), 200, 1000), jax.random.fold_in(seeds[3], 1), 200, 999).astype(jnp.int32)
    embed_real = scatter_about(seeds[4], (KIN, D), KIN ** -0.5, 0.5)
    time_real = scatter_about(seeds[5], (FREQ, 3, D), FREQ ** -0.5, 0.375, ((0, 32),))
    query_real = draw_query_real(jax.random.fold_in(seeds[20], 71), 0)
    key_real = draw_key_real(jax.random.fold_in(seeds[20], 71), 0)
    value_real = scatter_about(seeds[8], (D, HEADS * HD), D ** -0.5, 0.078125, ((1, 32),))
    out_real = scatter_about(seeds[9], (HEADS * HD, D), (HEADS * HD) ** -0.5, 0.09375, ((0, 32),))
    gain_real = jnp.clip(jnp.exp(math.log(3.0) - 2.4849066 * jax.random.uniform(seeds[10], (2, HEADS * HD), jnp.float32) ** level_of(seeds[10], (2, HEADS * HD), ((1, 32),), -0.2, 0.2)), 0.25, 3.0)
    proj_real = scatter_about(seeds[11], (PATCH, D), D ** -0.5, 0.078125)
    embed_fake = scatter_about(seeds[12], (KIN, D), KIN ** -0.5, 0.5)
    time_fake = scatter_about(seeds[13], (FREQ, 3, D), FREQ ** -0.5, 0.375, ((0, 32),))
    query_fake = draw_query_fake(jax.random.fold_in(seeds[20], 71), 0)
    key_fake = draw_key_fake(jax.random.fold_in(seeds[20], 71), 0)
    value_fake = scatter_about(seeds[16], (D, HEADS * HD), D ** -0.5, 0.078125, ((1, 32),))
    out_fake = scatter_about(seeds[17], (HEADS * HD, D), (HEADS * HD) ** -0.5, 0.09375, ((0, 32),))
    gain_fake = jnp.clip(jnp.exp(math.log(3.0) - 2.4849066 * jax.random.uniform(seeds[18], (2, HEADS * HD), jnp.float32) ** level_of(seeds[18], (2, HEADS * HD), ((1, 32),), -0.2, 0.2)), 0.25, 3.0)
    proj_fake = scatter_about(seeds[19], (PATCH, D), D ** -0.5, 0.078125)
    return dict(hidden_states=hidden_states, gen_weight=gen_weight, noise_field=noise_field, timesteps=timesteps, embed_real=embed_real, time_real=time_real, query_real=query_real, key_real=key_real, value_real=value_real, out_real=out_real, gain_real=gain_real, proj_real=proj_real, embed_fake=embed_fake, time_fake=time_fake, query_fake=query_fake, key_fake=key_fake, value_fake=value_fake, out_fake=out_fake, gain_fake=gain_fake, proj_fake=proj_fake)


norm_floor = 0.05
gap_floor = 0.25
highest = lax.Precision.HIGHEST

def sinusoid(time_step):
    half_freq = FREQ // 2
    frequency = jnp.exp(-math.log(10000.0) * jnp.arange(half_freq, dtype=jnp.float32) / half_freq)
    angles = time_step.astype(jnp.float32) * frequency
    return jnp.concatenate([jnp.cos(angles), jnp.sin(angles)]).astype(jnp.bfloat16)

def rms_round(vector, gain_row):
    return (vector * lax.rsqrt(lax.optimization_barrier(jnp.mean(vector * vector, axis=1, keepdims=True)) + norm_floor) * gain_row[None, :]).astype(jnp.bfloat16)

def velocity(noisy_patch, sinus_wave, embed_table, time_table, query_proj, key_proj, value_proj, out_proj, norm_gains, final_proj):
    earlier = jnp.concatenate([jnp.zeros((PATCH, FTOK), jnp.bfloat16), noisy_patch[:, :TOKENS - FTOK]], axis=1)
    stacked = jnp.concatenate([noisy_patch, earlier], axis=0)
    embedded = lax.dot_general(stacked, embed_table, (((0,), (0,)), ((), ())), preferred_element_type=jnp.float32)
    row_mean = lax.optimization_barrier(jnp.mean(embedded, axis=1, keepdims=True))
    centered = embedded - row_mean
    rscale = lax.rsqrt(lax.optimization_barrier(jnp.mean(centered * centered, axis=1, keepdims=True)) + norm_floor)
    modulation = jnp.einsum('f,fcd->cd', sinus_wave.astype(jnp.float32), time_table.astype(jnp.float32))
    normed = centered * rscale * (1.0 + modulation[1])[None, :] + modulation[0][None, :]
    queries = jnp.dot(normed, query_proj.astype(jnp.float32), precision=highest)
    keys_all = jnp.dot(normed, key_proj.astype(jnp.float32), precision=highest)
    values_all = jnp.dot(normed, value_proj.astype(jnp.float32), precision=highest).astype(jnp.bfloat16)
    query_norm = rms_round(queries, norm_gains[0])
    key_norm = rms_round(keys_all, norm_gains[1])
    frames = jnp.arange(TOKENS, dtype=jnp.int32) // FTOK
    allowed = frames[None, :] <= frames[:, None]

    def one_head(head_index):
        start_col = head_index * HD
        query_head = lax.dynamic_slice_in_dim(query_norm, start_col, HD, 1)
        key_head = lax.dynamic_slice_in_dim(key_norm, start_col, HD, 1)
        value_head = lax.dynamic_slice_in_dim(values_all, start_col, HD, 1)
        scores = jnp.dot(query_head, key_head.T, preferred_element_type=jnp.float32) / math.sqrt(HD)
        scores = jnp.where(allowed, scores, -1e+30)
        row_peak = lax.optimization_barrier(jnp.max(scores, axis=1, keepdims=True))
        exp_scores = jnp.exp(scores - row_peak)
        attn_probs = (exp_scores / lax.optimization_barrier(jnp.sum(exp_scores, axis=1, keepdims=True))).astype(jnp.bfloat16)
        return jnp.dot(attn_probs, value_head, preferred_element_type=jnp.float32).astype(jnp.bfloat16)
    per_head = lax.map(one_head, jnp.arange(HEADS, dtype=jnp.int32))
    attended = jnp.transpose(per_head, (1, 0, 2)).reshape(TOKENS, HEADS * HD)
    mixed = jnp.dot(attended, out_proj, preferred_element_type=jnp.float32)
    residual = embedded + mixed * modulation[2][None, :]
    return lax.dot_general(final_proj.astype(jnp.float32), residual, (((1,), (1,)), ((), ())), precision=highest)

def reference(hidden_states, gen_weight, noise_field, timesteps, embed_real, time_real, query_real, key_real, value_real, out_real, gain_real, proj_real, embed_fake, time_fake, query_fake, key_fake, value_fake, out_fake, gain_fake, proj_fake):
    grad_root = math.sqrt(SAMPLES * TOKENS)
    gradients = []
    grad_total = jnp.zeros((PATCH, D), jnp.float32)
    for sample in range(SAMPLES):
        time_step = timesteps[sample]
        level_raw = time_step.astype(jnp.float32) / 1000.0
        noise_level = 5.0 * level_raw / (1.0 + 4.0 * level_raw)
        generated = lax.dot_general(gen_weight, hidden_states[sample], (((1,), (1,)), ((), ())), preferred_element_type=jnp.float32).astype(jnp.bfloat16)
        noisy_patch = ((1.0 - noise_level) * generated.astype(jnp.float32) + noise_level * noise_field[sample].astype(jnp.float32)).astype(jnp.bfloat16)
        sinus_wave = sinusoid(time_step)
        vel_real = velocity(noisy_patch, sinus_wave, embed_real, time_real, query_real, key_real, value_real, out_real, gain_real, proj_real)
        vel_fake = velocity(noisy_patch, sinus_wave, embed_fake, time_fake, query_fake, key_fake, value_fake, out_fake, gain_fake, proj_fake)
        pred_real = noisy_patch.astype(jnp.float32) - noise_level * vel_real
        pred_fake = noisy_patch.astype(jnp.float32) - noise_level * vel_fake
        gap_mean = jnp.sum(jnp.abs(generated.astype(jnp.float32) - pred_real)) / (PATCH * TOKENS)
        normalizer = jnp.maximum(gap_mean, gap_floor)
        gap_diff = pred_fake - pred_real
        gradients.append(gap_diff / normalizer)
        difference = gap_diff.astype(jnp.bfloat16)
        partial_grad = jnp.dot(difference, hidden_states[sample], preferred_element_type=jnp.float32)
        grad_total = grad_total + partial_grad / normalizer / grad_root
    return (jnp.stack(gradients), grad_total)
```

```python
import functools
import math

import jax
import jax.numpy as jnp
from jax import lax
from jax.experimental import pallas as pl
from jax.experimental.pallas import tpu as pltpu
from jax.sharding import PartitionSpec as P

HD = 128
FREQ = 256
FT = 128
MESH = pl.DeviceIdType.MESH

norm_floor = 0.05
gap_floor = 0.25
highest = lax.Precision.HIGHEST
f32 = jnp.float32
bf16 = jnp.bfloat16


def split2(a):
    hi = a.astype(bf16)
    lo = (a - hi.astype(f32)).astype(bf16)
    return hi, lo


def stack2(a):
    hi, lo = split2(a)
    return jnp.concatenate([hi, lo], axis=0)


def mm(a, b):
    return jnp.dot(a, b, preferred_element_type=f32)


def mm_t(a, b):
    return lax.dot_general(a, b, (((1,), (1,)), ((), ())), preferred_element_type=f32)


def attend_block(block, blk, qt_ref, k_ref, v_ref, m_ref, o_ref):
    q_at = pl.multiple_of(block * blk, blk)
    frames = blk // FT

    def tile(net, k_at, diagonal):
        s = mm(k_ref[net, pl.ds(k_at, blk), :], qt_ref[net, :, pl.ds(q_at, blk)])
        if diagonal:
            rows = []
            for r in range(frames):
                part = s[r * FT : (r + 1) * FT]
                if r:
                    gone = jnp.full((FT, r * FT), -1e30, f32)
                    part = jnp.concatenate([gone, part[:, r * FT :]], axis=1)
                rows.append(part)
            s = jnp.concatenate(rows, axis=0)
        return s

    for net in range(2):
        s = tile(net, q_at, True)
        top = jnp.max(s, axis=0, keepdims=True)
        p = jnp.exp2(s - top).astype(bf16)
        m_ref[net] = jnp.broadcast_to(top, (8, blk))
        o_ref[net] = mm(v_ref[net, :, pl.ds(q_at, blk)], p)

    def step(kb, _):
        k_at = pl.multiple_of(kb * blk, blk)
        ss = [tile(net, k_at, False) for net in range(2)]
        for net in range(2):
            s = ss[net]
            old = m_ref[net, 0:1, :]
            top = jnp.maximum(old, jnp.max(s, axis=0, keepdims=True))
            p = jnp.exp2(s - top).astype(bf16)
            fade = jnp.exp2(old - top)
            m_ref[net] = jnp.broadcast_to(top, (8, blk))
            o_ref[net] = o_ref[net] * fade + mm(v_ref[net, :, pl.ds(k_at, blk)], p)
        return 0

    lax.fori_loop(0, block, step, 0)


def kernel(
    n, nz, blk,
    sc, noise, time_r, time_f, gain_r, gain_f,
    hidden_h, genw_h, emb_rh, emb_fh, proj_rh, proj_fh, out_rh, out_fh,
    wq_r, wk_r, wv_r, wq_f, wk_f, wv_f,
    dmd_ref, wg_ref,
    hid, genw, emb, proj, outw, wqk, wv,
    modbuf, modin, modfull, xg, xs, gen_s, mu_s, gmat, rmat,
    lhs, acc, lhs2, acc2, accv, rs_s, qraw, kraw, nbuf, nin, nfull,
    qt, kn, vt, m_s, o_s,
    tsend, trecv, gapbuf, wsend, wrecv, zbuf,
    lsem, s_mod, r_mod, s_mod2, r_mod2, s_x, r_x, s_n, r_n, s_n2, r_n2,
    s_t, r_t, s_g, r_g, s_w, r_w, s_z, r_z, s_a, r_a,
):
    me = lax.axis_index("tm")
    mz = lax.axis_index("batch")
    d = hid.shape[1]
    groups = d // 1024
    tokens = n * FT

    loads = []

    def load(src, dst):
        c = pltpu.make_async_copy(src, dst, lsem.at[len(loads)])
        c.start()
        loads.append(c)
        return c

    ld_hid = load(hidden_h.at[0], hid)
    ld_gen = load(genw_h, genw)
    ld_emb = [load(emb_rh, emb.at[0]), load(emb_fh, emb.at[1])]
    ld_proj = [load(proj_rh, proj.at[0]), load(proj_fh, proj.at[1])]
    ld_qk = []
    for net, (a, b) in enumerate(((wq_r, wk_r), (wq_f, wk_f))):
        ld_qk.append(load(a, wqk.at[net, :, 0:HD]))
        ld_qk.append(load(b, wqk.at[net, :, HD : 2 * HD]))
    ld_v = [load(wv_r, wv.at[0]), load(wv_f, wv.at[1])]
    ld_out = [load(out_rh, outw.at[0]), load(out_fh, outw.at[1])]

    barrier = pltpu.get_barrier_semaphore()

    def greet(i, _):
        pl.semaphore_signal(
            barrier, inc=1, device_id={"tm": lax.rem(me + i, n)}, device_id_type=MESH
        )
        return 0

    lax.fori_loop(1, n, greet, 0)
    for i in range(1, nz):
        pl.semaphore_signal(
            barrier, inc=1, device_id={"batch": lax.rem(mz + i, nz)}, device_id_type=MESH
        )

    def rc(src, dst, ssem, rsem, j):
        return pltpu.make_async_remote_copy(
            src_ref=src, dst_ref=dst, send_sem=ssem, recv_sem=rsem,
            device_id={"tm": j}, device_id_type=MESH,
        )

    def spread(src_of, dst_of, ss, rr):
        def body(i, _):
            j = lax.rem(me + i, n)
            rc(src_of(j), dst_of(me), ss.at[i], rr.at[i], j).start()
            return 0

        lax.fori_loop(1, n, body, 0)

    def collect(src_of, dst_of, ss, rr):
        def body(i, _):
            j = lax.rem(me + i, n)
            frm = lax.rem(me + n - i, n)
            c = rc(src_of(j), dst_of(frm), ss.at[i], rr.at[i], j)
            c.wait_recv()
            c.wait_send()
            return 0

        lax.fori_loop(1, n, body, 0)

    for p in range(6 * groups, n):
        modbuf[p] = jnp.zeros((8, 128), f32)
    for net, table in enumerate((time_r, time_f)):
        for g in range(groups):
            part = None
            for f in range(table.shape[0]):
                term = sc[8 + f] * table[f, :, g * 1024 : (g + 1) * 1024].astype(f32)
                part = term if part is None else part + term
            for c in range(3):
                for r in range(8):
                    modbuf[(net * 3 + c) * groups + g, r : r + 1, :] = part[
                        c : c + 1, r * 128 : (r + 1) * 128
                    ]
    modin[me] = modbuf[me]
    pl.semaphore_wait(barrier, n - 1 + nz - 1)
    spread(lambda j: modbuf.at[j], lambda s: modin.at[s], s_mod, r_mod)

    ld_hid.wait()
    ld_gen.wait()
    generated = mm_t(genw[...], hid[...]).astype(bf16)
    gen_s[...] = generated
    xg[0] = jnp.zeros(xg.shape[1:], bf16)
    xg[me + 1] = (sc[1] * generated.astype(f32) + sc[0] * noise[0].astype(f32)).astype(bf16)
    spread(lambda j: xg.at[me + 1], lambda s: xg.at[s + 1], s_x, r_x)

    for net in range(2):
        ld_emb[net].wait()
        ld_proj[net].wait()

        def total(g, t):
            at = pl.multiple_of(g * 1024, 1024)
            return t + jnp.sum(emb[net, :, pl.ds(at, 1024)].astype(f32), axis=1, keepdims=True)

        mu = lax.fori_loop(0, groups, total, jnp.zeros((128, 1), f32)) / d
        mu_s[net] = jnp.broadcast_to(mu, (128, 128))

        def gram(g, t):
            at = pl.multiple_of(g * 1024, 1024)
            e = emb[net, :, pl.ds(at, 1024)]
            hi, lo = split2(e.astype(f32) - mu)
            both = jnp.concatenate([hi, lo], axis=0)
            return t[0] + mm_t(both, hi), t[1] + mm_t(proj[net, :, pl.ds(at, 1024)], e)

        gg, rr = lax.fori_loop(
            0, groups, gram, (jnp.zeros((256, 128), f32), jnp.zeros((64, 128), f32))
        )
        lh = gg[128:256]
        gmat[net] = stack2((gg[0:128] + lh + lh.T) / d)
        rmat[net] = stack2(rr)

    collect(lambda j: modbuf.at[j], lambda s: modin.at[s], s_mod, r_mod)
    modfull[me] = jnp.sum(modin[...], axis=0)
    spread(lambda j: modfull.at[me], lambda s: modfull.at[s], s_mod2, r_mod2)

    collect(lambda j: xg.at[me + 1], lambda s: xg.at[s + 1], s_x, r_x)

    def place(j, _):
        at = pl.multiple_of(j * FT, FT)
        xs[0:64, pl.ds(at, FT)] = xg[j + 1]
        xs[64:128, pl.ds(at, FT)] = xg[j]
        return 0

    lax.fori_loop(0, n, place, 0)

    width = blk

    def variances(t, _):
        at = pl.multiple_of(t * width, width)
        x = xs[:, pl.ds(at, width)]
        for net in range(2):
            y = mm(gmat[net], x)
            var = jnp.sum((y[0:128] + y[128:256]) * x.astype(f32), axis=0, keepdims=True)
            rs = lax.rsqrt(jnp.maximum(var, 0.0) + norm_floor)
            rs_s[net, :, pl.ds(at, width)] = jnp.broadcast_to(rs, (8, width))
        return 0

    lax.fori_loop(0, tokens // width, variances, 0)

    collect(lambda j: modfull.at[me], lambda s: modfull.at[s], s_mod2, r_mod2)

    for c in ld_qk:
        c.wait()
    row = lax.broadcasted_iota(jnp.int32, (16, 128), 0)
    for net in range(2):
        acc[...] = jnp.zeros_like(acc)

        def fold(g, _):
            at = pl.multiple_of(g * 1024, 1024)
            shift8 = modfull[(net * 3 + 0) * groups + g]
            scale8 = modfull[(net * 3 + 1) * groups + g]
            for r in range(8):
                col = pl.multiple_of(at + r * 128, 128)
                e = emb[net, :, pl.ds(col, 128)].astype(f32) - mu_s[net]
                hi, lo = split2(e * (1.0 + scale8[r : r + 1, :]))
                sh, sl = split2(shift8[r : r + 1, :])
                lhs[net, 0:128, pl.ds(col, 128)] = hi
                lhs[net, 128:256, pl.ds(col, 128)] = lo
                tail = jnp.where(
                    row == 0, sh.astype(f32), jnp.where(row == 1, sl.astype(f32), 0.0)
                )
                lhs[net, 256:272, pl.ds(col, 128)] = tail.astype(bf16)
            acc[...] += mm(lhs[net, :, pl.ds(at, 1024)], wqk[net, pl.ds(at, 1024), :])
            return 0

        lax.fori_loop(0, groups, fold, 0)
        a = acc[0:128, :] + acc[128:256, :]
        off = acc[256:257, :] + acc[257:258, :]
        a_q = stack2(a[:, 0:HD].T)
        a_k = stack2(a[:, HD : 2 * HD].T)
        off_q = jnp.broadcast_to(off[:, 0:HD], (128, 128)).T[:, 0:1]
        off_k = jnp.broadcast_to(off[:, HD : 2 * HD], (128, 128)).T[:, 0:1]

        def project(t, _):
            at = pl.multiple_of(t * width, width)
            x = xs[:, pl.ds(at, width)]
            rs = rs_s[net, 0:1, pl.ds(at, width)]
            for which, (mat, off_c, dst) in enumerate(((a_q, off_q, qraw), (a_k, off_k, kraw))):
                y = mm(mat, x)
                y = (y[0:128] + y[128:256]) * rs + off_c
                dst[net, :, pl.ds(at, width)] = y
                sq = jnp.sum(y * y, axis=0, keepdims=True)
                for r in range(width // FT):
                    nbuf[t * (width // FT) + r, net * 2 + which : net * 2 + which + 1, :] = sq[
                        :, r * FT : (r + 1) * FT
                    ]
            return 0

        lax.fori_loop(0, tokens // width, project, 0)

    nin[me] = nbuf[me]
    spread(lambda j: nbuf.at[j], lambda s: nin.at[s], s_n, r_n)

    for c in ld_v + ld_out:
        c.wait()
    for net in range(2):
        accv[...] = jnp.zeros_like(accv)
        acc2[...] = jnp.zeros_like(acc2)

        def fold_v(g, _):
            at = pl.multiple_of(g * 1024, 1024)
            gate8 = modfull[(net * 3 + 2) * groups + g]
            for r in range(8):
                col = pl.multiple_of(at + r * 128, 128)
                hi, lo = split2(proj[net, :, pl.ds(col, 128)].astype(f32) * gate8[r : r + 1, :])
                lhs2[0:64, r * 128 : (r + 1) * 128] = hi
                lhs2[64:128, r * 128 : (r + 1) * 128] = lo
            accv[...] += mm(lhs[net, :, pl.ds(at, 1024)], wv[net, pl.ds(at, 1024), :])
            acc2[...] += mm_t(lhs2[...], outw[net, :, pl.ds(at, 1024)])
            return 0

        lax.fori_loop(0, groups, fold_v, 0)
        a = accv[0:128, :] + accv[128:256, :]
        off = accv[256:257, :] + accv[257:258, :]
        out_t = acc2[0:64, :] + acc2[64:128, :]
        b_mat = stack2(
            lax.dot_general(
                out_t, a, (((1,), (1,)), ((), ())), precision=highest, preferred_element_type=f32
            )
        )
        off_v = jnp.sum(out_t * off, axis=1, keepdims=True)
        ones = jnp.where(lax.broadcasted_iota(jnp.int32, (16, width), 0) == 0, 1.0, 0.0)

        def values(t, _):
            at = pl.multiple_of(t * width, width)
            y = mm(b_mat, xs[:, pl.ds(at, width)])
            y = (y[0:64] + y[64:128]) * rs_s[net, 0:1, pl.ds(at, width)] + off_v
            vt[net, 0:64, pl.ds(at, width)] = y.astype(bf16)
            vt[net, 64:80, pl.ds(at, width)] = ones.astype(bf16)
            return 0

        lax.fori_loop(0, tokens // width, values, 0)

    collect(lambda j: nbuf.at[j], lambda s: nin.at[s], s_n, r_n)
    nfull[me] = lax.rsqrt(jnp.sum(nin[...], axis=0) / tokens_cols(n) + norm_floor)
    spread(lambda j: nfull.at[me], lambda s: nfull.at[s], s_n2, r_n2)
    collect(lambda j: nfull.at[me], lambda s: nfull.at[s], s_n2, r_n2)

    for net, gain in enumerate((gain_r, gain_f)):
        both = gain[0:1, :] * gain[1:2, :] * (math.log2(math.e) / math.sqrt(HD))
        g_col = jnp.broadcast_to(both, (128, 128)).T

        def normalise(j, _):
            at = pl.multiple_of(j * FT, FT)
            sq = nfull[j, net * 2 : net * 2 + 1, :]
            sk = nfull[j, net * 2 + 1 : net * 2 + 2, :]
            qt[net, :, pl.ds(at, FT)] = (qraw[net, :, pl.ds(at, FT)] * sq * g_col).astype(bf16)
            kn[net, pl.ds(at, FT), :] = (kraw[net, :, pl.ds(at, FT)] * sk).T.astype(bf16)
            return 0

        lax.fori_loop(0, n, normalise, 0)

    blocks = tokens // blk
    per = blk // FT

    def t_copy(f):
        return rc(tsend.at[f], trecv.at[me], s_t.at[f], r_t.at[me], f)

    def one_block(s, _):
        block = lax.rem(s + me, blocks)
        attend_block(block, blk, qt, kn, vt, m_s, o_s)
        for net in range(2):
            o = o_s[net]
            y = (o[0:64] / o[64:65]).astype(bf16)
            for r in range(per):
                tsend[block * per + r, net * 64 : (net + 1) * 64, :] = y[:, r * FT : (r + 1) * FT]
        for r in range(per):
            f = block * per + r

            @pl.when(f != me)
            def _():
                t_copy(f).start()

        return 0

    lax.fori_loop(0, blocks, one_block, 0)
    trecv[me] = tsend[me]

    def t_wait(i, _):
        frm = lax.rem(me + n - i, n)
        f = lax.rem(me + i, n)
        rc(tsend.at[f], trecv.at[frm], s_t.at[f], r_t.at[frm], f).wait_recv()
        t_copy(f).wait_send()
        return 0

    lax.fori_loop(1, n, t_wait, 0)

    def add_up(s, t):
        return t + trecv[s].astype(f32)

    vel = lax.fori_loop(0, n, add_up, jnp.zeros((128, FT), f32))
    x_own = jnp.concatenate([xg[me + 1], xg[me]], axis=0)
    base_r = mm(rmat[0], x_own)
    base_f = mm(rmat[1], x_own)
    vel_r = vel[0:64] + base_r[0:64] + base_r[64:128]
    vel_f = vel[64:128] + base_f[0:64] + base_f[64:128]
    noisy = xg[me + 1].astype(f32)
    pred_r = noisy - sc[0] * vel_r
    pred_f = noisy - sc[0] * vel_f
    gap = jnp.abs(gen_s[...].astype(f32) - pred_r)
    gsum = gap[0:8]
    for r in range(1, 8):
        gsum = gsum + gap[r * 8 : (r + 1) * 8]
    gapbuf[me] = gsum
    spread(lambda j: gapbuf.at[me], lambda s: gapbuf.at[s], s_g, r_g)
    diff = pred_f - pred_r
    diff_b = diff.astype(bf16)

    def wg_part(g, _):
        at = pl.multiple_of(g * 1024, 1024)
        y = mm(diff_b, hid[:, pl.ds(at, 1024)]).astype(bf16)
        for r in range(8):
            to = pl.multiple_of((g * 8 + r) * 64, 64)
            wsend[pl.ds(to, 64), :] = y[:, r * 128 : (r + 1) * 128]
        return 0

    lax.fori_loop(0, groups, wg_part, 0)
    rows = wsend.shape[0] // n

    def w_src(j):
        return wsend.at[pl.ds(pl.multiple_of(j * rows, 16), rows), :]

    spread(w_src, lambda s: wrecv.at[s], s_w, r_w)
    wrecv[me] = wsend[pl.ds(pl.multiple_of(me * rows, 16), rows), :]
    collect(lambda j: gapbuf.at[me], lambda s: gapbuf.at[s], s_g, r_g)
    gap_all = jnp.sum(jnp.sum(gapbuf[...], axis=0), keepdims=True)
    inv = 1.0 / jnp.maximum(gap_all / (64.0 * tokens), gap_floor)
    dmd_ref[0] = diff * inv
    collect(w_src, lambda s: wrecv.at[s], s_w, r_w)

    def add_w(s, t):
        return t + wrecv[s].astype(f32)

    wsum = lax.fori_loop(0, n, add_w, jnp.zeros((rows, 128), f32))
    zbuf[mz] = (wsum * (inv / math.sqrt(nz * tokens))).astype(bf16)

    def zc(i, frm):
        j = lax.rem(mz + i, nz)
        return pltpu.make_async_remote_copy(
            src_ref=zbuf.at[mz], dst_ref=zbuf.at[frm], send_sem=s_z.at[i], recv_sem=r_z.at[i],
            device_id={"batch": j}, device_id_type=MESH,
        )

    for i in range(1, nz):
        zc(i, mz).start()
    for i in range(1, nz):
        c = zc(i, lax.rem(mz + nz - i, nz))
        c.wait_recv()
        c.wait_send()
    whole = zbuf[0].astype(f32)
    for z in range(1, nz):
        whole = whole + zbuf[z].astype(f32)
    wg_ref[me] = whole.astype(bf16)
    spread(lambda j: wg_ref.at[me], lambda s: wg_ref.at[s], s_a, r_a)
    collect(lambda j: wg_ref.at[me], lambda s: wg_ref.at[s], s_a, r_a)


def tokens_cols(n):
    return float(n * HD)


def per_device(
    hidden_states, gen_weight, noise_field, timesteps,
    embed_real, time_real, query_real, key_real, value_real, out_real, gain_real, proj_real,
    embed_fake, time_fake, query_fake, key_fake, value_fake, out_fake, gain_fake, proj_fake,
):
    n = lax.axis_size("tm")
    nz = lax.axis_size("batch")
    d = hidden_states.shape[2]
    tokens = n * FT
    blk = 512
    rows = 64 * d // 128 // n
    fr = time_real.shape[0]
    step = timesteps[0].astype(f32)
    raw = step / 1000.0
    sigma = 5.0 * raw / (1.0 + 4.0 * raw)
    half = FREQ // 2
    at = lax.axis_index("tm") * fr + jnp.arange(fr, dtype=jnp.int32)
    freq = jnp.exp(-math.log(10000.0) * (at % half).astype(f32) / half)
    wave = jnp.where(at < half, jnp.cos(step * freq), jnp.sin(step * freq))
    wave = wave.astype(bf16).astype(f32)
    slot = jnp.arange(8)
    head = jnp.where(slot == 0, sigma, jnp.where(slot == 1, 1.0 - sigma, 0.0))
    sc = jnp.concatenate([head, wave])

    vm = pl.BlockSpec(memory_space=pltpu.VMEM)
    hbm = pl.BlockSpec(memory_space=pl.ANY)
    sems = pltpu.SemaphoreType.DMA
    nb = tokens // blk
    scratch = [
        pltpu.VMEM((FT, d), bf16),
        pltpu.VMEM((64, d), bf16),
        pltpu.VMEM((2, 128, d), bf16),
        pltpu.VMEM((2, 64, d), bf16),
        pltpu.VMEM((2, 128, d), bf16),
        pltpu.VMEM((2, d, 256), bf16),
        pltpu.VMEM((2, d, 128), bf16),
        pltpu.VMEM((n, 8, 128), f32),
        pltpu.VMEM((n, 8, 128), f32),
        pltpu.VMEM((n, 8, 128), f32),
        pltpu.VMEM((n + 1, 64, 128), bf16),
        pltpu.VMEM((128, tokens), bf16),
        pltpu.VMEM((64, 128), bf16),
        pltpu.VMEM((2, 128, 128), f32),
        pltpu.VMEM((2, 256, 128), bf16),
        pltpu.VMEM((2, 128, 128), bf16),
        pltpu.VMEM((2, 272, d), bf16),
        pltpu.VMEM((272, 256), f32),
        pltpu.VMEM((128, 1024), bf16),
        pltpu.VMEM((128, 128), f32),
        pltpu.VMEM((272, 128), f32),
        pltpu.VMEM((2, 8, tokens), f32),
        pltpu.VMEM((2, 128, tokens), f32),
        pltpu.VMEM((2, 128, tokens), f32),
        pltpu.VMEM((n, 8, 128), f32),
        pltpu.VMEM((n, 8, 128), f32),
        pltpu.VMEM((n, 8, 128), f32),
        pltpu.VMEM((2, 128, tokens), bf16),
        pltpu.VMEM((2, tokens, 128), bf16),
        pltpu.VMEM((2, 80, tokens), bf16),
        pltpu.VMEM((2, 8, blk), f32),
        pltpu.VMEM((2, 80, blk), f32),
        pltpu.VMEM((n, 128, 128), bf16),
        pltpu.VMEM((n, 128, 128), bf16),
        pltpu.VMEM((n, 8, 128), f32),
        pltpu.VMEM((rows * n, 128), bf16),
        pltpu.VMEM((n, rows, 128), bf16),
        pltpu.VMEM((nz, rows, 128), bf16),
        sems((16,)),
    ] + [sems((n,)) for _ in range(20)]
    dmd, wg = pl.pallas_call(
        functools.partial(kernel, n, nz, blk),
        out_shape=(
            jax.ShapeDtypeStruct((1, 64, FT), f32),
            jax.ShapeDtypeStruct((n, rows, 128), bf16),
        ),
        in_specs=[pl.BlockSpec(memory_space=pltpu.SMEM)] + [vm] * 5 + [hbm] * 14,
        out_specs=(vm, vm),
        scratch_shapes=scratch,
        compiler_params=pltpu.CompilerParams(
            collective_id=0, has_side_effects=True, vmem_limit_bytes=60 * 1024 * 1024
        ),
        name="dmd",
    )(
        sc, noise_field, time_real, time_fake, gain_real, gain_fake,
        hidden_states, gen_weight, embed_real, embed_fake, proj_real, proj_fake,
        out_real, out_fake,
        query_real, key_real, value_real, query_fake, key_fake, value_fake,
    )
    wg = wg.reshape(d // 128, 64, 128).transpose(1, 0, 2).reshape(64, d).astype(f32)
    return dmd, wg


def solution(mesh):
    in_specs = (
        P("batch", "tm", None), P(), P("batch", None, "tm"), P("batch"),
        P(), P("tm", None, None), P(None, "tm"), P(None, "tm"), P(None, "tm"),
        P("tm", None), P(None, "tm"), P(),
        P(), P("tm", None, None), P(None, "tm"), P(None, "tm"), P(None, "tm"),
        P("tm", None), P(None, "tm"), P(),
    )
    out_specs = (P("batch", None, "tm"), P())
    return jax.shard_map(
        per_device, mesh=mesh, in_specs=in_specs, out_specs=out_specs, check_vma=False
    )
```

```python
import functools
import math

import jax
import jax.numpy as jnp
from jax import lax
from jax.experimental import pallas as pl
from jax.experimental.pallas import tpu as pltpu
from jax.sharding import PartitionSpec as P

HD = 128
FREQ = 256
FT = 128
MESH = pl.DeviceIdType.MESH

norm_floor = 0.05
gap_floor = 0.25
highest = lax.Precision.HIGHEST
f32 = jnp.float32
bf16 = jnp.bfloat16


def split2(a):
    hi = a.astype(bf16)
    lo = (a - hi.astype(f32)).astype(bf16)
    return hi, lo


def stack2(a):
    hi, lo = split2(a)
    return jnp.concatenate([hi, lo], axis=0)


def mm(a, b):
    return jnp.dot(a, b, preferred_element_type=f32)


def mm_t(a, b):
    return lax.dot_general(a, b, (((1,), (1,)), ((), ())), preferred_element_type=f32)


class Phase:
    def __init__(self):
        self.now = None

    def __call__(self, name):
        if self.now is not None:
            self.now.__exit__(None, None, None)
        self.now = None
        if name:
            self.now = jax.named_scope(name)
            self.now.__enter__()


def attend_block(block, blk, tokens, qt_ref, k_ref, v_ref, m_ref, o_ref, s_ref):
    q_at = pl.multiple_of(block * blk, blk)
    frames = blk // FT

    def score(net, k_at):
        return mm(k_ref[net, pl.ds(k_at, blk), :], qt_ref[net, :, pl.ds(q_at, blk)])

    for net in range(2):
        s_ref[net] = score(net, 0)
    for net in range(2):
        s = score(net, q_at)
        rows = []
        for r in range(frames):
            part = s[r * FT : (r + 1) * FT]
            if r:
                gone = jnp.full((FT, r * FT), -1e30, f32)
                part = jnp.concatenate([gone, part[:, r * FT :]], axis=1)
            rows.append(part)
        s = jnp.concatenate(rows, axis=0)
        top = jnp.max(s, axis=0, keepdims=True)
        p = jnp.exp2(s - top).astype(bf16)
        m_ref[net] = jnp.broadcast_to(top, (8, blk))
        o_ref[net] = mm(v_ref[net, :, pl.ds(q_at, blk)], p)

    def step(kb, _):
        k_at = pl.multiple_of(kb * blk, blk)
        next_at = pl.multiple_of(jnp.minimum(kb + 1, tokens // blk - 1) * blk, blk)
        for net in range(2):
            s = s_ref[net]
            old = m_ref[net, 0:1, :]
            top = jnp.maximum(old, jnp.max(s, axis=0, keepdims=True))
            p = jnp.exp2(s - top).astype(bf16)
            ahead = score(net, next_at)
            fade = jnp.exp2(old - top)
            o_ref[net] = o_ref[net] * fade + mm(v_ref[net, :, pl.ds(k_at, blk)], p)
            m_ref[net] = jnp.broadcast_to(top, (8, blk))
            s_ref[net] = ahead
        return 0

    lax.fori_loop(0, block, step, 0)


def block_at(s, me, per, blocks):
    home = me // per
    if blocks != 8:
        return lax.rem(home + 1 + s, blocks)
    dx = jnp.where(s < 2, 2, jnp.where(s < 6, 1 + 2 * lax.rem(s - 2, 2), 0))
    dy = jnp.where(s < 2, 1 - s, jnp.where(s < 4, 1, jnp.where(s < 6, 0, 7 - s)))
    x = lax.rem(home // 2 + dx, 4)
    y = lax.rem(home + dy, 2)
    return x * 2 + y


def kernel(
    n, nz, blk,
    sc, wave, noise, gain_r, gain_f,
    time_rh, time_fh, hidden_h, genw_h, emb_rh, emb_fh, proj_rh, proj_fh, out_rh, out_fh,
    wq_r, wk_r, wv_r, wq_f, wk_f, wv_f,
    dmd_ref, wg_ref,
    times, hid, genw, emb, proj, outw, wqk, wv,
    modbuf, modin, modfull, xg, xs, gen_s, mu_s, gmat, rmat,
    lhs, acc, lhs2, acc2, accv, rs_s, qraw, kraw, ktok, nbuf, nin, nfull,
    qt, kn, vt, m_s, o_s, s_s,
    tsend, trecv, gapbuf, wown, wgive, wtake, wsend, wrecv, zbuf,
    lsem, sem,
):
    me = lax.axis_index("tm")
    mz = lax.axis_index("batch")
    core = lax.rem(me, 2)
    chip = me // 2
    other = me + 1 - 2 * core
    chips = n // 2
    d = hid.shape[1]
    groups = d // 1024
    tokens = n * FT
    ph = Phase()
    loads = []

    def load(src, dst):
        c = pltpu.make_async_copy(src, dst, lsem.at[len(loads)])
        c.start()
        loads.append(c)
        return c

    ld_time = [load(time_rh, times.at[0]), load(time_fh, times.at[1])]
    ld_hid = load(hidden_h.at[0], hid)
    ld_gen = load(genw_h, genw)
    ld_emb = [load(emb_rh, emb.at[0]), load(emb_fh, emb.at[1])]
    ld_proj = [load(proj_rh, proj.at[0]), load(proj_fh, proj.at[1])]
    ld_qk = []
    for net, (a, b) in enumerate(((wq_r, wk_r), (wq_f, wk_f))):
        ld_qk.append(load(a, wqk.at[net, :, 0:HD]))
        ld_qk.append(load(b, wqk.at[net, :, HD : 2 * HD]))
    ld_v = [load(wv_r, wv.at[0]), load(wv_f, wv.at[1])]
    ld_out = [load(out_rh, outw.at[0]), load(out_fh, outw.at[1])]

    barrier = pltpu.get_barrier_semaphore()

    def greet(i, _):
        pl.semaphore_signal(
            barrier, inc=1, device_id={"tm": lax.rem(me + i, n)}, device_id_type=MESH
        )
        return 0

    lax.fori_loop(1, n, greet, 0)
    for i in range(1, nz):
        pl.semaphore_signal(
            barrier, inc=1, device_id={"batch": lax.rem(mz + i, nz)}, device_id_type=MESH
        )

    used = [0]

    class Lane:
        def __init__(self):
            self.send = sem.at[used[0]]
            self.recv = sem.at[used[0] + 1]
            used[0] += 2

        def to(self, src, dst, j, axis="tm"):
            return pltpu.make_async_remote_copy(
                src_ref=src, dst_ref=dst, send_sem=self.send, recv_sem=self.recv,
                device_id={axis: j}, device_id_type=MESH,
            )

        def all(self, src_of, dst):
            def body(i, _):
                j = lax.rem(me + i, n)
                self.to(src_of(j), dst, j).start()
                return 0

            lax.fori_loop(1, n, body, 0)

        def mates(self, src_of, dst):
            def body(i, _):
                j = lax.rem(chip + i, chips)
                self.to(src_of(j), dst, 2 * j + core).start()
                return 0

            lax.fori_loop(1, chips, body, 0)

        def wait(self, view):
            c = self.to(view, view, other)
            c.wait_recv()
            c.wait_send()

    mod_rs, mod_ag, xl, xf = Lane(), Lane(), Lane(), Lane()
    nrm_rs, nrm_ag, tl, gl = Lane(), Lane(), Lane(), Lane()
    w_pair, w_rs, w_z, w_ag, w_fw = Lane(), Lane(), Lane(), Lane(), Lane()

    ph("share")
    for p in range(6 * groups, n):
        modbuf[p] = jnp.zeros((8, 128), f32)
    for net in range(2):
        ld_time[net].wait()
        for c in range(3):
            for b in range(8 * groups):
                t = times[net, c, :, b * 128 : (b + 1) * 128].astype(f32)
                part = jnp.sum(t * wave[...], axis=0, keepdims=True)
                modbuf[(net * 3 + c) * groups + b // 8, b % 8 : b % 8 + 1, :] = part
    modin[me] = modbuf[me]

    ph("generate")
    ld_hid.wait()
    ld_gen.wait()
    generated = mm_t(genw[...], hid[...]).astype(bf16)
    gen_s[...] = generated
    xg[chip, core] = (sc[1] * generated.astype(f32) + sc[0] * noise[0].astype(f32)).astype(bf16)

    def weight_terms(net):
        ld_emb[net].wait()
        ld_proj[net].wait()

        def total(g, t):
            at = pl.multiple_of(g * 1024, 1024)
            return t + jnp.sum(emb[net, :, pl.ds(at, 1024)].astype(f32), axis=1, keepdims=True)

        mu = lax.fori_loop(0, groups, total, jnp.zeros((128, 1), f32)) / d
        mu_s[net] = jnp.broadcast_to(mu, (128, 128))

        def gram(g, t):
            at = pl.multiple_of(g * 1024, 1024)
            e = emb[net, :, pl.ds(at, 1024)]
            hi, lo = split2(e.astype(f32) - mu)
            both = jnp.concatenate([hi, lo], axis=0)
            return t[0] + mm_t(both, hi), t[1] + mm_t(proj[net, :, pl.ds(at, 1024)], e)

        gg, rr = lax.fori_loop(
            0, groups, gram, (jnp.zeros((256, 128), f32), jnp.zeros((64, 128), f32))
        )
        lh = gg[128:256]
        gmat[net] = stack2((gg[0:128] + lh + lh.T) / d)
        rmat[net] = stack2(rr)

    ph("weights0")
    weight_terms(0)
    ph("barrier")
    pl.semaphore_wait(barrier, n - 1 + nz - 1)
    mod_rs.all(lambda j: modbuf.at[j], modin.at[me])
    mine = xg.at[chip, core]
    xl.mates(lambda j: mine, mine)
    ph("weights1")
    weight_terms(1)

    ph("mod_rs")
    mod_rs.wait(modin.at[pl.ds(0, n - 1)])
    modfull[me] = jnp.sum(modin[...], axis=0)
    mod_ag.all(lambda j: modfull.at[me], modfull.at[me])

    ph("x_wait")
    xl.wait(xg.at[pl.ds(0, chips - 1), core])
    xf.to(xg.at[:, core], xg.at[:, core], other).start()
    xf.wait(xg.at[:, core])

    ph("place_var")

    def place(j, _):
        at = pl.multiple_of(j * FT, FT)
        xs[0:64, pl.ds(at, FT)] = xg[j // 2, lax.rem(j, 2)]
        return 0

    def place_late(j, _):
        at = pl.multiple_of(j * FT, FT)
        xs[64:128, pl.ds(at, FT)] = xg[(j - 1) // 2, lax.rem(j - 1, 2)]
        return 0

    xs[64:128, 0:FT] = jnp.zeros((64, FT), bf16)
    lax.fori_loop(0, n, place, 0)
    lax.fori_loop(1, n, place_late, 0)

    width = blk

    def variances(t, _):
        at = pl.multiple_of(t * width, width)
        x = xs[:, pl.ds(at, width)]
        for net in range(2):
            y = mm(gmat[net], x)
            var = jnp.sum((y[0:128] + y[128:256]) * x.astype(f32), axis=0, keepdims=True)
            rs = lax.rsqrt(jnp.maximum(var, 0.0) + norm_floor)
            rs_s[net, :, pl.ds(at, width)] = jnp.broadcast_to(rs, (8, width))
        return 0

    lax.fori_loop(0, tokens // width, variances, 0)
    for c in ld_qk:
        c.wait()
    ph("mod_ag_wait")
    mod_ag.wait(modfull.at[pl.ds(0, n - 1)])

    ph("qk_fold")
    row = lax.broadcasted_iota(jnp.int32, (16, 128), 0)
    acc[...] = jnp.zeros_like(acc)

    def fold(g, _):
        at = pl.multiple_of(g * 1024, 1024)
        for net in range(2):
            shift8 = modfull[(net * 3 + 0) * groups + g]
            scale8 = modfull[(net * 3 + 1) * groups + g]
            for r in range(8):
                col = pl.multiple_of(at + r * 128, 128)
                e = emb[net, :, pl.ds(col, 128)].astype(f32) - mu_s[net]
                lhs[net, 0:128, pl.ds(col, 128)] = (e * (1.0 + scale8[r : r + 1, :])).astype(bf16)
                sh, sl = split2(shift8[r : r + 1, :])
                tail = jnp.where(
                    row == 0, sh.astype(f32), jnp.where(row == 1, sl.astype(f32), 0.0)
                )
                lhs[net, 128:144, pl.ds(col, 128)] = tail.astype(bf16)
            acc[net] += mm(lhs[net, :, pl.ds(at, 1024)], wqk[net, pl.ds(at, 1024), :])
        return 0

    lax.fori_loop(0, groups, fold, 0)
    ph("qk_project")
    mats = []
    for net in range(2):
        off = acc[net, 128:129, :] + acc[net, 129:130, :]
        for which in range(2):
            cols = slice(which * HD, (which + 1) * HD)
            mat = acc[net, 0:128, cols].T.astype(bf16)
            mats.append((mat, jnp.broadcast_to(off[:, cols], (128, 128)).T[:, 0:1]))

    def project(t, _):
        at = pl.multiple_of(t * width, width)
        x = xs[:, pl.ds(at, width)]
        for net in range(2):
            rs = rs_s[net, 0:1, pl.ds(at, width)]
            for which, dst in enumerate((qraw, kraw)):
                mat, off_c = mats[net * 2 + which]
                y = mm(mat, x) * rs + off_c
                dst[net, :, pl.ds(at, width)] = y
                sq = jnp.sum(y * y, axis=0, keepdims=True)
                for r in range(width // FT):
                    nbuf[t * (width // FT) + r, net * 2 + which : net * 2 + which + 1, :] = sq[
                        :, r * FT : (r + 1) * FT
                    ]
        return 0

    lax.fori_loop(0, tokens // width, project, 0)

    ph("norm_send")
    nin[me] = nbuf[me]
    nrm_rs.all(lambda j: nbuf.at[j], nin.at[me])

    ph("v_fold")
    for c in ld_v + ld_out:
        c.wait()
    accv[...] = jnp.zeros_like(accv)
    acc2[...] = jnp.zeros_like(acc2)

    def fold_v(g, _):
        at = pl.multiple_of(g * 1024, 1024)
        for net in range(2):
            gate8 = modfull[(net * 3 + 2) * groups + g]
            for r in range(8):
                col = pl.multiple_of(at + r * 128, 128)
                gated = proj[net, :, pl.ds(col, 128)].astype(f32) * gate8[r : r + 1, :]
                hi, lo = split2(gated)
                lhs2[net, 0:64, r * 128 : (r + 1) * 128] = hi
                lhs2[net, 64:128, r * 128 : (r + 1) * 128] = lo
            accv[net] += mm(lhs[net, :, pl.ds(at, 1024)], wv[net, pl.ds(at, 1024), :])
            acc2[net] += mm_t(lhs2[net], outw[net, :, pl.ds(at, 1024)])
        return 0

    lax.fori_loop(0, groups, fold_v, 0)

    ph("norm_rs_wait")
    nrm_rs.wait(nin.at[pl.ds(0, n - 1)])
    nfull[me] = lax.rsqrt(jnp.sum(nin[...], axis=0) / float(n * HD) + norm_floor)
    nrm_ag.all(lambda j: nfull.at[me], nfull.at[me])

    ph("values")
    vmats = []
    for net in range(2):
        a = accv[net, 0:128, :]
        off = accv[net, 128:129, :] + accv[net, 129:130, :]
        out_t = acc2[net, 0:64, :] + acc2[net, 64:128, :]
        b_mat = stack2(
            lax.dot_general(
                out_t, a, (((1,), (1,)), ((), ())), precision=highest, preferred_element_type=f32
            )
        )
        vmats.append((b_mat, jnp.sum(out_t * off, axis=1, keepdims=True)))
    ones = jnp.where(lax.broadcasted_iota(jnp.int32, (16, width), 0) == 0, 1.0, 0.0)

    def values(t, _):
        at = pl.multiple_of(t * width, width)
        x = xs[:, pl.ds(at, width)]
        for net in range(2):
            y = mm(vmats[net][0], x)
            y = (y[0:64] + y[64:128]) * rs_s[net, 0:1, pl.ds(at, width)] + vmats[net][1]
            vt[net, 0:64, pl.ds(at, width)] = y.astype(bf16)
            vt[net, 64:80, pl.ds(at, width)] = ones.astype(bf16)
        return 0

    lax.fori_loop(0, tokens // width, values, 0)
    ph("turn")
    gains = []
    for gain in (gain_r, gain_f):
        both = gain[0:1, :] * gain[1:2, :] * (math.log2(math.e) / math.sqrt(HD))
        gains.append(jnp.broadcast_to(both, (128, 128)).T)

    def turn(j, _):
        at = pl.multiple_of(j * FT, FT)
        for net in range(2):
            ktok[net, pl.ds(at, FT), :] = kraw[net, :, pl.ds(at, FT)].T
            qraw[net, :, pl.ds(at, FT)] = qraw[net, :, pl.ds(at, FT)] * gains[net]
        return 0

    lax.fori_loop(0, n, turn, 0)
    ph("norm_ag_wait")
    nrm_ag.wait(nfull.at[pl.ds(0, n - 1)])

    ph("normalise")

    def normalise(j, _):
        at = pl.multiple_of(j * FT, FT)
        scales = nfull[j]
        tall = jnp.concatenate([scales] * 16, axis=0).T
        for net in range(2):
            sq = scales[net * 2 : net * 2 + 1, :]
            sk = tall[:, net * 2 + 1 : net * 2 + 2]
            qt[net, :, pl.ds(at, FT)] = (qraw[net, :, pl.ds(at, FT)] * sq).astype(bf16)
            kn[net, pl.ds(at, FT), :] = (ktok[net, pl.ds(at, FT), :] * sk).astype(bf16)
        return 0

    lax.fori_loop(0, n, normalise, 0)

    ph("attend")
    blocks = tokens // blk
    per = blk // FT

    def one_block(s, _):
        block = block_at(s, me, per, blocks)
        attend_block(block, blk, tokens, qt, kn, vt, m_s, o_s, s_s)
        for net in range(2):
            o = o_s[net]
            y = (o[0:64] / o[64:65]).astype(bf16)
            for r in range(per):
                tsend[block * per + r, net * 64 : (net + 1) * 64, :] = y[:, r * FT : (r + 1) * FT]
        for r in range(per):
            f = block * per + r

            @pl.when(f != me)
            def _():
                tl.to(tsend.at[f], trecv.at[me], f).start()

        return 0

    lax.fori_loop(0, blocks, one_block, 0)
    ph("t_wait")
    trecv[me] = tsend[me]
    tl.wait(trecv.at[pl.ds(0, n - 1)])

    ph("finish")

    def add_up(s, t):
        return t + trecv[s].astype(f32)

    vel = lax.fori_loop(0, n, add_up, jnp.zeros((128, FT), f32))
    x_own = xs[:, pl.ds(pl.multiple_of(me * FT, FT), FT)]
    base_r = mm(rmat[0], x_own)
    base_f = mm(rmat[1], x_own)
    vel_r = vel[0:64] + base_r[0:64] + base_r[64:128]
    vel_f = vel[64:128] + base_f[0:64] + base_f[64:128]
    noisy = x_own[0:64].astype(f32)
    pred_r = noisy - sc[0] * vel_r
    pred_f = noisy - sc[0] * vel_f
    gap = jnp.abs(gen_s[...].astype(f32) - pred_r)
    gsum = gap[0:8]
    for r in range(1, 8):
        gsum = gsum + gap[r * 8 : (r + 1) * 8]
    gapbuf[me] = gsum
    gl.all(lambda j: gapbuf.at[me], gapbuf.at[me])
    diff = pred_f - pred_r
    dmd_ref[0] = diff
    diff_b = diff.astype(bf16)

    ph("wg_mm")
    half = d // 2
    stride = 512

    def wg_part(h, dst):
        def body(g, _):
            at = pl.multiple_of(h * half + g * stride, stride)
            y = mm(diff_b, hid[:, pl.ds(at, stride)])
            for r in range(stride // 128):
                to = pl.multiple_of((g * (stride // 128) + r) * 64, 64)
                dst[pl.ds(to, 64), :] = y[:, r * 128 : (r + 1) * 128].astype(dst.dtype)
            return 0

        lax.fori_loop(0, half // stride, body, 0)

    wg_part(1 - core, wgive)
    w_pair.to(wgive, wtake, other).start()
    wg_part(core, wown)
    ph("w_pair")
    w_pair.wait(wtake)
    rows = wrecv.shape[1]

    def pair_sum(j, _):
        at = pl.ds(pl.multiple_of(j * rows, 16), rows)
        wsend[j] = (wown[at, :] + wtake[at, :].astype(f32)).astype(bf16)
        return 0

    lax.fori_loop(0, chips, pair_sum, 0)
    w_rs.mates(lambda j: wsend.at[j], wrecv.at[chip])
    wrecv[chip] = wsend[chip]
    ph("gap_wait")
    gl.wait(gapbuf.at[pl.ds(0, n - 1)])
    gap_all = jnp.sum(jnp.sum(gapbuf[...], axis=0), keepdims=True)
    inv = 1.0 / jnp.maximum(gap_all / (64.0 * tokens), gap_floor)
    dmd_ref[0] = dmd_ref[0] * inv
    ph("w_wait")
    w_rs.wait(wrecv.at[pl.ds(0, chips - 1)])

    def add_w(s, t):
        return t + wrecv[s].astype(f32)

    wsum = lax.fori_loop(0, chips, add_w, jnp.zeros((rows, 128), f32))
    zbuf[mz] = (wsum * (inv / math.sqrt(nz * tokens))).astype(bf16)
    ph("w_z")
    for i in range(1, nz):
        w_z.to(zbuf.at[mz], zbuf.at[mz], lax.rem(mz + i, nz), "batch").start()
    zview = zbuf.at[pl.ds(0, nz - 1)]
    zwait = w_z.to(zview, zview, lax.rem(mz + 1, nz), "batch")
    zwait.wait_recv()
    zwait.wait_send()
    whole = zbuf[0].astype(f32)
    for z in range(1, nz):
        whole = whole + zbuf[z].astype(f32)
    ph("w_ag")
    wg_ref[core, chip] = whole.astype(bf16)
    part = wg_ref.at[core, chip]
    w_ag.mates(lambda j: part, part)
    w_ag.wait(wg_ref.at[core, pl.ds(0, chips - 1)])
    ph("w_forward")
    w_fw.to(wg_ref.at[core], wg_ref.at[core], other).start()
    w_fw.wait(wg_ref.at[core])
    ph(None)


def per_device(
    hidden_states, gen_weight, noise_field, timesteps,
    embed_real, time_real, query_real, key_real, value_real, out_real, gain_real, proj_real,
    embed_fake, time_fake, query_fake, key_fake, value_fake, out_fake, gain_fake, proj_fake,
):
    n = lax.axis_size("tm")
    nz = lax.axis_size("batch")
    d = hidden_states.shape[2]
    tokens = n * FT
    blk = 512
    rows = 64 * d // 128 // n
    chips = n // 2
    fr = time_real.shape[0]
    step = timesteps[0].astype(f32)
    raw = step / 1000.0
    sigma = 5.0 * raw / (1.0 + 4.0 * raw)
    half = FREQ // 2
    at = lax.axis_index("tm") * fr + jnp.arange(fr, dtype=jnp.int32)
    freq = jnp.exp(-math.log(10000.0) * (at % half).astype(f32) / half)
    wave = jnp.where(at < half, jnp.cos(step * freq), jnp.sin(step * freq))
    wave = wave.astype(bf16).astype(f32)
    wave = jnp.broadcast_to(wave[:, None], (fr, 128))
    slot = jnp.arange(8)
    sc = jnp.where(slot == 0, sigma, jnp.where(slot == 1, 1.0 - sigma, 0.0))

    vm = pl.BlockSpec(memory_space=pltpu.VMEM)
    hbm = pl.BlockSpec(memory_space=pl.ANY)
    sems = pltpu.SemaphoreType.DMA
    scratch = [
        pltpu.VMEM((2, 3, fr, d), bf16),
        pltpu.VMEM((FT, d), bf16),
        pltpu.VMEM((64, d), bf16),
        pltpu.VMEM((2, 128, d), bf16),
        pltpu.VMEM((2, 64, d), bf16),
        pltpu.VMEM((2, 128, d), bf16),
        pltpu.VMEM((2, d, 256), bf16),
        pltpu.VMEM((2, d, 128), bf16),
        pltpu.VMEM((n, 8, 128), f32),
        pltpu.VMEM((n, 8, 128), f32),
        pltpu.VMEM((n, 8, 128), f32),
        pltpu.VMEM((chips, 2, 64, 128), bf16),
        pltpu.VMEM((128, tokens), bf16),
        pltpu.VMEM((64, 128), bf16),
        pltpu.VMEM((2, 128, 128), f32),
        pltpu.VMEM((2, 256, 128), bf16),
        pltpu.VMEM((2, 128, 128), bf16),
        pltpu.VMEM((2, 144, d), bf16),
        pltpu.VMEM((2, 144, 256), f32),
        pltpu.VMEM((2, 128, 1024), bf16),
        pltpu.VMEM((2, 128, 128), f32),
        pltpu.VMEM((2, 144, 128), f32),
        pltpu.VMEM((2, 8, tokens), f32),
        pltpu.VMEM((2, 128, tokens), f32),
        pltpu.VMEM((2, 128, tokens), f32),
        pltpu.VMEM((2, tokens, 128), f32),
        pltpu.VMEM((n, 8, 128), f32),
        pltpu.VMEM((n, 8, 128), f32),
        pltpu.VMEM((n, 8, 128), f32),
        pltpu.VMEM((2, 128, tokens), bf16),
        pltpu.VMEM((2, tokens, 128), bf16),
        pltpu.VMEM((2, 80, tokens), bf16),
        pltpu.VMEM((2, 8, blk), f32),
        pltpu.VMEM((2, 80, blk), f32),
        pltpu.VMEM((2, blk, blk), f32),
        pltpu.VMEM((n, 128, 128), bf16),
        pltpu.VMEM((n, 128, 128), bf16),
        pltpu.VMEM((n, 8, 128), f32),
        pltpu.VMEM((rows * chips, 128), f32),
        pltpu.VMEM((rows * chips, 128), bf16),
        pltpu.VMEM((rows * chips, 128), bf16),
        pltpu.VMEM((chips, rows, 128), bf16),
        pltpu.VMEM((chips, rows, 128), bf16),
        pltpu.VMEM((nz, rows, 128), bf16),
        sems((16,)),
        sems((26,)),
    ]
    dmd, wg = pl.pallas_call(
        functools.partial(kernel, n, nz, blk),
        out_shape=(
            jax.ShapeDtypeStruct((1, 64, FT), f32),
            jax.ShapeDtypeStruct((2, chips, rows, 128), bf16),
        ),
        in_specs=[pl.BlockSpec(memory_space=pltpu.SMEM)] + [vm] * 4 + [hbm] * 16,
        out_specs=(vm, vm),
        scratch_shapes=scratch,
        compiler_params=pltpu.CompilerParams(
            collective_id=0, has_side_effects=True, vmem_limit_bytes=62 * 1024 * 1024
        ),
        name="dmd",
    )(
        sc, wave, noise_field, gain_real, gain_fake,
        time_real.transpose(1, 0, 2), time_fake.transpose(1, 0, 2),
        hidden_states, gen_weight, embed_real, embed_fake, proj_real, proj_fake,
        out_real, out_fake,
        query_real, key_real, value_real, query_fake, key_fake, value_fake,
    )
    wg = wg.reshape(d // 128, 64, 128).transpose(1, 0, 2).reshape(64, d).astype(f32)
    return dmd, wg


def solution(mesh):
    in_specs = (
        P("batch", "tm", None), P(), P("batch", None, "tm"), P("batch"),
        P(), P("tm", None, None), P(None, "tm"), P(None, "tm"), P(None, "tm"),
        P("tm", None), P(None, "tm"), P(),
        P(), P("tm", None, None), P(None, "tm"), P(None, "tm"), P(None, "tm"),
        P("tm", None), P(None, "tm"), P(),
    )
    out_specs = (P("batch", None, "tm"), P())
    return jax.shard_map(
        per_device, mesh=mesh, in_specs=in_specs, out_specs=out_specs, check_vma=False
    )
```

```python
import functools
import math

import jax
import jax.numpy as jnp
from jax import lax
from jax.experimental import pallas as pl
from jax.experimental.pallas import tpu as pltpu
from jax.sharding import PartitionSpec as P

HD = 128
FREQ = 256
FT = 128
GS = 8
MESH = pl.DeviceIdType.MESH

norm_floor = 0.05
gap_floor = 0.25
highest = lax.Precision.HIGHEST
f32 = jnp.float32
bf16 = jnp.bfloat16


def split2(a):
    hi = a.astype(bf16)
    lo = (a - hi.astype(f32)).astype(bf16)
    return hi, lo


def stack2(a):
    hi, lo = split2(a)
    return jnp.concatenate([hi, lo], axis=0)


def mm(a, b):
    return jnp.dot(a, b, preferred_element_type=f32)


def mm_t(a, b):
    return lax.dot_general(a, b, (((1,), (1,)), ((), ())), preferred_element_type=f32)


class Phase:
    def __init__(self):
        self.now = None

    def __call__(self, name):
        if self.now is not None:
            self.now.__exit__(None, None, None)
        self.now = None
        if name:
            self.now = jax.named_scope(name)
            self.now.__enter__()


def attend_block(block, blk, tokens, qt_ref, k_ref, v_ref, m_ref, o_ref, s_ref):
    q_at = pl.multiple_of(block * blk, blk)
    frames = blk // FT

    def score(net, k_at):
        return mm(k_ref[net, pl.ds(k_at, blk), :], qt_ref[net, :, pl.ds(q_at, blk)])

    for net in range(2):
        s_ref[net] = score(net, 0)
    for net in range(2):
        s = score(net, q_at)
        rows = []
        for r in range(frames):
            part = s[r * FT : (r + 1) * FT]
            if r:
                gone = jnp.full((FT, r * FT), -1e30, f32)
                part = jnp.concatenate([gone, part[:, r * FT :]], axis=1)
            rows.append(part)
        s = jnp.concatenate(rows, axis=0)
        top = jnp.max(s, axis=0, keepdims=True)
        p = jnp.exp2(s - top).astype(bf16)
        m_ref[net] = jnp.broadcast_to(top, (8, blk))
        o_ref[net] = mm(v_ref[net, :, pl.ds(q_at, blk)], p)

    def step(kb, _):
        k_at = pl.multiple_of(kb * blk, blk)
        next_at = pl.multiple_of(jnp.minimum(kb + 1, tokens // blk - 1) * blk, blk)
        for net in range(2):
            s = s_ref[net]
            old = m_ref[net, 0:1, :]
            top = jnp.maximum(old, jnp.max(s, axis=0, keepdims=True))
            p = jnp.exp2(s - top).astype(bf16)
            ahead = score(net, next_at)
            fade = jnp.exp2(old - top)
            o_ref[net] = o_ref[net] * fade + mm(v_ref[net, :, pl.ds(k_at, blk)], p)
            m_ref[net] = jnp.broadcast_to(top, (8, blk))
            s_ref[net] = ahead
        return 0

    lax.fori_loop(0, block, step, 0)


def block_at(s, me, per, blocks):
    home = me // per
    if blocks != 8:
        return lax.rem(home + 1 + s, blocks)
    dx = jnp.where(s < 2, 2, jnp.where(s < 6, 1 + 2 * lax.rem(s - 2, 2), 0))
    dy = jnp.where(s < 2, 1 - s, jnp.where(s < 4, 1, jnp.where(s < 6, 0, 7 - s)))
    x = lax.rem(home // 2 + dx, 4)
    y = lax.rem(home + dy, 2)
    return x * 2 + y


def kernel(
    n, nz, blk,
    sc, wave, noise, gain_r, gain_f,
    time_rh, time_fh, hidden_h, genw_h, emb_rh, emb_fh, proj_rh, proj_fh, out_rh, out_fh,
    wq_r, wk_r, wv_r, wq_f, wk_f, wv_f,
    dmd_ref, wg_ref,
    times, hid, genw, emb, proj, outw, wqk, wv,
    modbuf, modin, modfull, xg, xs, gen_s, mu_s, gmat, rmat,
    lhs, acc, lhs2, acc2, accv, rs_s, qraw, kraw, nbuf, nin, nfull,
    qt, kn, vt, m_s, o_s, s_s,
    tsend, trecv, gapbuf, hcol, dcat, wsend, wrecv, zbuf,
    lsem, sem,
):
    me = lax.axis_index("tm")
    mz = lax.axis_index("batch")
    core = lax.rem(me, 2)
    chip = me // 2
    other = me + 1 - 2 * core
    chips = n // 2
    d = hid.shape[1]
    groups = d // 1024
    tokens = n * FT
    ph = Phase()
    loads = []

    def load(src, dst):
        c = pltpu.make_async_copy(src, dst, lsem.at[len(loads)])
        c.start()
        loads.append(c)
        return c

    ld_time = [load(time_rh, times.at[0]), load(time_fh, times.at[1])]
    ld_hid = load(hidden_h.at[0], hid)
    ld_gen = load(genw_h, genw)
    ld_emb = [load(emb_rh, emb.at[0]), load(emb_fh, emb.at[1])]
    ld_proj = [load(proj_rh, proj.at[0]), load(proj_fh, proj.at[1])]
    ld_qk = []
    for net, (a, b) in enumerate(((wq_r, wk_r), (wq_f, wk_f))):
        ld_qk.append(load(a, wqk.at[net, :, 0:HD]))
        ld_qk.append(load(b, wqk.at[net, :, HD : 2 * HD]))
    ld_v = [load(wv_r, wv.at[0]), load(wv_f, wv.at[1])]
    ld_out = [load(out_rh, outw.at[0]), load(out_fh, outw.at[1])]

    barrier = pltpu.get_barrier_semaphore()

    def greet(i, _):
        pl.semaphore_signal(
            barrier, inc=1, device_id={"tm": lax.rem(me + i, n)}, device_id_type=MESH
        )
        return 0

    lax.fori_loop(1, n, greet, 0)
    for i in range(1, nz):
        pl.semaphore_signal(
            barrier, inc=1, device_id={"batch": lax.rem(mz + i, nz)}, device_id_type=MESH
        )

    used = [0]

    class Lane:
        def __init__(self):
            self.send = sem.at[used[0]]
            self.recv = sem.at[used[0] + 1]
            used[0] += 2

        def to(self, src, dst, j, axis="tm"):
            return pltpu.make_async_remote_copy(
                src_ref=src, dst_ref=dst, send_sem=self.send, recv_sem=self.recv,
                device_id={axis: j}, device_id_type=MESH,
            )

        def all(self, src_of, dst):
            def body(i, _):
                j = lax.rem(me + i, n)
                self.to(src_of(j), dst, j).start()
                return 0

            lax.fori_loop(1, n, body, 0)

        def mates(self, src_of, dst):
            def body(i, _):
                j = lax.rem(chip + i, chips)
                self.to(src_of(j), dst, 2 * j + core).start()
                return 0

            lax.fori_loop(1, chips, body, 0)

        def wait(self, view):
            c = self.to(view, view, other)
            c.wait_recv()
            c.wait_send()

    mod_rs, mod_ag, xl, xf = Lane(), Lane(), Lane(), Lane()
    nrm_rs, nrm_ag, tl, gl = Lane(), Lane(), Lane(), Lane()
    hl, dl, w_rs, w_z, w_ag, w_fw = Lane(), Lane(), Lane(), Lane(), Lane(), Lane()
    member = lax.rem(me, GS)
    home = me - member
    gx = n // GS
    myx = me // GS

    ph("share")
    for p in range(6 * groups, n):
        modbuf[p] = jnp.zeros((8, 128), f32)
    for net in range(2):
        ld_time[net].wait()
        for c in range(3):
            for b in range(8 * groups):
                t = times[net, c, :, b * 128 : (b + 1) * 128].astype(f32)
                part = jnp.sum(t * wave[...], axis=0, keepdims=True)
                modbuf[(net * 3 + c) * groups + b // 8, b % 8 : b % 8 + 1, :] = part
    modin[me] = modbuf[me]

    ph("barrier")
    pl.semaphore_wait(barrier, n - 1 + nz - 1)
    mod_rs.all(lambda j: modbuf.at[j], modin.at[me])

    ph("generate")
    ld_hid.wait()
    ld_gen.wait()
    generated = mm_t(genw[...], hid[...]).astype(bf16)
    gen_s[...] = generated
    xg[chip, core] = (sc[1] * generated.astype(f32) + sc[0] * noise[0].astype(f32)).astype(bf16)
    mine = xg.at[chip, core]
    xl.mates(lambda j: mine, mine)

    ph("weights")
    ones_k = jnp.ones((1024, 128), bf16)
    for net in range(2):
        ld_emb[net].wait()
        ld_proj[net].wait()

        def gram(g, t):
            at = pl.multiple_of(g * 1024, 1024)
            e = emb[net, :, pl.ds(at, 1024)]
            return (
                t[0] + mm_t(e, e),
                t[1] + mm(e, ones_k),
                t[2] + mm_t(proj[net, :, pl.ds(at, 1024)], e),
            )

        zero = jnp.zeros((128, 128), f32)
        ee, mu, rr = lax.fori_loop(0, groups, gram, (zero, zero, jnp.zeros((64, 128), f32)))
        mu = mu / d
        mu_s[net] = mu
        gmat[net] = stack2(ee / d - mu * mu.T)
        rmat[net] = stack2(rr)

    ph("mod_rs")
    mod_rs.wait(modin.at[pl.ds(0, n - 1)])
    modfull[me] = jnp.sum(modin[...], axis=0)
    mod_ag.all(lambda j: modfull.at[me], modfull.at[me])

    ph("x_wait")
    xl.wait(xg.at[pl.ds(0, chips - 1), core])
    xf.to(xg.at[:, core], xg.at[:, core], other).start()
    xf.wait(xg.at[:, core])

    ph("place_var")

    def place(j, _):
        at = pl.multiple_of(j * FT, FT)
        xs[0:64, pl.ds(at, FT)] = xg[j // 2, lax.rem(j, 2)]
        return 0

    def place_late(j, _):
        at = pl.multiple_of(j * FT + FT, FT)
        xs[64:128, pl.ds(at, FT)] = xg[j // 2, lax.rem(j, 2)]
        return 0

    xs[64:128, 0:FT] = jnp.zeros((64, FT), bf16)
    lax.fori_loop(0, n, place, 0, unroll=8)
    lax.fori_loop(0, n - 1, place_late, 0, unroll=8)

    width = blk

    def variances(t, _):
        at = pl.multiple_of(t * width, width)
        x = xs[:, pl.ds(at, width)]
        for net in range(2):
            y = mm(gmat[net], x)
            var = jnp.sum((y[0:128] + y[128:256]) * x.astype(f32), axis=0, keepdims=True)
            rs = lax.rsqrt(jnp.maximum(var, 0.0) + norm_floor)
            rs_s[net, :, pl.ds(at, width)] = jnp.broadcast_to(rs, (8, width))
        return 0

    lax.fori_loop(0, tokens // width, variances, 0, unroll=2)
    for c in ld_qk:
        c.wait()
    ph("mod_ag_wait")
    mod_ag.wait(modfull.at[pl.ds(0, n - 1)])

    ph("qk_fold")
    row = lax.broadcasted_iota(jnp.int32, (16, 128), 0)
    acc[...] = jnp.zeros_like(acc)

    def fold(g, _):
        at = pl.multiple_of(g * 1024, 1024)
        for net in range(2):
            shift8 = modfull[(net * 3 + 0) * groups + g]
            scale8 = modfull[(net * 3 + 1) * groups + g]
            for r in range(8):
                col = pl.multiple_of(at + r * 128, 128)
                e = emb[net, :, pl.ds(col, 128)].astype(f32) - mu_s[net]
                lhs[net, 0:128, pl.ds(col, 128)] = (e * (1.0 + scale8[r : r + 1, :])).astype(bf16)
                sh, sl = split2(shift8[r : r + 1, :])
                tail = jnp.where(
                    row == 0, sh.astype(f32), jnp.where(row == 1, sl.astype(f32), 0.0)
                )
                lhs[net, 128:144, pl.ds(col, 128)] = tail.astype(bf16)
            acc[net] += mm(lhs[net, :, pl.ds(at, 1024)], wqk[net, pl.ds(at, 1024), :])
        return 0

    lax.fori_loop(0, groups, fold, 0)
    ph("qk_project")
    mats = []
    for net in range(2):
        off = acc[net, 128:129, :] + acc[net, 129:130, :]
        for which in range(2):
            cols = slice(which * HD, (which + 1) * HD)
            mat = acc[net, 0:128, cols].T.astype(bf16)
            mats.append((mat, jnp.broadcast_to(off[:, cols], (128, 128)).T[:, 0:1]))

    def project(t, _):
        at = pl.multiple_of(t * width, width)
        x = xs[:, pl.ds(at, width)]
        for net in range(2):
            rs = rs_s[net, 0:1, pl.ds(at, width)]
            for which, dst in enumerate((qraw, kraw)):
                mat, off_c = mats[net * 2 + which]
                y = mm(mat, x) * rs + off_c
                dst[net, :, pl.ds(at, width)] = y
                sq = jnp.sum(y * y, axis=0, keepdims=True)
                for r in range(width // FT):
                    nbuf[t * (width // FT) + r, net * 2 + which : net * 2 + which + 1, :] = sq[
                        :, r * FT : (r + 1) * FT
                    ]
        return 0

    lax.fori_loop(0, tokens // width, project, 0, unroll=2)

    ph("norm_send")
    nin[me] = nbuf[me]
    nrm_rs.all(lambda j: nbuf.at[j], nin.at[me])

    ph("v_fold")
    for c in ld_v + ld_out:
        c.wait()
    accv[...] = jnp.zeros_like(accv)
    acc2[...] = jnp.zeros_like(acc2)

    def fold_v(g, _):
        at = pl.multiple_of(g * 1024, 1024)
        for net in range(2):
            gate8 = modfull[(net * 3 + 2) * groups + g]
            for r in range(8):
                col = pl.multiple_of(at + r * 128, 128)
                gated = proj[net, :, pl.ds(col, 128)].astype(f32) * gate8[r : r + 1, :]
                hi, lo = split2(gated)
                lhs2[net, 0:64, r * 128 : (r + 1) * 128] = hi
                lhs2[net, 64:128, r * 128 : (r + 1) * 128] = lo
            accv[net] += mm(lhs[net, :, pl.ds(at, 1024)], wv[net, pl.ds(at, 1024), :])
            acc2[net] += mm_t(lhs2[net], outw[net, :, pl.ds(at, 1024)])
        return 0

    lax.fori_loop(0, groups, fold_v, 0)

    ph("norm_rs_wait")
    nrm_rs.wait(nin.at[pl.ds(0, n - 1)])
    nfull[me] = lax.rsqrt(jnp.sum(nin[...], axis=0) / float(n * HD) + norm_floor)
    nrm_ag.all(lambda j: nfull.at[me], nfull.at[me])

    ph("values")
    vmats = []
    for net in range(2):
        a = accv[net, 0:128, :]
        off = accv[net, 128:129, :] + accv[net, 129:130, :]
        out_t = acc2[net, 0:64, :] + acc2[net, 64:128, :]
        b_mat = stack2(
            lax.dot_general(
                out_t, a, (((1,), (1,)), ((), ())), precision=highest, preferred_element_type=f32
            )
        )
        vmats.append((b_mat, jnp.sum(out_t * off, axis=1, keepdims=True)))
    ones = jnp.where(lax.broadcasted_iota(jnp.int32, (16, width), 0) == 0, 1.0, 0.0)

    def values(t, _):
        at = pl.multiple_of(t * width, width)
        x = xs[:, pl.ds(at, width)]
        for net in range(2):
            y = mm(vmats[net][0], x)
            y = (y[0:64] + y[64:128]) * rs_s[net, 0:1, pl.ds(at, width)] + vmats[net][1]
            vt[net, 0:64, pl.ds(at, width)] = y.astype(bf16)
            vt[net, 64:80, pl.ds(at, width)] = ones.astype(bf16)
        return 0

    lax.fori_loop(0, tokens // width, values, 0, unroll=2)
    gains = []
    for gain in (gain_r, gain_f):
        both = gain[0:1, :] * gain[1:2, :] * (math.log2(math.e) / math.sqrt(HD))
        gains.append(jnp.broadcast_to(both, (128, 128)).T)
    same = lax.broadcasted_iota(jnp.int32, (256, 256), 0) == lax.broadcasted_iota(
        jnp.int32, (256, 256), 1
    )
    eye = jnp.where(same, 1.0, 0.0).astype(bf16)
    ph("norm_ag_wait")
    nrm_ag.wait(nfull.at[pl.ds(0, n - 1)])

    ph("normalise")

    def normalise(t, _):
        at = pl.multiple_of(t * 256, 256)
        k_rows = []
        for net in range(2):
            k_cols = []
            for half in range(2):
                scales = nfull[t * 2 + half]
                to = pl.ds(pl.multiple_of(at + half * FT, FT), FT)
                sq = scales[net * 2 : net * 2 + 1, :]
                sk = scales[net * 2 + 1 : net * 2 + 2, :]
                qt[net, :, to] = (qraw[net, :, to] * sq * gains[net]).astype(bf16)
                k_cols.append((kraw[net, :, to] * sk).astype(bf16))
            k_rows.append(jnp.concatenate(k_cols, axis=1))
        turned = mm_t(eye, jnp.concatenate(k_rows, axis=0)).astype(bf16)
        for net in range(2):
            kn[net, pl.ds(at, 256), :] = turned[:, net * HD : (net + 1) * HD]
        return 0

    lax.fori_loop(0, tokens // 256, normalise, 0, unroll=2)

    def share_cols(i, _):
        j = lax.rem(member + i, GS)
        src = hid.at[:, pl.ds(pl.multiple_of(j * hcol.shape[1], 128), hcol.shape[1])]
        hl.to(src, hcol.at[pl.ds(pl.multiple_of(member * FT, FT), FT), :], home + j).start()
        return 0

    lax.fori_loop(1, GS, share_cols, 0)
    hcol[pl.ds(pl.multiple_of(member * FT, FT), FT), :] = hid[
        :, pl.ds(pl.multiple_of(member * hcol.shape[1], 128), hcol.shape[1])
    ]

    ph("attend")
    blocks = tokens // blk
    per = blk // FT

    def one_block(s, _):
        block = block_at(s, me, per, blocks)
        attend_block(block, blk, tokens, qt, kn, vt, m_s, o_s, s_s)
        for net in range(2):
            o = o_s[net]
            y = (o[0:64] / o[64:65]).astype(bf16)
            for r in range(per):
                tsend[block * per + r, net * 64 : (net + 1) * 64, :] = y[:, r * FT : (r + 1) * FT]
        for r in range(per):
            f = block * per + r

            @pl.when(f != me)
            def _():
                tl.to(tsend.at[f], trecv.at[me], f).start()

        return 0

    lax.fori_loop(0, blocks, one_block, 0)
    ph("t_wait")
    x_own = xs[:, pl.ds(pl.multiple_of(me * FT, FT), FT)]
    base_r = mm(rmat[0], x_own)
    base_f = mm(rmat[1], x_own)
    noisy = x_own[0:64].astype(f32)
    trecv[me] = tsend[me]
    tl.wait(trecv.at[pl.ds(0, n - 1)])

    ph("finish")

    def add_up(s, t):
        return t + trecv[s].astype(f32)

    vel = lax.fori_loop(0, n, add_up, jnp.zeros((128, FT), f32), unroll=8)
    vel_r = vel[0:64] + base_r[0:64] + base_r[64:128]
    vel_f = vel[64:128] + base_f[0:64] + base_f[64:128]
    pred_r = noisy - sc[0] * vel_r
    pred_f = noisy - sc[0] * vel_f
    gap = jnp.abs(gen_s[...].astype(f32) - pred_r)
    gsum = gap[0:8]
    for r in range(1, 8):
        gsum = gsum + gap[r * 8 : (r + 1) * 8]
    gapbuf[me] = gsum
    diff = pred_f - pred_r
    own = dcat.at[:, pl.ds(pl.multiple_of(member * FT, FT), FT)]
    own[...] = diff.astype(bf16)

    def share_diff(i, _):
        dl.to(own, own, home + lax.rem(member + i, GS)).start()
        return 0

    lax.fori_loop(1, GS, share_diff, 0)
    gl.all(lambda j: gapbuf.at[me], gapbuf.at[me])
    dmd_ref[0] = diff
    ph("h_wait")
    hl.wait(hcol.at[pl.ds(0, (GS - 1) * FT), :])
    ph("d_wait")
    dl.wait(dcat.at[:, pl.ds(0, (GS - 1) * FT)])
    ph("wg_mm")
    wsend[...] = mm(dcat[...], hcol[...]).astype(bf16)
    rows = wrecv.shape[1]

    def x_rows(x):
        return pl.ds(pl.multiple_of(x * rows, 16), rows)

    for i in range(1, gx):
        x = lax.rem(myx + i, gx)
        w_rs.to(wsend.at[x_rows(x), :], wrecv.at[myx], x * GS + member).start()
    wrecv[myx] = wsend[x_rows(myx), :]
    ph("gap_wait")
    gl.wait(gapbuf.at[pl.ds(0, n - 1)])
    gap_all = jnp.sum(jnp.sum(gapbuf[...], axis=0), keepdims=True)
    inv = 1.0 / jnp.maximum(gap_all / (64.0 * tokens), gap_floor)
    dmd_ref[0] = dmd_ref[0] * inv
    ph("w_wait")
    if gx > 1:
        w_rs.wait(wrecv.at[pl.ds(0, gx - 1)])
    wsum = wrecv[0].astype(f32)
    for x in range(1, gx):
        wsum = wsum + wrecv[x].astype(f32)
    zbuf[mz] = (wsum * (inv / math.sqrt(nz * tokens))).astype(bf16)
    ph("w_z")
    for i in range(1, nz):
        w_z.to(zbuf.at[mz], zbuf.at[mz], lax.rem(mz + i, nz), "batch").start()
    if nz > 1:
        zview = zbuf.at[pl.ds(0, nz - 1)]
        zwait = w_z.to(zview, zview, lax.rem(mz + 1, nz), "batch")
        zwait.wait_recv()
        zwait.wait_send()
    whole = zbuf[0].astype(f32)
    for z in range(1, nz):
        whole = whole + zbuf[z].astype(f32)
    ph("w_ag")
    cols = wrecv.shape[2]

    def col(g):
        return pl.ds(pl.multiple_of(g * cols, 128), cols)

    part = wg_ref.at[x_rows(myx), col(member)]
    part[...] = whole.astype(bf16)
    w_ag.mates(lambda j: part, part)
    fold_by = next(k for k in range(1, chips) if (chips - 1) % k == 0 and (chips - 1) // k <= GS)
    w_ag.wait(wg_ref.at[pl.ds(0, fold_by * rows), pl.ds(0, (chips - 1) // fold_by * cols)])
    ph("w_forward")
    for y in range(GS // 2):
        view = wg_ref.at[:, col(2 * y + core)]
        w_fw.to(view, view, other).start()
    w_fw.wait(wg_ref.at[:, pl.ds(0, d // 2)])
    ph(None)


def per_device(
    hidden_states, gen_weight, noise_field, timesteps,
    embed_real, time_real, query_real, key_real, value_real, out_real, gain_real, proj_real,
    embed_fake, time_fake, query_fake, key_fake, value_fake, out_fake, gain_fake, proj_fake,
):
    n = lax.axis_size("tm")
    nz = lax.axis_size("batch")
    d = hidden_states.shape[2]
    tokens = n * FT
    blk = 512
    chips = n // 2
    gx = n // GS
    rows = 64 // gx
    cols = d // GS
    fr = time_real.shape[0]
    step = timesteps[0].astype(f32)
    raw = step / 1000.0
    sigma = 5.0 * raw / (1.0 + 4.0 * raw)
    half = FREQ // 2
    at = lax.axis_index("tm") * fr + jnp.arange(fr, dtype=jnp.int32)
    freq = jnp.exp(-math.log(10000.0) * (at % half).astype(f32) / half)
    wave = jnp.where(at < half, jnp.cos(step * freq), jnp.sin(step * freq))
    wave = wave.astype(bf16).astype(f32)
    wave = jnp.broadcast_to(wave[:, None], (fr, 128))
    slot = jnp.arange(8)
    sc = jnp.where(slot == 0, sigma, jnp.where(slot == 1, 1.0 - sigma, 0.0))

    vm = pl.BlockSpec(memory_space=pltpu.VMEM)
    hbm = pl.BlockSpec(memory_space=pl.ANY)
    sems = pltpu.SemaphoreType.DMA
    scratch = [
        pltpu.VMEM((2, 3, fr, d), bf16),
        pltpu.VMEM((FT, d), bf16),
        pltpu.VMEM((64, d), bf16),
        pltpu.VMEM((2, 128, d), bf16),
        pltpu.VMEM((2, 64, d), bf16),
        pltpu.VMEM((2, 128, d), bf16),
        pltpu.VMEM((2, d, 256), bf16),
        pltpu.VMEM((2, d, 128), bf16),
        pltpu.VMEM((n, 8, 128), f32),
        pltpu.VMEM((n, 8, 128), f32),
        pltpu.VMEM((n, 8, 128), f32),
        pltpu.VMEM((chips, 2, 64, 128), bf16),
        pltpu.VMEM((128, tokens), bf16),
        pltpu.VMEM((64, 128), bf16),
        pltpu.VMEM((2, 128, 128), f32),
        pltpu.VMEM((2, 256, 128), bf16),
        pltpu.VMEM((2, 128, 128), bf16),
        pltpu.VMEM((2, 144, d), bf16),
        pltpu.VMEM((2, 144, 256), f32),
        pltpu.VMEM((2, 128, 1024), bf16),
        pltpu.VMEM((2, 128, 128), f32),
        pltpu.VMEM((2, 144, 128), f32),
        pltpu.VMEM((2, 8, tokens), f32),
        pltpu.VMEM((2, 128, tokens), f32),
        pltpu.VMEM((2, 128, tokens), f32),
        pltpu.VMEM((n, 8, 128), f32),
        pltpu.VMEM((n, 8, 128), f32),
        pltpu.VMEM((n, 8, 128), f32),
        pltpu.VMEM((2, 128, tokens), bf16),
        pltpu.VMEM((2, tokens, 128), bf16),
        pltpu.VMEM((2, 80, tokens), bf16),
        pltpu.VMEM((2, 8, blk), f32),
        pltpu.VMEM((2, 80, blk), f32),
        pltpu.VMEM((2, blk, blk), f32),
        pltpu.VMEM((n, 128, 128), bf16),
        pltpu.VMEM((n, 128, 128), bf16),
        pltpu.VMEM((n, 8, 128), f32),
        pltpu.VMEM((GS * FT, cols), bf16),
        pltpu.VMEM((64, GS * FT), bf16),
        pltpu.VMEM((64, cols), bf16),
        pltpu.VMEM((gx, rows, cols), bf16),
        pltpu.VMEM((nz, rows, cols), bf16),
        sems((16,)),
        sems((28,)),
    ]
    dmd, wg = pl.pallas_call(
        functools.partial(kernel, n, nz, blk),
        out_shape=(
            jax.ShapeDtypeStruct((1, 64, FT), f32),
            jax.ShapeDtypeStruct((64, d), bf16),
        ),
        in_specs=[pl.BlockSpec(memory_space=pltpu.SMEM)] + [vm] * 4 + [hbm] * 16,
        out_specs=(vm, vm),
        scratch_shapes=scratch,
        compiler_params=pltpu.CompilerParams(
            collective_id=0, has_side_effects=True, vmem_limit_bytes=62 * 1024 * 1024
        ),
        name="dmd",
    )(
        sc, wave, noise_field, gain_real, gain_fake,
        time_real.transpose(1, 0, 2), time_fake.transpose(1, 0, 2),
        hidden_states, gen_weight, embed_real, embed_fake, proj_real, proj_fake,
        out_real, out_fake,
        query_real, key_real, value_real, query_fake, key_fake, value_fake,
    )
    return dmd, wg.astype(f32)


def solution(mesh):
    in_specs = (
        P("batch", "tm", None), P(), P("batch", None, "tm"), P("batch"),
        P(), P("tm", None, None), P(None, "tm"), P(None, "tm"), P(None, "tm"),
        P("tm", None), P(None, "tm"), P(),
        P(), P("tm", None, None), P(None, "tm"), P(None, "tm"), P(None, "tm"),
        P("tm", None), P(None, "tm"), P(),
    )
    out_specs = (P("batch", None, "tm"), P())
    return jax.shard_map(
        per_device, mesh=mesh, in_specs=in_specs, out_specs=out_specs, check_vma=False
    )
```

```python
import functools
import math

import jax
import jax.numpy as jnp
from jax import lax
from jax.experimental import pallas as pl
from jax.experimental.pallas import tpu as pltpu
from jax.sharding import PartitionSpec as P

HD = 128
FREQ = 256
FT = 128
GS = 8
MESH = pl.DeviceIdType.MESH

norm_floor = 0.05
gap_floor = 0.25
highest = lax.Precision.HIGHEST
f32 = jnp.float32
bf16 = jnp.bfloat16


def split2(a):
    hi = a.astype(bf16)
    lo = (a - hi.astype(f32)).astype(bf16)
    return hi, lo


def stack2(a):
    hi, lo = split2(a)
    return jnp.concatenate([hi, lo], axis=0)


def mm(a, b):
    return jnp.dot(a, b, preferred_element_type=f32)


def mm_t(a, b):
    return lax.dot_general(a, b, (((1,), (1,)), ((), ())), preferred_element_type=f32)


class Phase:
    def __init__(self):
        self.now = None

    def __call__(self, name):
        if self.now is not None:
            self.now.__exit__(None, None, None)
        self.now = None
        if name:
            self.now = jax.named_scope(name)
            self.now.__enter__()


def attend_block(block, later, blk, qt_ref, k_ref, v_ref, m_ref, o_ref, s_ref):
    frames = blk // FT

    def score(net, k_block, q_block):
        k_at = pl.multiple_of(k_block * blk, blk)
        q_at = pl.multiple_of(q_block * blk, blk)
        return mm(k_ref[net, pl.ds(k_at, blk), :], qt_ref[net, :, pl.ds(q_at, blk)])

    if later is None:
        for net in range(2):
            s_ref[net] = score(net, block, block)
        return

    def advance(kb, last, first):
        next_k = jnp.where(last, later, 0 if first else kb + 1)
        next_q = jnp.where(last, later, block)
        k_at = pl.multiple_of(kb * blk, blk)
        for net in range(2):
            s = s_ref[net]
            if first:
                rows = []
                for r in range(frames):
                    part = s[r * FT : (r + 1) * FT]
                    if r:
                        gone = jnp.full((FT, r * FT), -1e30, f32)
                        part = jnp.concatenate([gone, part[:, r * FT :]], axis=1)
                    rows.append(part)
                s = jnp.concatenate(rows, axis=0)
            top = jnp.max(s, axis=0, keepdims=True)
            if not first:
                old = m_ref[net, 0:1, :]
                top = jnp.maximum(old, top)
            p = jnp.exp2(s - top).astype(bf16)
            s_ref[net] = score(net, next_k, next_q)
            o = mm(v_ref[net, :, pl.ds(k_at, blk)], p)
            if not first:
                o = o_ref[net] * jnp.exp2(old - top) + o
            o_ref[net] = o
            m_ref[net] = jnp.broadcast_to(top, (8, blk))

    advance(block, block == 0, True)

    def pair(i, _):
        for u in range(2):
            kb = i * 2 + u
            advance(kb, kb == block - 1, False)
        return 0

    def single(kb, _):
        advance(kb, kb == block - 1, False)
        return 0

    lax.fori_loop(0, block // 2, pair, 0)
    lax.fori_loop(block // 2 * 2, block, single, 0)


def block_at(s, me, per, blocks):
    home = me // per
    if blocks != 8:
        return lax.rem(home + 1 + s, blocks)
    dx = jnp.where(s < 2, 2, jnp.where(s < 6, 1 + 2 * lax.rem(s - 2, 2), 0))
    dy = jnp.where(s < 2, 1 - s, jnp.where(s < 4, 1, jnp.where(s < 6, 0, 7 - s)))
    x = lax.rem(home // 2 + dx, 4)
    y = lax.rem(home + dy, 2)
    return x * 2 + y


def kernel(
    n, nz, blk,
    step_ref,
    noise_h, gain_rh, gain_fh, time_rh, time_fh, hidden_h, genw_h, emb_rh, emb_fh, proj_rh, proj_fh, out_rh, out_fh,
    wq_r, wk_r, wv_r, wq_f, wk_f, wv_f,
    dmd_ref, wg_ref,
    noise, gain, times, hid, genw, emb, proj, outw, wqk, wv,
    modbuf, modout, modin, modall, modfull, xg, xs, gen_s, mu_s, gmat, rmat,
    lhs, acc, lhs2, acc2, accv, rs_s, qraw, kraw, nbuf, nin, nfull,
    qt, kn, vt, m_s, o_s, s_s,
    tsend, trecv, gapbuf, hcol, dcat, wsend, wrecv, zbuf,
    lsem, sem,
):
    me = lax.axis_index("tm")
    mz = lax.axis_index("batch")
    core = lax.rem(me, 2)
    chip = me // 2
    other = me + 1 - 2 * core
    chips = n // 2
    d = hid.shape[1]
    groups = d // 1024
    tokens = n * FT
    ph = Phase()
    loads = []

    def load(src, dst):
        c = pltpu.make_async_copy(src, dst, lsem.at[len(loads)])
        c.start()
        loads.append(c)
        return c

    ld_time = [load(time_rh, times.at[0]), load(time_fh, times.at[1])]
    ld_noise = load(noise_h.at[0], noise)
    ld_hid = load(hidden_h.at[0], hid)
    ld_gen = load(genw_h, genw)
    ld_emb = [load(emb_rh, emb.at[0]), load(emb_fh, emb.at[1])]
    ld_proj = [load(proj_rh, proj.at[0]), load(proj_fh, proj.at[1])]
    ld_qk = []
    for net, (a, b) in enumerate(((wq_r, wk_r), (wq_f, wk_f))):
        ld_qk.append(load(a, wqk.at[net, :, 0:HD]))
        ld_qk.append(load(b, wqk.at[net, :, HD : 2 * HD]))
    ld_v = [load(wv_r, wv.at[0]), load(wv_f, wv.at[1])]
    ld_out = [load(out_rh, outw.at[0]), load(out_fh, outw.at[1])]

    ld_gain = [load(gain_rh, gain.at[0]), load(gain_fh, gain.at[1])]

    barrier = pltpu.get_barrier_semaphore()

    def greet(i, _):
        pl.semaphore_signal(
            barrier, inc=1, device_id={"tm": lax.rem(me + i, n)}, device_id_type=MESH
        )
        return 0

    lax.fori_loop(1, n, greet, 0)
    for i in range(1, nz):
        pl.semaphore_signal(
            barrier, inc=1, device_id={"batch": lax.rem(mz + i, nz)}, device_id_type=MESH
        )

    used = [0]

    class Lane:
        def __init__(self):
            self.send = sem.at[used[0]]
            self.recv = sem.at[used[0] + 1]
            used[0] += 2

        def to(self, src, dst, j, axis="tm"):
            return pltpu.make_async_remote_copy(
                src_ref=src, dst_ref=dst, send_sem=self.send, recv_sem=self.recv,
                device_id={axis: j}, device_id_type=MESH,
            )

        def all(self, src_of, dst):
            def body(i, _):
                j = lax.rem(me + i, n)
                self.to(src_of(j), dst, j).start()
                return 0

            lax.fori_loop(1, n, body, 0)

        def mates(self, src_of, dst):
            def body(i, _):
                j = lax.rem(chip + i, chips)
                self.to(src_of(j), dst, 2 * j + core).start()
                return 0

            lax.fori_loop(1, chips, body, 0)

        def wait(self, view):
            c = self.to(view, view, other)
            c.wait_recv()
            c.wait_send()

        def owners(self, src_of, dst, count):
            def body(i, _):
                j = lax.rem(chip + i, chips)

                @pl.when(jnp.logical_and(j < count, 2 * j + 1 != me))
                def _():
                    self.to(src_of(j), dst, 2 * j + 1).start()

                return 0

            lax.fori_loop(0, chips, body, 0)

        def to_owner(self, whole, count, then):
            owner = jnp.logical_and(core == 1, chip < count)

            @pl.when(owner)
            def _():
                self.to(whole, whole, other).wait_recv()
                then()

                def body(i, _):
                    j = lax.rem(me + i, n)
                    self.back.to(self.result, self.result, j).start()
                    return 0

                lax.fori_loop(1, n, body, 0)

            return owner

        def settle(self, owner, sent, fewer):
            @pl.when(owner)
            def _():
                self.to(fewer, fewer, other).wait_send()

            @pl.when(jnp.logical_not(owner))
            def _():
                self.to(sent, sent, other).wait_send()

        def gather(self, owner, whole, all_in, fewer):
            @pl.when(owner)
            def _():
                self.to(whole, whole, other).wait_send()
                self.to(fewer, fewer, other).wait_recv()

            @pl.when(jnp.logical_not(owner))
            def _():
                self.to(all_in, all_in, other).wait_recv()

    pieces = (6 * groups + 1) // 2
    mod_rs, mod_ag, xl, xf = Lane(), Lane(), Lane(), Lane()
    nrm_rs, nrm_ag, tl, gl = Lane(), Lane(), Lane(), Lane()
    hl, dl, w_rs, w_z, w_ag, w_fw = Lane(), Lane(), Lane(), Lane(), Lane(), Lane()
    gy = GS // 2
    half_d = d // 2
    slot = pl.ds(pl.multiple_of(core * FT, FT), FT)

    def half_of(c):
        return pl.ds(pl.multiple_of(c * half_d, 128), half_d)


    ph("share")
    step = jnp.full((1, 128), step_ref[0], jnp.int32).astype(f32)
    raw = step / 1000.0
    sigma = 5.0 * raw / (1.0 + 4.0 * raw)
    freqs = times.shape[2]
    first = me * freqs + lax.broadcasted_iota(jnp.int32, (freqs, 128), 0)
    k = lax.rem(first, FREQ // 2).astype(f32)
    angle = step * jnp.exp(k * (-math.log(10000.0) / (FREQ // 2)))
    turns = jnp.floor(angle * (0.5 / math.pi) + 0.5)
    angle = (angle - turns * 6.28125) - turns * (2.0 * math.pi - 6.28125)
    wave = jnp.where(first < FREQ // 2, jnp.cos(angle), jnp.sin(angle)).astype(bf16).astype(f32)
    for p in range(6 * groups, 2 * pieces):
        modbuf[p] = jnp.zeros((8, 128), f32)
    for net in range(2):
        ld_time[net].wait()
        for c in range(3):
            for b in range(8 * groups):
                t = times[net, c, :, b * 128 : (b + 1) * 128].astype(f32)
                part = jnp.sum(t * wave, axis=0, keepdims=True)
                modbuf[(net * 3 + c) * groups + b // 8, b % 8 : b % 8 + 1, :] = part
    for j in range(pieces):
        pair = jnp.concatenate([modbuf[2 * j], modbuf[2 * j + 1]], axis=0)
        modout[j] = pair.astype(bf16)
    ph("barrier")
    pl.semaphore_wait(barrier, n - 1 + nz - 1)
    mod_rs.owners(lambda j: modout.at[j], modin.at[me], pieces)

    ph("generate")
    ld_hid.wait()
    ld_gen.wait()
    generated = mm_t(genw[...], hid[...]).astype(bf16)
    gen_s[...] = generated
    ld_noise.wait()
    mixed = (1.0 - sigma) * generated.astype(f32) + sigma * noise[...].astype(f32)
    xg[chip, core] = mixed.astype(bf16)
    mine = xg.at[chip, core]
    xl.mates(lambda j: mine, mine)

    ph("weights")
    ones_k = jnp.ones((1024, 128), bf16)

    def weight_terms(net):
        ld_emb[net].wait()
        ld_proj[net].wait()

        def gram(g, t):
            at = pl.multiple_of(g * 1024, 1024)
            e = emb[net, :, pl.ds(at, 1024)]
            return (
                t[0] + mm_t(e, e),
                t[1] + mm(e, ones_k),
                t[2] + mm_t(proj[net, :, pl.ds(at, 1024)], e),
            )

        zero = jnp.zeros((128, 128), f32)
        ee, mu, rr = lax.fori_loop(0, groups, gram, (zero, zero, jnp.zeros((64, 128), f32)))
        mu = mu / d
        mu_s[net] = mu
        gmat[net] = stack2(ee / d - mu * mu.T)
        rmat[net] = stack2(rr)

    weight_terms(0)
    ph("mod_rs")

    def add_mod():
        modin[me] = modout[chip]
        total = modin[0].astype(f32)
        for j in range(1, n):
            total = total + modin[j].astype(f32)
        modall[chip] = total.astype(bf16)

    mod_rs.back, mod_rs.result = mod_ag, modall.at[chip]
    mod_owner = mod_rs.to_owner(modin.at[pl.ds(0, n - 1)], pieces, add_mod)
    mod_rs.settle(mod_owner, modout.at[pl.ds(0, pieces)], modout.at[pl.ds(0, pieces - 1)])
    hl.to(hid.at[:, half_of(1 - core)], hcol.at[slot, :], other).start()

    ph("x_wait")
    xl.wait(xg.at[pl.ds(0, chips - 1), core])
    xf.to(xg.at[:, core], xg.at[:, core], other).start()
    ph("weights1")
    weight_terms(1)
    hcol[slot, :] = hid[:, half_of(core)]
    ph("x_fwait")
    xf.wait(xg.at[:, core])

    ph("place_var")

    def place(j, _):
        at = pl.multiple_of(j * FT, FT)
        xs[0:64, pl.ds(at, FT)] = xg[j // 2, lax.rem(j, 2)]
        return 0

    def place_late(j, _):
        at = pl.multiple_of(j * FT + FT, FT)
        xs[64:128, pl.ds(at, FT)] = xg[j // 2, lax.rem(j, 2)]
        return 0

    xs[64:128, 0:FT] = jnp.zeros((64, FT), bf16)
    lax.fori_loop(0, n, place, 0, unroll=8)
    lax.fori_loop(0, n - 1, place_late, 0, unroll=8)

    width = blk

    def variances(t, _):
        at = pl.multiple_of(t * width, width)
        x = xs[:, pl.ds(at, width)]
        for net in range(2):
            y = mm(gmat[net], x)
            var = jnp.sum((y[0:128] + y[128:256]) * x.astype(f32), axis=0, keepdims=True)
            rs = lax.rsqrt(jnp.maximum(var, 0.0) + norm_floor)
            rs_s[net, :, pl.ds(at, width)] = jnp.broadcast_to(rs, (8, width))
        return 0

    lax.fori_loop(0, tokens // width, variances, 0, unroll=2)
    for c in ld_qk:
        c.wait()
    ph("mod_ag_wait")
    mod_ag.gather(
        mod_owner, modin.at[pl.ds(0, n - 1)], modall.at[pl.ds(0, pieces)],
        modall.at[pl.ds(0, pieces - 1)],
    )
    for j in range(pieces):
        both = modall[j].astype(f32)
        modfull[2 * j] = both[0:8]
        modfull[2 * j + 1] = both[8:16]

    ph("qk_fold")
    row = lax.broadcasted_iota(jnp.int32, (16, 128), 0)
    acc[...] = jnp.zeros_like(acc)

    def fold(g, _):
        at = pl.multiple_of(g * 1024, 1024)
        for net in range(2):
            shift8 = modfull[(net * 3 + 0) * groups + g]
            scale8 = modfull[(net * 3 + 1) * groups + g]
            for r in range(8):
                col = pl.multiple_of(at + r * 128, 128)
                e = emb[net, :, pl.ds(col, 128)].astype(f32) - mu_s[net]
                lhs[net, 0:128, pl.ds(col, 128)] = (e * (1.0 + scale8[r : r + 1, :])).astype(bf16)
                sh, sl = split2(shift8[r : r + 1, :])
                tail = jnp.where(
                    row == 0, sh.astype(f32), jnp.where(row == 1, sl.astype(f32), 0.0)
                )
                lhs[net, 128:144, pl.ds(col, 128)] = tail.astype(bf16)
            acc[net] += mm(lhs[net, :, pl.ds(at, 1024)], wqk[net, pl.ds(at, 1024), :])
        return 0

    lax.fori_loop(0, groups, fold, 0)
    ph("qk_project")
    mats = []
    for net in range(2):
        off = acc[net, 128:129, :] + acc[net, 129:130, :]
        for which in range(2):
            cols = slice(which * HD, (which + 1) * HD)
            mat = acc[net, 0:128, cols].T.astype(bf16)
            mats.append((mat, jnp.broadcast_to(off[:, cols], (128, 128)).T[:, 0:1]))

    def project(t, _):
        at = pl.multiple_of(t * width, width)
        x = xs[:, pl.ds(at, width)]
        for net in range(2):
            rs = rs_s[net, 0:1, pl.ds(at, width)]
            for which, dst in enumerate((qraw, kraw)):
                mat, off_c = mats[net * 2 + which]
                y = mm(mat, x) * rs + off_c
                dst[net, :, pl.ds(at, width)] = y
                sq = jnp.sum(y * y, axis=0, keepdims=True)
                for r in range(width // FT):
                    row = (r % 2) * 4 + net * 2 + which
                    nbuf[t * (width // FT // 2) + r // 2, row : row + 1, :] = sq[
                        :, r * FT : (r + 1) * FT
                    ]
        return 0

    lax.fori_loop(0, tokens // width, project, 0, unroll=2)

    ph("norm_send")
    nrm_rs.owners(lambda j: nbuf.at[j], nin.at[me], chips)

    ph("v_fold")
    for c in ld_v + ld_out:
        c.wait()
    accv[...] = jnp.zeros_like(accv)
    acc2[...] = jnp.zeros_like(acc2)

    def fold_v(g, _):
        at = pl.multiple_of(g * 1024, 1024)
        for net in range(2):
            gate8 = modfull[(net * 3 + 2) * groups + g]
            for r in range(8):
                col = pl.multiple_of(at + r * 128, 128)
                gated = proj[net, :, pl.ds(col, 128)].astype(f32) * gate8[r : r + 1, :]
                hi, lo = split2(gated)
                lhs2[net, 0:64, r * 128 : (r + 1) * 128] = hi
                lhs2[net, 64:128, r * 128 : (r + 1) * 128] = lo
            accv[net] += mm(lhs[net, :, pl.ds(at, 1024)], wv[net, pl.ds(at, 1024), :])
            acc2[net] += mm_t(lhs2[net], outw[net, :, pl.ds(at, 1024)])
        return 0

    lax.fori_loop(0, groups, fold_v, 0)

    ph("norm_rs_wait")

    def add_norm():
        nin[me] = nbuf[chip]
        nfull[chip] = lax.rsqrt(jnp.sum(nin[...], axis=0) / float(n * HD) + norm_floor)

    nrm_rs.back, nrm_rs.result = nrm_ag, nfull.at[chip]
    nrm_owner = nrm_rs.to_owner(nin.at[pl.ds(0, n - 1)], chips, add_norm)
    nrm_rs.settle(nrm_owner, nbuf.at[pl.ds(0, chips)], nbuf.at[pl.ds(0, chips - 1)])

    ph("values")
    vmats = []
    for net in range(2):
        a = accv[net, 0:128, :]
        off = accv[net, 128:129, :] + accv[net, 129:130, :]
        out_t = acc2[net, 0:64, :] + acc2[net, 64:128, :]
        b_mat = stack2(
            lax.dot_general(
                out_t, a, (((1,), (1,)), ((), ())), precision=highest, preferred_element_type=f32
            )
        )
        vmats.append((b_mat, jnp.sum(out_t * off, axis=1, keepdims=True)))
    ones = jnp.where(lax.broadcasted_iota(jnp.int32, (16, width), 0) == 0, 1.0, 0.0)

    def values(t, _):
        at = pl.multiple_of(t * width, width)
        x = xs[:, pl.ds(at, width)]
        for net in range(2):
            y = mm(vmats[net][0], x)
            y = (y[0:64] + y[64:128]) * rs_s[net, 0:1, pl.ds(at, width)] + vmats[net][1]
            vt[net, 0:64, pl.ds(at, width)] = y.astype(bf16)
            vt[net, 64:80, pl.ds(at, width)] = ones.astype(bf16)
        return 0

    lax.fori_loop(0, tokens // width, values, 0, unroll=2)
    gains = []
    for net in range(2):
        ld_gain[net].wait()
        both = gain[net, 0:1, :] * gain[net, 1:2, :] * (math.log2(math.e) / math.sqrt(HD))
        gains.append(jnp.broadcast_to(both, (128, 128)).T)

    def gained(t, _):
        at = pl.multiple_of(t * FT, FT)
        for net in range(2):
            qraw[net, :, pl.ds(at, FT)] = qraw[net, :, pl.ds(at, FT)] * gains[net]
        return 0

    lax.fori_loop(0, n, gained, 0, unroll=4)
    same = lax.broadcasted_iota(jnp.int32, (256, 256), 0) == lax.broadcasted_iota(
        jnp.int32, (256, 256), 1
    )
    eye = jnp.where(same, 1.0, 0.0).astype(bf16)
    ph("norm_ag_wait")
    nrm_ag.gather(
        nrm_owner, nin.at[pl.ds(0, n - 1)], nfull.at[pl.ds(0, chips)],
        nfull.at[pl.ds(0, chips - 1)],
    )

    ph("normalise")

    def normalise(t, _):
        at = pl.multiple_of(t * 256, 256)
        k_rows = []
        for net in range(2):
            k_cols = []
            for half in range(2):
                scales = nfull[t]
                to = pl.ds(pl.multiple_of(at + half * FT, FT), FT)
                at_row = half * 4 + net * 2
                sq = scales[at_row : at_row + 1, :]
                sk = scales[at_row + 1 : at_row + 2, :]
                qt[net, :, to] = (qraw[net, :, to] * sq).astype(bf16)
                k_cols.append((kraw[net, :, to] * sk).astype(bf16))
            k_rows.append(jnp.concatenate(k_cols, axis=1))
        turned = mm_t(eye, jnp.concatenate(k_rows, axis=0)).astype(bf16)
        for net in range(2):
            kn[net, pl.ds(at, 256), :] = turned[:, net * HD : (net + 1) * HD]
        return 0

    lax.fori_loop(0, tokens // 256, normalise, 0, unroll=4)

    ph("attend")
    blocks = tokens // blk
    per = blk // FT

    def one_block(s, _):
        block = block_at(s, me, per, blocks)
        later = block_at(lax.rem(s + 1, blocks), me, per, blocks)
        attend_block(block, later, blk, qt, kn, vt, m_s, o_s, s_s)
        for net in range(2):
            o = o_s[net]
            y = (o[0:64] / o[64:65]).astype(bf16)
            for r in range(per):
                tsend[block * per + r, net * 64 : (net + 1) * 64, :] = y[:, r * FT : (r + 1) * FT]
        for r in range(per):
            f = block * per + r

            @pl.when(f != me)
            def _():
                tl.to(tsend.at[f], trecv.at[me], f).start()

        return 0

    attend_block(block_at(0, me, per, blocks), None, blk, qt, kn, vt, m_s, o_s, s_s)
    lax.fori_loop(0, blocks, one_block, 0)
    ph("t_wait")
    x_own = xs[:, pl.ds(pl.multiple_of(me * FT, FT), FT)]
    base_r = mm(rmat[0], x_own)
    base_f = mm(rmat[1], x_own)
    noisy = x_own[0:64].astype(f32)
    trecv[me] = tsend[me]
    tl.wait(trecv.at[pl.ds(0, n - 1)])

    ph("finish")

    def add_up(s, t):
        return t + trecv[s].astype(f32)

    vel = lax.fori_loop(0, n, add_up, jnp.zeros((128, FT), f32), unroll=8)
    vel_r = vel[0:64] + base_r[0:64] + base_r[64:128]
    vel_f = vel[64:128] + base_f[0:64] + base_f[64:128]
    pred_r = noisy - sigma * vel_r
    pred_f = noisy - sigma * vel_f
    gap = jnp.abs(gen_s[...].astype(f32) - pred_r)
    gsum = gap[0:8]
    for r in range(1, 8):
        gsum = gsum + gap[r * 8 : (r + 1) * 8]
    gapbuf[me] = gsum
    diff = pred_f - pred_r
    own = dcat.at[:, slot]
    own[...] = diff.astype(bf16)
    dl.to(own, own, other).start()
    gl.all(lambda j: gapbuf.at[me], gapbuf.at[me])
    dmd_ref[0] = diff
    ph("h_wait")
    hl.wait(hcol.at[pl.ds(0, FT), :])
    ph("d_wait")
    dl.wait(dcat.at[:, pl.ds(0, FT)])
    ph("wg_mm")
    wsend[...] = mm(dcat[...], hcol[...]).astype(bf16)
    rows = wrecv.shape[1]
    cols = wrecv.shape[2]

    def piece(j, c):
        return (
            pl.ds(pl.multiple_of(j // gy * rows, 16), rows),
            pl.ds(pl.multiple_of(c * half_d + lax.rem(j, gy) * cols, 128), cols),
        )

    w_rs.mates(lambda j: wsend.at[piece(j, 0)], wrecv.at[chip])
    wrecv[chip] = wsend[piece(chip, 0)]
    ph("gap_wait")
    gl.wait(gapbuf.at[pl.ds(0, n - 1)])
    gap_all = jnp.sum(jnp.sum(gapbuf[...], axis=0), keepdims=True)
    inv = 1.0 / jnp.maximum(gap_all / (64.0 * tokens), gap_floor)
    dmd_ref[0] = dmd_ref[0] * inv
    ph("w_wait")
    w_rs.wait(wrecv.at[pl.ds(0, chips - 1)])
    wsum = wrecv[0].astype(f32)
    for j in range(1, chips):
        wsum = wsum + wrecv[j].astype(f32)
    zbuf[mz] = (wsum * (inv / math.sqrt(nz * tokens))).astype(bf16)
    ph("w_z")
    for i in range(1, nz):
        w_z.to(zbuf.at[mz], zbuf.at[mz], lax.rem(mz + i, nz), "batch").start()
    if nz > 1:
        zview = zbuf.at[pl.ds(0, nz - 1)]
        zwait = w_z.to(zview, zview, lax.rem(mz + 1, nz), "batch")
        zwait.wait_recv()
        zwait.wait_send()
    whole = zbuf[0].astype(f32)
    for z in range(1, nz):
        whole = whole + zbuf[z].astype(f32)
    ph("w_ag")
    part = wg_ref.at[piece(chip, core)]
    part[...] = whole.astype(bf16)
    w_ag.mates(lambda j: part, part)
    w_ag.wait(wrecv.at[pl.ds(0, chips - 1)])
    ph("w_forward")
    mine_half = wg_ref.at[:, half_of(core)]
    w_fw.to(mine_half, mine_half, other).start()
    w_fw.wait(mine_half)
    ph(None)


def per_device(
    hidden_states, gen_weight, noise_field, timesteps,
    embed_real, time_real, query_real, key_real, value_real, out_real, gain_real, proj_real,
    embed_fake, time_fake, query_fake, key_fake, value_fake, out_fake, gain_fake, proj_fake,
):
    n = lax.axis_size("tm")
    nz = lax.axis_size("batch")
    d = hidden_states.shape[2]
    tokens = n * FT
    blk = 512
    chips = n // 2
    rows = 64 // (n // GS)
    cols = d // GS
    fr = time_real.shape[0]
    vm = pl.BlockSpec(memory_space=pltpu.VMEM)
    hbm = pl.BlockSpec(memory_space=pl.ANY)
    sems = pltpu.SemaphoreType.DMA
    scratch = [
        pltpu.VMEM((64, FT), bf16),
        pltpu.VMEM((2, 2, HD), f32),
        pltpu.VMEM((2, 3, fr, d), bf16),
        pltpu.VMEM((FT, d), bf16),
        pltpu.VMEM((64, d), bf16),
        pltpu.VMEM((2, 128, d), bf16),
        pltpu.VMEM((2, 64, d), bf16),
        pltpu.VMEM((2, 128, d), bf16),
        pltpu.VMEM((2, d, 256), bf16),
        pltpu.VMEM((2, d, 128), bf16),
        pltpu.VMEM((n, 8, 128), f32),
        pltpu.VMEM((chips, 16, 128), bf16),
        pltpu.VMEM((n, 16, 128), bf16),
        pltpu.VMEM((chips, 16, 128), bf16),
        pltpu.VMEM((n, 8, 128), f32),
        pltpu.VMEM((chips, 2, 64, 128), bf16),
        pltpu.VMEM((128, tokens), bf16),
        pltpu.VMEM((64, 128), bf16),
        pltpu.VMEM((2, 128, 128), f32),
        pltpu.VMEM((2, 256, 128), bf16),
        pltpu.VMEM((2, 128, 128), bf16),
        pltpu.VMEM((2, 144, d), bf16),
        pltpu.VMEM((2, 144, 256), f32),
        pltpu.VMEM((2, 128, 1024), bf16),
        pltpu.VMEM((2, 128, 128), f32),
        pltpu.VMEM((2, 144, 128), f32),
        pltpu.VMEM((2, 8, tokens), f32),
        pltpu.VMEM((2, 128, tokens), f32),
        pltpu.VMEM((2, 128, tokens), f32),
        pltpu.VMEM((chips, 8, 128), f32),
        pltpu.VMEM((n, 8, 128), f32),
        pltpu.VMEM((chips, 8, 128), f32),
        pltpu.VMEM((2, 128, tokens), bf16),
        pltpu.VMEM((2, tokens, 128), bf16),
        pltpu.VMEM((2, 80, tokens), bf16),
        pltpu.VMEM((2, 8, blk), f32),
        pltpu.VMEM((2, 80, blk), f32),
        pltpu.VMEM((2, blk, blk), f32),
        pltpu.VMEM((n, 128, 128), bf16),
        pltpu.VMEM((n, 128, 128), bf16),
        pltpu.VMEM((n, 8, 128), f32),
        pltpu.VMEM((2 * FT, d // 2), bf16),
        pltpu.VMEM((64, 2 * FT), bf16),
        pltpu.VMEM((64, d // 2), bf16),
        pltpu.VMEM((chips, rows, cols), bf16),
        pltpu.VMEM((nz, rows, cols), bf16),
        sems((20,)),
        sems((28,)),
    ]
    dmd, wg = pl.pallas_call(
        functools.partial(kernel, n, nz, blk),
        out_shape=(
            jax.ShapeDtypeStruct((1, 64, FT), f32),
            jax.ShapeDtypeStruct((64, d), bf16),
        ),
        in_specs=[pl.BlockSpec(memory_space=pltpu.SMEM)] + [hbm] * 19,
        out_specs=(vm, vm),
        scratch_shapes=scratch,
        compiler_params=pltpu.CompilerParams(
            collective_id=0, has_side_effects=True, vmem_limit_bytes=62 * 1024 * 1024
        ),
        name="dmd",
    )(
        timesteps, noise_field, gain_real, gain_fake,
        time_real.transpose(1, 0, 2), time_fake.transpose(1, 0, 2),
        hidden_states, gen_weight, embed_real, embed_fake, proj_real, proj_fake,
        out_real, out_fake,
        query_real, key_real, value_real, query_fake, key_fake, value_fake,
    )
    return dmd, wg.astype(f32)


def solution(mesh):
    in_specs = (
        P("batch", "tm", None), P(), P("batch", None, "tm"), P("batch"),
        P(), P("tm", None, None), P(None, "tm"), P(None, "tm"), P(None, "tm"),
        P("tm", None), P(None, "tm"), P(),
        P(), P("tm", None, None), P(None, "tm"), P(None, "tm"), P(None, "tm"),
        P("tm", None), P(None, "tm"), P(),
    )
    out_specs = (P("batch", None, "tm"), P())
    return jax.shard_map(
        per_device, mesh=mesh, in_specs=in_specs, out_specs=out_specs, check_vma=False
    )
```

```python
import functools
import math

import jax
import jax.numpy as jnp
from jax import lax
from jax.experimental import pallas as pl
from jax.experimental.pallas import tpu as pltpu
from jax.sharding import PartitionSpec as P

HD = 128
FREQ = 256
FT = 128
GS = 8
MESH = pl.DeviceIdType.MESH

norm_floor = 0.05
gap_floor = 0.25
highest = lax.Precision.HIGHEST
f32 = jnp.float32
bf16 = jnp.bfloat16


def split2(a):
    hi = a.astype(bf16)
    lo = (a - hi.astype(f32)).astype(bf16)
    return hi, lo


def stack2(a):
    hi, lo = split2(a)
    return jnp.concatenate([hi, lo], axis=0)


def mm(a, b):
    return jnp.dot(a, b, preferred_element_type=f32)


def mm_t(a, b):
    return lax.dot_general(a, b, (((1,), (1,)), ((), ())), preferred_element_type=f32)


class Phase:
    def __init__(self):
        self.now = None

    def __call__(self, name):
        if self.now is not None:
            self.now.__exit__(None, None, None)
        self.now = None
        if name:
            self.now = jax.named_scope(name)
            self.now.__enter__()


def attend_block(block, later, blk, qt_ref, k_ref, v_ref, m_ref, o_ref, s_ref):
    frames = blk // FT

    def score(net, k_block, q_block):
        k_at = pl.multiple_of(k_block * blk, blk)
        q_at = pl.multiple_of(q_block * blk, blk)
        return mm(k_ref[net, pl.ds(k_at, blk), :], qt_ref[net, :, pl.ds(q_at, blk)])

    if later is None:
        for net in range(2):
            s_ref[net] = score(net, block, block)
        return

    def advance(kb, last, first):
        next_k = jnp.where(last, later, 0 if first else kb + 1)
        next_q = jnp.where(last, later, block)
        k_at = pl.multiple_of(kb * blk, blk)
        for net in range(2):
            s = s_ref[net]
            if first:
                rows = []
                for r in range(frames):
                    part = s[r * FT : (r + 1) * FT]
                    if r:
                        gone = jnp.full((FT, r * FT), -1e30, f32)
                        part = jnp.concatenate([gone, part[:, r * FT :]], axis=1)
                    rows.append(part)
                s = jnp.concatenate(rows, axis=0)
            top = jnp.max(s, axis=0, keepdims=True)
            if not first:
                old = m_ref[net, 0:1, :]
                top = jnp.maximum(old, top)
            p = jnp.exp2(s - top).astype(bf16)
            s_ref[net] = score(net, next_k, next_q)
            o = mm(v_ref[net, :, pl.ds(k_at, blk)], p)
            if not first:
                o = o_ref[net] * jnp.exp2(old - top) + o
            o_ref[net] = o
            m_ref[net] = jnp.broadcast_to(top, (8, blk))

    odd = lax.rem(block, 2)

    @pl.when(odd == 0)
    def _():
        advance(block, block == 0, True)

    @pl.when(odd == 1)
    def _():
        advance(block, False, True)
        advance(0, block == 1, False)

    def pair(i, _):
        for u in range(2):
            kb = odd + i * 2 + u
            advance(kb, kb == block - 1, False)
        return 0

    lax.fori_loop(0, block // 2, pair, 0)


def block_at(s, me, per, blocks):
    home = me // per
    if blocks != 8:
        return lax.rem(home + 1 + s, blocks)
    dx = jnp.where(s < 2, 2, jnp.where(s < 6, 1 + 2 * lax.rem(s - 2, 2), 0))
    dy = jnp.where(s < 2, 1 - s, jnp.where(s < 4, 1, jnp.where(s < 6, 0, 7 - s)))
    x = lax.rem(home // 2 + dx, 4)
    y = lax.rem(home + dy, 2)
    return x * 2 + y


def kernel(
    n, nz, blk,
    step_ref,
    noise_h, gain_rh, gain_fh, time_rh, time_fh, hidden_h, genw_h, emb_rh, emb_fh, proj_rh, proj_fh, out_rh, out_fh,
    wq_r, wk_r, wv_r, wq_f, wk_f, wv_f,
    dmd_ref, wg_ref,
    noise, gain, times, hid, genw, emb, proj, outw, wqk, wv,
    modbuf, modout, modin, modall, modfull, xg, xs, gen_s, mu_s, gmat, rmat,
    lhs, acc, lhs2, acc2, accv, rs_s, qraw, kraw, nbuf, nin, nfull,
    qt, kn, vt, m_s, o_s, s_s,
    tsend, trecv, gapbuf, hcol, dcat, wsend, wrecv, zbuf,
    lsem, sem,
):
    me = lax.axis_index("tm")
    mz = lax.axis_index("batch")
    core = lax.rem(me, 2)
    chip = me // 2
    other = me + 1 - 2 * core
    chips = n // 2
    d = hid.shape[1]
    groups = d // 1024
    tokens = n * FT
    ph = Phase()
    loads = []

    def load(src, dst):
        c = pltpu.make_async_copy(src, dst, lsem.at[len(loads)])
        c.start()
        loads.append(c)
        return c

    ld_time = [load(time_rh, times.at[0]), load(time_fh, times.at[1])]
    ld_noise = load(noise_h.at[0], noise)
    ld_hid = load(hidden_h.at[0], hid)
    ld_gen = load(genw_h, genw)
    ld_emb = [load(emb_rh, emb.at[0]), load(emb_fh, emb.at[1])]
    ld_proj = [load(proj_rh, proj.at[0]), load(proj_fh, proj.at[1])]
    ld_qk = []
    for net, (a, b) in enumerate(((wq_r, wk_r), (wq_f, wk_f))):
        ld_qk.append(load(a, wqk.at[net, :, 0:HD]))
        ld_qk.append(load(b, wqk.at[net, :, HD : 2 * HD]))
    ld_v = [load(wv_r, wv.at[0]), load(wv_f, wv.at[1])]
    ld_out = [load(out_rh, outw.at[0]), load(out_fh, outw.at[1])]

    ld_gain = [load(gain_rh, gain.at[0]), load(gain_fh, gain.at[1])]

    barrier = pltpu.get_barrier_semaphore()

    def greet(i, _):
        pl.semaphore_signal(
            barrier, inc=1, device_id={"tm": lax.rem(me + i, n)}, device_id_type=MESH
        )
        return 0

    lax.fori_loop(1, n, greet, 0)
    for i in range(1, nz):
        pl.semaphore_signal(
            barrier, inc=1, device_id={"batch": lax.rem(mz + i, nz)}, device_id_type=MESH
        )

    used = [0]
    wide = chips // 4
    shifts = [(dx, dy) for dx in range(wide) for dy in range(4) if dx or dy]
    shifts.sort(key=lambda t: -min(t[0], wide - t[0]) - min(t[1], 4 - t[1]))
    far_first = [
        lax.rem(chip // 4 + dx, wide) * 4 + lax.rem(lax.rem(chip, 4) + dy, 4) for dx, dy in shifts
    ]

    class Lane:
        def __init__(self):
            self.send = sem.at[used[0]]
            self.recv = sem.at[used[0] + 1]
            used[0] += 2

        def to(self, src, dst, j, axis="tm"):
            return pltpu.make_async_remote_copy(
                src_ref=src, dst_ref=dst, send_sem=self.send, recv_sem=self.recv,
                device_id={axis: j}, device_id_type=MESH,
            )

        def all(self, src_of, dst):
            def body(i, _):
                j = lax.rem(me + i, n)
                self.to(src_of(j), dst, j).start()
                return 0

            lax.fori_loop(1, n, body, 0)

        def mates(self, src_of, dst):
            for j in far_first:
                self.to(src_of(j), dst, 2 * j + core).start()

        def wait(self, view):
            c = self.to(view, view, other)
            c.wait_recv()
            c.wait_send()

        def owners(self, src_of, dst, count):
            for j in far_first + [chip]:

                @pl.when(jnp.logical_and(j < count, 2 * j + 1 != me))
                def _():
                    self.to(src_of(j), dst, 2 * j + 1).start()

        def to_owner(self, whole, count, then):
            owner = jnp.logical_and(core == 1, chip < count)

            @pl.when(owner)
            def _():
                self.to(whole, whole, other).wait_recv()
                then()

                for j in far_first:
                    for c in range(2):
                        self.back.to(self.result, self.result, 2 * j + c).start()
                self.back.to(self.result, self.result, other).start()

            return owner

        def settle(self, owner, sent, fewer):
            @pl.when(owner)
            def _():
                self.to(fewer, fewer, other).wait_send()

            @pl.when(jnp.logical_not(owner))
            def _():
                self.to(sent, sent, other).wait_send()

        def gather(self, owner, whole, all_in, fewer):
            @pl.when(owner)
            def _():
                self.to(whole, whole, other).wait_send()
                self.to(fewer, fewer, other).wait_recv()

            @pl.when(jnp.logical_not(owner))
            def _():
                self.to(all_in, all_in, other).wait_recv()

    pieces = (6 * groups + 1) // 2
    mod_rs, mod_ag, xl, xf = Lane(), Lane(), Lane(), Lane()
    nrm_rs, nrm_ag, tl, gl = Lane(), Lane(), Lane(), Lane()
    hl, dl, w_rs, w_z, w_ag, w_fw = Lane(), Lane(), Lane(), Lane(), Lane(), Lane()
    gy = GS // 2
    half_d = d // 2
    slot = pl.ds(pl.multiple_of(core * FT, FT), FT)

    def half_of(c):
        return pl.ds(pl.multiple_of(c * half_d, 128), half_d)


    ph("share")
    step = jnp.full((1, 128), step_ref[0], jnp.int32).astype(f32)
    raw = step / 1000.0
    sigma = 5.0 * raw / (1.0 + 4.0 * raw)
    freqs = times.shape[2]
    first = me * freqs + lax.broadcasted_iota(jnp.int32, (freqs, 128), 0)
    k = lax.rem(first, FREQ // 2).astype(f32)
    angle = step * jnp.exp(k * (-math.log(10000.0) / (FREQ // 2)))
    turns = jnp.floor(angle * (0.5 / math.pi) + 0.5)
    angle = (angle - turns * 6.28125) - turns * (2.0 * math.pi - 6.28125)
    wave = jnp.where(first < FREQ // 2, jnp.cos(angle), jnp.sin(angle)).astype(bf16).astype(f32)
    for p in range(6 * groups, 2 * pieces):
        modbuf[p] = jnp.zeros((8, 128), f32)
    for net in range(2):
        ld_time[net].wait()
        for c in range(3):
            for b in range(8 * groups):
                t = times[net, c, :, b * 128 : (b + 1) * 128].astype(f32)
                part = jnp.sum(t * wave, axis=0, keepdims=True)
                modbuf[(net * 3 + c) * groups + b // 8, b % 8 : b % 8 + 1, :] = part
    for j in range(pieces):
        pair = jnp.concatenate([modbuf[2 * j], modbuf[2 * j + 1]], axis=0)
        modout[j] = pair.astype(bf16)
    ph("barrier")
    pl.semaphore_wait(barrier, n - 1 + nz - 1)
    mod_rs.owners(lambda j: modout.at[j], modin.at[me], pieces)

    ph("generate")
    ld_hid.wait()
    ld_gen.wait()
    generated = mm_t(genw[...], hid[...]).astype(bf16)
    gen_s[...] = generated
    ld_noise.wait()
    mixed = (1.0 - sigma) * generated.astype(f32) + sigma * noise[...].astype(f32)
    xg[chip, core] = mixed.astype(bf16)
    mine = xg.at[chip, core]
    xl.mates(lambda j: mine, mine)

    ph("weights")
    ones_k = jnp.ones((1024, 128), bf16)

    def weight_terms(net):
        ld_emb[net].wait()
        ld_proj[net].wait()

        def gram(g, t):
            at = pl.multiple_of(g * 1024, 1024)
            e = emb[net, :, pl.ds(at, 1024)]
            return (
                t[0] + mm_t(e, e),
                t[1] + mm(e, ones_k),
                t[2] + mm_t(proj[net, :, pl.ds(at, 1024)], e),
            )

        zero = jnp.zeros((128, 128), f32)
        ee, mu, rr = lax.fori_loop(
            0, groups, gram, (zero, zero, jnp.zeros((64, 128), f32)), unroll=True
        )
        mu = mu / d
        mu_s[net] = mu
        gmat[net] = stack2(ee / d - mu * mu.T)
        rmat[net] = stack2(rr)

    weight_terms(0)
    ph("mod_rs")

    def add_mod():
        modin[me] = modout[chip]
        total = modin[0].astype(f32)
        for j in range(1, n):
            total = total + modin[j].astype(f32)
        modall[chip] = total.astype(bf16)

    mod_rs.back, mod_rs.result = mod_ag, modall.at[chip]
    mod_owner = mod_rs.to_owner(modin.at[pl.ds(0, n - 1)], pieces, add_mod)
    mod_rs.settle(mod_owner, modout.at[pl.ds(0, pieces)], modout.at[pl.ds(0, pieces - 1)])
    hl.to(hid.at[:, half_of(1 - core)], hcol.at[slot, :], other).start()

    ph("weights1")
    weight_terms(1)
    hcol[slot, :] = hid[:, half_of(core)]

    ph("x_wait")
    xl.wait(xg.at[pl.ds(0, chips - 1), core])
    xf.to(xg.at[:, core], xg.at[:, core], other).start()
    xs[64:128, 0:FT] = jnp.zeros((64, FT), bf16)

    def place(parity, i):
        at = pl.multiple_of(i * (2 * FT) + parity * FT, FT)
        x = xg[i, parity]
        xs[0:64, pl.ds(at, FT)] = x
        return at, x

    def place_both(parity):
        def body(i, _):
            at, x = place(parity, i)
            xs[64:128, pl.ds(pl.multiple_of(at + FT, FT), FT)] = x
            return 0

        return body

    lax.fori_loop(0, chips - 1, place_both(core), 0, unroll=5)
    ph("x_fwait")
    xf.wait(xg.at[:, core])

    ph("place_var")

    lax.fori_loop(0, chips - 1, place_both(1 - core), 0, unroll=5)
    at, x = place(0, chips - 1)
    xs[64:128, pl.ds(pl.multiple_of(at + FT, FT), FT)] = x
    place(1, chips - 1)

    width = blk

    def variances(t, _):
        at = pl.multiple_of(t * width, width)
        x = xs[:, pl.ds(at, width)]
        for net in range(2):
            y = mm(gmat[net], x)
            var = jnp.sum((y[0:128] + y[128:256]) * x.astype(f32), axis=0, keepdims=True)
            rs = lax.rsqrt(jnp.maximum(var, 0.0) + norm_floor)
            rs_s[net, :, pl.ds(at, width)] = jnp.broadcast_to(rs, (8, width))
        return 0

    lax.fori_loop(0, tokens // width, variances, 0, unroll=4)
    for c in ld_qk:
        c.wait()
    ph("mod_ag_wait")
    mod_ag.gather(
        mod_owner, modin.at[pl.ds(0, n - 1)], modall.at[pl.ds(0, pieces)],
        modall.at[pl.ds(0, pieces - 1)],
    )
    for j in range(pieces):
        both = modall[j].astype(f32)
        modfull[2 * j] = both[0:8]
        modfull[2 * j + 1] = both[8:16]

    ph("qk_fold")
    row = lax.broadcasted_iota(jnp.int32, (16, 128), 0)
    acc[...] = jnp.zeros_like(acc)

    def fold(g, _):
        at = pl.multiple_of(g * 1024, 1024)
        for net in range(2):
            shift8 = modfull[(net * 3 + 0) * groups + g]
            scale8 = modfull[(net * 3 + 1) * groups + g]
            for r in range(8):
                col = pl.multiple_of(at + r * 128, 128)
                e = emb[net, :, pl.ds(col, 128)].astype(f32) - mu_s[net]
                lhs[net, 0:128, pl.ds(col, 128)] = (e * (1.0 + scale8[r : r + 1, :])).astype(bf16)
                sh, sl = split2(shift8[r : r + 1, :])
                tail = jnp.where(
                    row == 0, sh.astype(f32), jnp.where(row == 1, sl.astype(f32), 0.0)
                )
                lhs[net, 128:144, pl.ds(col, 128)] = tail.astype(bf16)
            acc[net] += mm(lhs[net, :, pl.ds(at, 1024)], wqk[net, pl.ds(at, 1024), :])
        return 0

    lax.fori_loop(0, groups, fold, 0, unroll=True)
    ph("qk_project")
    mats = []
    for net in range(2):
        off = acc[net, 128:129, :] + acc[net, 129:130, :]
        for which in range(2):
            cols = slice(which * HD, (which + 1) * HD)
            mat = acc[net, 0:128, cols].T.astype(bf16)
            mats.append((mat, jnp.broadcast_to(off[:, cols], (128, 128)).T[:, 0:1]))

    def project(t, _):
        at = pl.multiple_of(t * width, width)
        x = xs[:, pl.ds(at, width)]
        for net in range(2):
            rs = rs_s[net, 0:1, pl.ds(at, width)]
            for which, dst in enumerate((qraw, kraw)):
                mat, off_c = mats[net * 2 + which]
                y = mm(mat, x) * rs + off_c
                dst[net, :, pl.ds(at, width)] = y
                sq = jnp.sum(y * y, axis=0, keepdims=True)
                for r in range(width // FT):
                    row = (r % 2) * 4 + net * 2 + which
                    nbuf[t * (width // FT // 2) + r // 2, row : row + 1, :] = sq[
                        :, r * FT : (r + 1) * FT
                    ]
        return 0

    lax.fori_loop(0, tokens // width, project, 0, unroll=True)

    ph("norm_send")
    nrm_rs.owners(lambda j: nbuf.at[j], nin.at[me], chips)

    ph("v_fold")
    for c in ld_v + ld_out:
        c.wait()
    accv[...] = jnp.zeros_like(accv)
    acc2[...] = jnp.zeros_like(acc2)

    def fold_v(g, _):
        at = pl.multiple_of(g * 1024, 1024)
        for net in range(2):
            gate8 = modfull[(net * 3 + 2) * groups + g]
            for r in range(8):
                col = pl.multiple_of(at + r * 128, 128)
                gated = proj[net, :, pl.ds(col, 128)].astype(f32) * gate8[r : r + 1, :]
                hi, lo = split2(gated)
                lhs2[net, 0:64, r * 128 : (r + 1) * 128] = hi
                lhs2[net, 64:128, r * 128 : (r + 1) * 128] = lo
            accv[net] += mm(lhs[net, :, pl.ds(at, 1024)], wv[net, pl.ds(at, 1024), :])
            acc2[net] += mm_t(lhs2[net], outw[net, :, pl.ds(at, 1024)])
        return 0

    lax.fori_loop(0, groups, fold_v, 0, unroll=True)

    ph("norm_rs_wait")

    def add_norm():
        nin[me] = nbuf[chip]
        nfull[chip] = lax.rsqrt(jnp.sum(nin[...], axis=0) / float(n * HD) + norm_floor)

    nrm_rs.back, nrm_rs.result = nrm_ag, nfull.at[chip]
    nrm_owner = nrm_rs.to_owner(nin.at[pl.ds(0, n - 1)], chips, add_norm)
    nrm_rs.settle(nrm_owner, nbuf.at[pl.ds(0, chips)], nbuf.at[pl.ds(0, chips - 1)])

    ph("values")
    vmats = []
    for net in range(2):
        a = accv[net, 0:128, :]
        off = accv[net, 128:129, :] + accv[net, 129:130, :]
        out_t = acc2[net, 0:64, :] + acc2[net, 64:128, :]
        b_mat = stack2(
            lax.dot_general(
                out_t, a, (((1,), (1,)), ((), ())), precision=highest, preferred_element_type=f32
            )
        )
        vmats.append((b_mat, jnp.sum(out_t * off, axis=1, keepdims=True)))
    ones = jnp.where(lax.broadcasted_iota(jnp.int32, (16, width), 0) == 0, 1.0, 0.0)

    def values(t, _):
        at = pl.multiple_of(t * width, width)
        x = xs[:, pl.ds(at, width)]
        for net in range(2):
            y = mm(vmats[net][0], x)
            y = (y[0:64] + y[64:128]) * rs_s[net, 0:1, pl.ds(at, width)] + vmats[net][1]
            vt[net, 0:64, pl.ds(at, width)] = y.astype(bf16)
            vt[net, 64:80, pl.ds(at, width)] = ones.astype(bf16)
        return 0

    lax.fori_loop(0, tokens // width, values, 0, unroll=4)
    gains = []
    for net in range(2):
        ld_gain[net].wait()
        both = gain[net, 0:1, :] * gain[net, 1:2, :] * (math.log2(math.e) / math.sqrt(HD))
        gains.append(jnp.broadcast_to(both, (128, 128)).T)

    def gained(t, _):
        at = pl.multiple_of(t * FT, FT)
        for net in range(2):
            qraw[net, :, pl.ds(at, FT)] = qraw[net, :, pl.ds(at, FT)] * gains[net]
        return 0

    lax.fori_loop(0, n, gained, 0, unroll=4)
    same = lax.broadcasted_iota(jnp.int32, (256, 256), 0) == lax.broadcasted_iota(
        jnp.int32, (256, 256), 1
    )
    eye = jnp.where(same, 1.0, 0.0).astype(bf16)
    ph("norm_ag_wait")
    nrm_ag.gather(
        nrm_owner, nin.at[pl.ds(0, n - 1)], nfull.at[pl.ds(0, chips)],
        nfull.at[pl.ds(0, chips - 1)],
    )

    ph("normalise")

    def normalise(t, _):
        at = pl.multiple_of(t * 256, 256)
        k_rows = []
        for net in range(2):
            k_cols = []
            for half in range(2):
                scales = nfull[t]
                to = pl.ds(pl.multiple_of(at + half * FT, FT), FT)
                at_row = half * 4 + net * 2
                sq = scales[at_row : at_row + 1, :]
                sk = scales[at_row + 1 : at_row + 2, :]
                qt[net, :, to] = (qraw[net, :, to] * sq).astype(bf16)
                k_cols.append((kraw[net, :, to] * sk).astype(bf16))
            k_rows.append(jnp.concatenate(k_cols, axis=1))
        turned = mm_t(eye, jnp.concatenate(k_rows, axis=0)).astype(bf16)
        for net in range(2):
            kn[net, pl.ds(at, 256), :] = turned[:, net * HD : (net + 1) * HD]
        return 0

    lax.fori_loop(0, tokens // 256, normalise, 0, unroll=True)

    ph("attend")
    blocks = tokens // blk
    per = blk // FT

    def one_block(s, _):
        block = block_at(s, me, per, blocks)
        later = block_at(lax.rem(s + 1, blocks), me, per, blocks)
        attend_block(block, later, blk, qt, kn, vt, m_s, o_s, s_s)
        for net in range(2):
            o = o_s[net]
            y = (o[0:64] / o[64:65]).astype(bf16)
            for r in range(per):
                tsend[block * per + r, net * 64 : (net + 1) * 64, :] = y[:, r * FT : (r + 1) * FT]
        for r in range(per):
            f = block * per + r

            @pl.when(f != me)
            def _():
                tl.to(tsend.at[f], trecv.at[me], f).start()

        return 0

    attend_block(block_at(0, me, per, blocks), None, blk, qt, kn, vt, m_s, o_s, s_s)
    lax.fori_loop(0, blocks, one_block, 0)
    ph("t_wait")
    x_own = xs[:, pl.ds(pl.multiple_of(me * FT, FT), FT)]
    base_r = mm(rmat[0], x_own)
    base_f = mm(rmat[1], x_own)
    noisy = x_own[0:64].astype(f32)
    trecv[me] = tsend[me]
    tl.wait(trecv.at[pl.ds(0, n - 1)])

    ph("finish")

    def add_up(s, t):
        return t + trecv[s].astype(f32)

    vel = lax.fori_loop(0, n, add_up, jnp.zeros((128, FT), f32), unroll=True)
    vel_r = vel[0:64] + base_r[0:64] + base_r[64:128]
    vel_f = vel[64:128] + base_f[0:64] + base_f[64:128]
    pred_r = noisy - sigma * vel_r
    pred_f = noisy - sigma * vel_f
    gap = jnp.abs(gen_s[...].astype(f32) - pred_r)
    gsum = gap[0:8]
    for r in range(1, 8):
        gsum = gsum + gap[r * 8 : (r + 1) * 8]
    gapbuf[me] = gsum
    diff = pred_f - pred_r
    own = dcat.at[:, slot]
    own[...] = diff.astype(bf16)
    dl.to(own, own, other).start()
    gl.all(lambda j: gapbuf.at[me], gapbuf.at[me])
    dmd_ref[0] = diff
    ph("h_wait")
    hl.wait(hcol.at[pl.ds(0, FT), :])
    ph("d_wait")
    dl.wait(dcat.at[:, pl.ds(0, FT)])
    ph("wg_mm")
    wsend[...] = mm(dcat[...], hcol[...]).astype(bf16)
    rows = wrecv.shape[1]
    cols = wrecv.shape[2]

    def piece(j, c):
        return (
            pl.ds(pl.multiple_of(j // gy * rows, 16), rows),
            pl.ds(pl.multiple_of(c * half_d + lax.rem(j, gy) * cols, 128), cols),
        )

    w_rs.mates(lambda j: wsend.at[piece(j, 0)], wrecv.at[chip])
    wrecv[chip] = wsend[piece(chip, 0)]
    ph("gap_wait")
    gl.wait(gapbuf.at[pl.ds(0, n - 1)])
    gap_all = jnp.sum(jnp.sum(gapbuf[...], axis=0), keepdims=True)
    inv = 1.0 / jnp.maximum(gap_all / (64.0 * tokens), gap_floor)
    dmd_ref[0] = dmd_ref[0] * inv
    ph("w_wait")
    w_rs.wait(wrecv.at[pl.ds(0, chips - 1)])
    wsum = wrecv[0].astype(f32)
    for j in range(1, chips):
        wsum = wsum + wrecv[j].astype(f32)
    zbuf[mz] = (wsum * (inv / math.sqrt(nz * tokens))).astype(bf16)
    ph("w_z")
    for i in range(1, nz):
        w_z.to(zbuf.at[mz], zbuf.at[mz], lax.rem(mz + i, nz), "batch").start()
    if nz > 1:
        zview = zbuf.at[pl.ds(0, nz - 1)]
        zwait = w_z.to(zview, zview, lax.rem(mz + 1, nz), "batch")
        zwait.wait_recv()
        zwait.wait_send()
    whole = zbuf[0].astype(f32)
    for z in range(1, nz):
        whole = whole + zbuf[z].astype(f32)
    ph("w_ag")
    part = wg_ref.at[piece(chip, core)]
    part[...] = whole.astype(bf16)
    w_ag.mates(lambda j: part, part)
    w_ag.wait(wrecv.at[pl.ds(0, chips - 1)])
    ph("w_forward")
    mine_half = wg_ref.at[:, half_of(core)]
    w_fw.to(mine_half, mine_half, other).start()
    w_fw.wait(mine_half)
    ph(None)


def per_device(
    hidden_states, gen_weight, noise_field, timesteps,
    embed_real, time_real, query_real, key_real, value_real, out_real, gain_real, proj_real,
    embed_fake, time_fake, query_fake, key_fake, value_fake, out_fake, gain_fake, proj_fake,
):
    n = lax.axis_size("tm")
    nz = lax.axis_size("batch")
    d = hidden_states.shape[2]
    tokens = n * FT
    blk = 512
    chips = n // 2
    rows = 64 // (n // GS)
    cols = d // GS
    fr = time_real.shape[0]
    vm = pl.BlockSpec(memory_space=pltpu.VMEM)
    hbm = pl.BlockSpec(memory_space=pl.ANY)
    sems = pltpu.SemaphoreType.DMA
    scratch = [
        pltpu.VMEM((64, FT), bf16),
        pltpu.VMEM((2, 2, HD), f32),
        pltpu.VMEM((2, 3, fr, d), bf16),
        pltpu.VMEM((FT, d), bf16),
        pltpu.VMEM((64, d), bf16),
        pltpu.VMEM((2, 128, d), bf16),
        pltpu.VMEM((2, 64, d), bf16),
        pltpu.VMEM((2, 128, d), bf16),
        pltpu.VMEM((2, d, 256), bf16),
        pltpu.VMEM((2, d, 128), bf16),
        pltpu.VMEM((n, 8, 128), f32),
        pltpu.VMEM((chips, 16, 128), bf16),
        pltpu.VMEM((n, 16, 128), bf16),
        pltpu.VMEM((chips, 16, 128), bf16),
        pltpu.VMEM((n, 8, 128), f32),
        pltpu.VMEM((chips, 2, 64, 128), bf16),
        pltpu.VMEM((128, tokens), bf16),
        pltpu.VMEM((64, 128), bf16),
        pltpu.VMEM((2, 128, 128), f32),
        pltpu.VMEM((2, 256, 128), bf16),
        pltpu.VMEM((2, 128, 128), bf16),
        pltpu.VMEM((2, 144, d), bf16),
        pltpu.VMEM((2, 144, 256), f32),
        pltpu.VMEM((2, 128, 1024), bf16),
        pltpu.VMEM((2, 128, 128), f32),
        pltpu.VMEM((2, 144, 128), f32),
        pltpu.VMEM((2, 8, tokens), f32),
        pltpu.VMEM((2, 128, tokens), f32),
        pltpu.VMEM((2, 128, tokens), f32),
        pltpu.VMEM((chips, 8, 128), f32),
        pltpu.VMEM((n, 8, 128), f32),
        pltpu.VMEM((chips, 8, 128), f32),
        pltpu.VMEM((2, 128, tokens), bf16),
        pltpu.VMEM((2, tokens, 128), bf16),
        pltpu.VMEM((2, 80, tokens), bf16),
        pltpu.VMEM((2, 8, blk), f32),
        pltpu.VMEM((2, 80, blk), f32),
        pltpu.VMEM((2, blk, blk), f32),
        pltpu.VMEM((n, 128, 128), bf16),
        pltpu.VMEM((n, 128, 128), bf16),
        pltpu.VMEM((n, 8, 128), f32),
        pltpu.VMEM((2 * FT, d // 2), bf16),
        pltpu.VMEM((64, 2 * FT), bf16),
        pltpu.VMEM((64, d // 2), bf16),
        pltpu.VMEM((chips, rows, cols), bf16),
        pltpu.VMEM((nz, rows, cols), bf16),
        sems((20,)),
        sems((28,)),
    ]
    dmd, wg = pl.pallas_call(
        functools.partial(kernel, n, nz, blk),
        out_shape=(
            jax.ShapeDtypeStruct((1, 64, FT), f32),
            jax.ShapeDtypeStruct((64, d), bf16),
        ),
        in_specs=[pl.BlockSpec(memory_space=pltpu.SMEM)] + [hbm] * 19,
        out_specs=(vm, vm),
        scratch_shapes=scratch,
        compiler_params=pltpu.CompilerParams(
            collective_id=0, has_side_effects=True, vmem_limit_bytes=62 * 1024 * 1024
        ),
        name="dmd",
    )(
        timesteps, noise_field, gain_real, gain_fake,
        time_real.transpose(1, 0, 2), time_fake.transpose(1, 0, 2),
        hidden_states, gen_weight, embed_real, embed_fake, proj_real, proj_fake,
        out_real, out_fake,
        query_real, key_real, value_real, query_fake, key_fake, value_fake,
    )
    return dmd, wg.astype(f32)


def solution(mesh):
    in_specs = (
        P("batch", "tm", None), P(), P("batch", None, "tm"), P("batch"),
        P(), P("tm", None, None), P(None, "tm"), P(None, "tm"), P(None, "tm"),
        P("tm", None), P(None, "tm"), P(),
        P(), P("tm", None, None), P(None, "tm"), P(None, "tm"), P(None, "tm"),
        P("tm", None), P(None, "tm"), P(),
    )
    out_specs = (P("batch", None, "tm"), P())
    return jax.shard_map(
        per_device, mesh=mesh, in_specs=in_specs, out_specs=out_specs, check_vma=False
    )
```

```python
import functools
import math

import jax
import jax.numpy as jnp
from jax import lax
from jax.experimental import pallas as pl
from jax.experimental.pallas import tpu as pltpu
from jax.sharding import PartitionSpec as P

HD = 128
FREQ = 256
FT = 128
GS = 8
MESH = pl.DeviceIdType.MESH

norm_floor = 0.05
gap_floor = 0.25
highest = lax.Precision.HIGHEST
f32 = jnp.float32
bf16 = jnp.bfloat16


def split2(a):
    hi = a.astype(bf16)
    lo = (a - hi.astype(f32)).astype(bf16)
    return hi, lo


def stack2(a):
    hi, lo = split2(a)
    return jnp.concatenate([hi, lo], axis=0)


def mm(a, b):
    return jnp.dot(a, b, preferred_element_type=f32)


def mm_t(a, b):
    return lax.dot_general(a, b, (((1,), (1,)), ((), ())), preferred_element_type=f32)


class Phase:
    def __init__(self):
        self.now = None

    def __call__(self, name):
        if self.now is not None:
            self.now.__exit__(None, None, None)
        self.now = None
        if name:
            self.now = jax.named_scope(name)
            self.now.__enter__()


def attend_block(block, later, blk, qt_ref, k_ref, v_ref, m_ref, o_ref, s_ref):
    frames = blk // FT

    def score(net, k_block, q_block):
        k_at = pl.multiple_of(k_block * blk, blk)
        q_at = pl.multiple_of(q_block * blk, blk)
        return mm(k_ref[net, pl.ds(k_at, blk), :], qt_ref[net, :, pl.ds(q_at, blk)])

    if later is None:
        for net in range(2):
            s_ref[0, net] = score(net, block, block)
        return

    def advance(kb, last, first, src, dst):
        next_k = jnp.where(last, later, 0 if first else kb + 1)
        next_q = jnp.where(last, later, block)
        k_at = pl.multiple_of(kb * blk, blk)
        for net in range(2):
            s = s_ref[src, net]
            if first:
                rows = []
                for r in range(frames):
                    part = s[r * FT : (r + 1) * FT]
                    if r:
                        gone = jnp.full((FT, r * FT), -1e30, f32)
                        part = jnp.concatenate([gone, part[:, r * FT :]], axis=1)
                    rows.append(part)
                s = jnp.concatenate(rows, axis=0)
            top = jnp.max(s, axis=0, keepdims=True)
            if not first:
                old = m_ref[net, 0:1, :]
                top = jnp.maximum(old, top)
            p = jnp.exp2(s - top).astype(bf16)
            s_ref[dst, net] = score(net, next_k, next_q)
            o = mm(v_ref[net, :, pl.ds(k_at, blk)], p)
            if not first:
                o = o_ref[net] * jnp.exp2(old - top) + o
            o_ref[net] = o
            m_ref[net] = jnp.broadcast_to(top, (8, blk))

    odd = lax.rem(block, 2)

    @pl.when(odd == 0)
    def _():
        advance(block, block == 0, True, 0, 0)

    @pl.when(odd == 1)
    def _():
        advance(block, False, True, 0, 1)
        advance(0, block == 1, False, 1, 0)

    def pair(i, _):
        for u in range(2):
            kb = odd + i * 2 + u
            advance(kb, kb == block - 1, False, u, 1 - u)
        return 0

    lax.fori_loop(0, block // 2, pair, 0)


def block_at(s, me, per, blocks):
    home = me // per
    if blocks != 8:
        return lax.rem(home + 1 + s, blocks)
    dx = jnp.where(s < 2, 2, jnp.where((s == 2) | (s == 7), 0, 1 + 2 * lax.rem(s - 1, 2)))
    dy = jnp.where((s == 0) | ((s > 1) & (s < 5)), 1, 0)
    x = lax.rem(home // 2 + dx, 4)
    y = lax.rem(home + dy, 2)
    return x * 2 + y


def kernel(
    n, nz, blk,
    step_ref,
    noise_h, gain_rh, gain_fh, time_rh, time_fh, hidden_h, genw_h, emb_rh, emb_fh, proj_rh, proj_fh, out_rh, out_fh,
    wq_r, wk_r, wv_r, wq_f, wk_f, wv_f,
    dmd_h, wg_h,
    noise, gain, times, hid, genw, emb, proj, outw, wqk, wv,
    modbuf, modout, modin, modall, modfull, xg, xs, gen_s, mu_s, gmat, rmat,
    lhs, acc, lhs2, acc2, accv, rs_s, qraw, kraw, nbuf, nin, nfull,
    qt, kn, vt, m_s, o_s, s_s,
    dmd_ref, wg_ref, tsend, trecv, gapbuf, hcol, dcat, wsend, wrecv, zbuf,
    lsem, sem,
):
    me = lax.axis_index("tm")
    mz = lax.axis_index("batch")
    core = lax.rem(me, 2)
    chip = me // 2
    other = me + 1 - 2 * core
    chips = n // 2
    d = hid.shape[1]
    groups = d // 1024
    tokens = n * FT
    ph = Phase()
    loads = []

    def load(src, dst):
        c = pltpu.make_async_copy(src, dst, lsem.at[len(loads)])
        c.start()
        loads.append(c)
        return c

    ld_time = [load(time_rh, times.at[0]), load(time_fh, times.at[1])]
    ld_noise = load(noise_h.at[0], noise)
    ld_hid = load(hidden_h.at[0], hid)
    ld_gen = load(genw_h, genw)
    ld_emb = [load(emb_rh, emb.at[0]), load(emb_fh, emb.at[1])]
    ld_proj = [load(proj_rh, proj.at[0]), load(proj_fh, proj.at[1])]
    ld_qk = []
    for net, (a, b) in enumerate(((wq_r, wk_r), (wq_f, wk_f))):
        ld_qk.append(load(a, wqk.at[net, :, 0:HD]))
        ld_qk.append(load(b, wqk.at[net, :, HD : 2 * HD]))
    ld_v = [load(wv_r, wv.at[0]), load(wv_f, wv.at[1])]
    ld_out = [load(out_rh, outw.at[0]), load(out_fh, outw.at[1])]

    ld_gain = [load(gain_rh, gain.at[0]), load(gain_fh, gain.at[1])]

    barrier = pltpu.get_barrier_semaphore()

    def greet(i, _):
        pl.semaphore_signal(
            barrier, inc=1, device_id={"tm": lax.rem(me + i, n)}, device_id_type=MESH
        )
        return 0

    lax.fori_loop(1, n, greet, 0)
    for i in range(1, nz):
        pl.semaphore_signal(
            barrier, inc=1, device_id={"batch": lax.rem(mz + i, nz)}, device_id_type=MESH
        )

    used = [0]
    wide = chips // 4
    shifts = [(dx, dy) for dx in range(wide) for dy in range(4) if dx or dy]
    shifts.sort(key=lambda t: -min(t[0], wide - t[0]) - min(t[1], 4 - t[1]))
    far_first = [
        lax.rem(chip // 4 + dx, wide) * 4 + lax.rem(lax.rem(chip, 4) + dy, 4) for dx, dy in shifts
    ]

    class Lane:
        def __init__(self):
            self.send = sem.at[used[0]]
            self.recv = sem.at[used[0] + 1]
            used[0] += 2

        def to(self, src, dst, j, axis="tm"):
            return pltpu.make_async_remote_copy(
                src_ref=src, dst_ref=dst, send_sem=self.send, recv_sem=self.recv,
                device_id={axis: j}, device_id_type=MESH,
            )

        def all(self, src_of, dst):
            def body(i, _):
                j = lax.rem(me + i, n)
                self.to(src_of(j), dst, j).start()
                return 0

            lax.fori_loop(1, n, body, 0)

        def mates(self, src_of, dst):
            for j in far_first:
                self.to(src_of(j), dst, 2 * j + core).start()

        def wait(self, view):
            c = self.to(view, view, other)
            c.wait_recv()
            c.wait_send()

        def owners(self, src_of, dst, count):
            for j in far_first + [chip]:

                @pl.when(jnp.logical_and(j < count, 2 * j + 1 != me))
                def _():
                    self.to(src_of(j), dst, 2 * j + 1).start()

        def to_owner(self, whole, count, then):
            owner = jnp.logical_and(core == 1, chip < count)

            @pl.when(owner)
            def _():
                self.to(whole, whole, other).wait_recv()
                then()

                for j in far_first:
                    for c in range(2):
                        self.back.to(self.result, self.result, 2 * j + c).start()
                self.back.to(self.result, self.result, other).start()

            return owner

        def settle(self, owner, sent, fewer):
            @pl.when(owner)
            def _():
                self.to(fewer, fewer, other).wait_send()

            @pl.when(jnp.logical_not(owner))
            def _():
                self.to(sent, sent, other).wait_send()

        def gather(self, owner, whole, all_in, fewer):
            @pl.when(owner)
            def _():
                self.to(whole, whole, other).wait_send()
                self.to(fewer, fewer, other).wait_recv()

            @pl.when(jnp.logical_not(owner))
            def _():
                self.to(all_in, all_in, other).wait_recv()

    pieces = (6 * groups + 1) // 2
    mod_rs, mod_ag, xl, xf = Lane(), Lane(), Lane(), Lane()
    nrm_rs, nrm_ag, tl, gl = Lane(), Lane(), Lane(), Lane()
    hl, dl, w_rs, w_z, w_ag, w_fw = Lane(), Lane(), Lane(), Lane(), Lane(), Lane()
    gy = GS // 2
    half_d = d // 2
    slot = pl.ds(pl.multiple_of(core * FT, FT), FT)

    def half_of(c):
        return pl.ds(pl.multiple_of(c * half_d, 128), half_d)


    ph("share")
    step = jnp.full((1, 128), step_ref[0], jnp.int32).astype(f32)
    raw = step / 1000.0
    sigma = 5.0 * raw / (1.0 + 4.0 * raw)
    freqs = times.shape[2]
    first = me * freqs + lax.broadcasted_iota(jnp.int32, (freqs, 128), 0)
    k = lax.rem(first, FREQ // 2).astype(f32)
    angle = step * jnp.exp(k * (-math.log(10000.0) / (FREQ // 2)))
    turns = jnp.floor(angle * (0.5 / math.pi) + 0.5)
    angle = (angle - turns * 6.28125) - turns * (2.0 * math.pi - 6.28125)
    wave = jnp.where(first < FREQ // 2, jnp.cos(angle), jnp.sin(angle)).astype(bf16).astype(f32)
    for p in range(6 * groups, 2 * pieces):
        modbuf[p] = jnp.zeros((8, 128), f32)
    for net in range(2):
        ld_time[net].wait()
        for c in range(3):
            for b in range(8 * groups):
                t = times[net, c, :, b * 128 : (b + 1) * 128].astype(f32)
                part = jnp.sum(t * wave, axis=0, keepdims=True)
                modbuf[(net * 3 + c) * groups + b // 8, b % 8 : b % 8 + 1, :] = part
    for j in range(pieces):
        pair = jnp.concatenate([modbuf[2 * j], modbuf[2 * j + 1]], axis=0)
        modout[j] = pair.astype(bf16)
    ph("generate")
    ld_hid.wait()
    ld_gen.wait()
    generated = mm_t(genw[...], hid[...]).astype(bf16)
    gen_s[...] = generated
    ld_noise.wait()
    mixed = (1.0 - sigma) * generated.astype(f32) + sigma * noise[...].astype(f32)
    xg[chip, core] = mixed.astype(bf16)
    ph("barrier")
    pl.semaphore_wait(barrier, n - 1 + nz - 1)
    mod_rs.owners(lambda j: modout.at[j], modin.at[me], pieces)

    mine = xg.at[chip, core]
    xl.mates(lambda j: mine, mine)

    ph("weights")
    ones_k = jnp.ones((1024, 128), bf16)

    def weight_terms(net):
        ld_emb[net].wait()
        ld_proj[net].wait()

        def gram(g, t):
            at = pl.multiple_of(g * 1024, 1024)
            e = emb[net, :, pl.ds(at, 1024)]
            return (
                t[0] + mm_t(e, e),
                t[1] + mm(e, ones_k),
                t[2] + mm_t(proj[net, :, pl.ds(at, 1024)], e),
            )

        zero = jnp.zeros((128, 128), f32)
        ee, mu, rr = lax.fori_loop(
            0, groups, gram, (zero, zero, jnp.zeros((64, 128), f32)), unroll=True
        )
        mu = mu / d
        mu_s[net] = mu
        gmat[net] = stack2(ee / d - mu * mu.T)
        rmat[net] = stack2(rr)

    weight_terms(0)
    ph("mod_rs")

    def add_mod():
        modin[me] = modout[chip]
        total = modin[0].astype(f32)
        for j in range(1, n):
            total = total + modin[j].astype(f32)
        modall[chip] = total.astype(bf16)

    mod_rs.back, mod_rs.result = mod_ag, modall.at[chip]
    mod_owner = mod_rs.to_owner(modin.at[pl.ds(0, n - 1)], pieces, add_mod)
    mod_rs.settle(mod_owner, modout.at[pl.ds(0, pieces)], modout.at[pl.ds(0, pieces - 1)])

    ph("weights1")
    weight_terms(1)
    hcol[slot, :] = hid[:, half_of(core)]

    ph("x_wait")
    xl.wait(xg.at[pl.ds(0, chips - 1), core])
    xf.to(xg.at[:, core], xg.at[:, core], other).start()
    xs[64:128, 0:FT] = jnp.zeros((64, FT), bf16)

    def place(parity, i):
        at = pl.multiple_of(i * (2 * FT) + parity * FT, FT)
        x = xg[i, parity]
        xs[0:64, pl.ds(at, FT)] = x
        return at, x

    def place_both(parity):
        def body(i, _):
            at, x = place(parity, i)
            xs[64:128, pl.ds(pl.multiple_of(at + FT, FT), FT)] = x
            return 0

        return body

    lax.fori_loop(0, chips - 1, place_both(core), 0, unroll=5)
    ph("x_fwait")
    xf.wait(xg.at[:, core])
    hl.to(hid.at[:, half_of(1 - core)], hcol.at[slot, :], other).start()

    ph("place_var")

    lax.fori_loop(0, chips - 1, place_both(1 - core), 0, unroll=5)
    at, x = place(0, chips - 1)
    xs[64:128, pl.ds(pl.multiple_of(at + FT, FT), FT)] = x
    place(1, chips - 1)

    width = blk

    def variances(t, _):
        at = pl.multiple_of(t * width, width)
        x = xs[:, pl.ds(at, width)]
        for net in range(2):
            y = mm(gmat[net], x)
            var = jnp.sum((y[0:128] + y[128:256]) * x.astype(f32), axis=0, keepdims=True)
            rs = lax.rsqrt(jnp.maximum(var, 0.0) + norm_floor)
            rs_s[net, :, pl.ds(at, width)] = jnp.broadcast_to(rs, (8, width))
        return 0

    lax.fori_loop(0, tokens // width, variances, 0, unroll=True)
    for c in ld_qk:
        c.wait()
    ph("mod_ag_wait")
    mod_ag.gather(
        mod_owner, modin.at[pl.ds(0, n - 1)], modall.at[pl.ds(0, pieces)],
        modall.at[pl.ds(0, pieces - 1)],
    )
    for j in range(pieces):
        both = modall[j].astype(f32)
        modfull[2 * j] = both[0:8]
        modfull[2 * j + 1] = both[8:16]

    ph("qk_fold")
    row = lax.broadcasted_iota(jnp.int32, (16, 128), 0)
    acc[...] = jnp.zeros_like(acc)

    def fold(g, _):
        at = pl.multiple_of(g * 1024, 1024)
        for net in range(2):
            shift8 = modfull[(net * 3 + 0) * groups + g]
            scale8 = modfull[(net * 3 + 1) * groups + g]
            for r in range(8):
                col = pl.multiple_of(at + r * 128, 128)
                e = emb[net, :, pl.ds(col, 128)].astype(f32) - mu_s[net]
                lhs[net, 0:128, pl.ds(col, 128)] = (e * (1.0 + scale8[r : r + 1, :])).astype(bf16)
                sh, sl = split2(shift8[r : r + 1, :])
                tail = jnp.where(
                    row == 0, sh.astype(f32), jnp.where(row == 1, sl.astype(f32), 0.0)
                )
                lhs[net, 128:144, pl.ds(col, 128)] = tail.astype(bf16)
            acc[net] += mm(lhs[net, :, pl.ds(at, 1024)], wqk[net, pl.ds(at, 1024), :])
        return 0

    lax.fori_loop(0, groups, fold, 0, unroll=True)
    ph("qk_project")
    mats = []
    for net in range(2):
        off = acc[net, 128:129, :] + acc[net, 129:130, :]
        for which in range(2):
            cols = slice(which * HD, (which + 1) * HD)
            mat = acc[net, 0:128, cols].T.astype(bf16)
            mats.append((mat, jnp.broadcast_to(off[:, cols], (128, 128)).T[:, 0:1]))

    def project(t, _):
        at = pl.multiple_of(t * width, width)
        x = xs[:, pl.ds(at, width)]
        for net in range(2):
            rs = rs_s[net, 0:1, pl.ds(at, width)]
            for which, dst in enumerate((qraw, kraw)):
                mat, off_c = mats[net * 2 + which]
                y = mm(mat, x) * rs + off_c
                dst[net, :, pl.ds(at, width)] = y
                sq = jnp.sum(y * y, axis=0, keepdims=True)
                for r in range(width // FT):
                    row = (r % 2) * 4 + net * 2 + which
                    nbuf[t * (width // FT // 2) + r // 2, row : row + 1, :] = sq[
                        :, r * FT : (r + 1) * FT
                    ]
        return 0

    lax.fori_loop(0, tokens // width, project, 0, unroll=True)

    ph("norm_send")
    nrm_rs.owners(lambda j: nbuf.at[j], nin.at[me], chips)

    ph("v_fold")
    for c in ld_v + ld_out:
        c.wait()
    accv[...] = jnp.zeros_like(accv)
    acc2[...] = jnp.zeros_like(acc2)

    def fold_v(g, _):
        at = pl.multiple_of(g * 1024, 1024)
        for net in range(2):
            gate8 = modfull[(net * 3 + 2) * groups + g]
            for r in range(8):
                col = pl.multiple_of(at + r * 128, 128)
                gated = proj[net, :, pl.ds(col, 128)].astype(f32) * gate8[r : r + 1, :]
                hi, lo = split2(gated)
                lhs2[net, 0:64, r * 128 : (r + 1) * 128] = hi
                lhs2[net, 64:128, r * 128 : (r + 1) * 128] = lo
            accv[net] += mm(lhs[net, :, pl.ds(at, 1024)], wv[net, pl.ds(at, 1024), :])
            acc2[net] += mm_t(lhs2[net], outw[net, :, pl.ds(at, 1024)])
        return 0

    lax.fori_loop(0, groups, fold_v, 0, unroll=True)

    ph("norm_rs_wait")

    def add_norm():
        nin[me] = nbuf[chip]
        nfull[chip] = lax.rsqrt(jnp.sum(nin[...], axis=0) / float(n * HD) + norm_floor)

    nrm_rs.back, nrm_rs.result = nrm_ag, nfull.at[chip]
    nrm_owner = nrm_rs.to_owner(nin.at[pl.ds(0, n - 1)], chips, add_norm)
    nrm_rs.settle(nrm_owner, nbuf.at[pl.ds(0, chips)], nbuf.at[pl.ds(0, chips - 1)])

    ph("values")
    vmats = []
    for net in range(2):
        a = accv[net, 0:128, :]
        off = accv[net, 128:129, :] + accv[net, 129:130, :]
        out_t = acc2[net, 0:64, :] + acc2[net, 64:128, :]
        b_mat = stack2(
            lax.dot_general(
                out_t, a, (((1,), (1,)), ((), ())), precision=highest, preferred_element_type=f32
            )
        )
        vmats.append((b_mat, jnp.sum(out_t * off, axis=1, keepdims=True)))
    ones = jnp.where(lax.broadcasted_iota(jnp.int32, (16, width), 0) == 0, 1.0, 0.0)

    def values(t, _):
        at = pl.multiple_of(t * width, width)
        x = xs[:, pl.ds(at, width)]
        for net in range(2):
            y = mm(vmats[net][0], x)
            y = (y[0:64] + y[64:128]) * rs_s[net, 0:1, pl.ds(at, width)] + vmats[net][1]
            vt[net, 0:64, pl.ds(at, width)] = y.astype(bf16)
            vt[net, 64:80, pl.ds(at, width)] = ones.astype(bf16)
        return 0

    lax.fori_loop(0, tokens // width, values, 0, unroll=4)
    gains = []
    for net in range(2):
        ld_gain[net].wait()
        both = gain[net, 0:1, :] * gain[net, 1:2, :] * (math.log2(math.e) / math.sqrt(HD))
        gains.append(jnp.broadcast_to(both, (128, 128)).T)

    def gained(t, _):
        at = pl.multiple_of(t * FT, FT)
        for net in range(2):
            qraw[net, :, pl.ds(at, FT)] = qraw[net, :, pl.ds(at, FT)] * gains[net]
        return 0

    lax.fori_loop(0, n, gained, 0, unroll=4)
    same = lax.broadcasted_iota(jnp.int32, (256, 256), 0) == lax.broadcasted_iota(
        jnp.int32, (256, 256), 1
    )
    eye = jnp.where(same, 1.0, 0.0).astype(bf16)
    ph("norm_ag_wait")
    nrm_ag.gather(
        nrm_owner, nin.at[pl.ds(0, n - 1)], nfull.at[pl.ds(0, chips)],
        nfull.at[pl.ds(0, chips - 1)],
    )

    ph("normalise")

    def normalise(t, _):
        at = pl.multiple_of(t * 256, 256)
        k_rows = []
        for net in range(2):
            k_cols = []
            for half in range(2):
                scales = nfull[t]
                to = pl.ds(pl.multiple_of(at + half * FT, FT), FT)
                at_row = half * 4 + net * 2
                sq = scales[at_row : at_row + 1, :]
                sk = scales[at_row + 1 : at_row + 2, :]
                qt[net, :, to] = (qraw[net, :, to] * sq).astype(bf16)
                k_cols.append((kraw[net, :, to] * sk).astype(bf16))
            k_rows.append(jnp.concatenate(k_cols, axis=1))
        turned = mm_t(eye, jnp.concatenate(k_rows, axis=0)).astype(bf16)
        for net in range(2):
            kn[net, pl.ds(at, 256), :] = turned[:, net * HD : (net + 1) * HD]
        return 0

    lax.fori_loop(0, tokens // 256, normalise, 0, unroll=True)

    ph("attend")
    blocks = tokens // blk
    per = blk // FT

    def one_block(s, _):
        block = block_at(s, me, per, blocks)
        later = block_at(lax.rem(s + 1, blocks), me, per, blocks)
        attend_block(block, later, blk, qt, kn, vt, m_s, o_s, s_s)
        for net in range(2):
            o = o_s[net]
            y = (o[0:64] / o[64:65]).astype(bf16)
            for r in range(per):
                tsend[block * per + r, net * 64 : (net + 1) * 64, :] = y[:, r * FT : (r + 1) * FT]
        for r in range(per):
            f = block * per + r

            @pl.when(f != me)
            def _():
                tl.to(tsend.at[f], trecv.at[me], f).start()

        return 0

    attend_block(block_at(0, me, per, blocks), None, blk, qt, kn, vt, m_s, o_s, s_s)
    lax.fori_loop(0, blocks, one_block, 0)
    ph("t_wait")
    x_own = xs[:, pl.ds(pl.multiple_of(me * FT, FT), FT)]
    base_r = mm(rmat[0], x_own)
    base_f = mm(rmat[1], x_own)
    noisy = x_own[0:64].astype(f32)
    trecv[me] = tsend[me]
    tl.wait(trecv.at[pl.ds(0, n - 1)])

    ph("finish")

    def add_up(s, t):
        return t + trecv[s].astype(f32)

    vel = lax.fori_loop(0, n, add_up, jnp.zeros((128, FT), f32), unroll=True)
    vel_r = vel[0:64] + base_r[0:64] + base_r[64:128]
    vel_f = vel[64:128] + base_f[0:64] + base_f[64:128]
    pred_r = noisy - sigma * vel_r
    pred_f = noisy - sigma * vel_f
    gap = jnp.abs(gen_s[...].astype(f32) - pred_r)
    gsum = gap[0:8]
    for r in range(1, 8):
        gsum = gsum + gap[r * 8 : (r + 1) * 8]
    gapbuf[me] = jnp.sum(gsum, axis=0, keepdims=True)
    diff = pred_f - pred_r
    own = dcat.at[:, slot]
    own[...] = diff.astype(bf16)
    dl.to(own, own, other).start()
    gl.all(lambda j: gapbuf.at[me], gapbuf.at[me])
    dmd_ref[...] = diff
    ph("h_wait")
    hl.wait(hcol.at[pl.ds(0, FT), :])
    ph("d_wait")
    dl.wait(dcat.at[:, pl.ds(0, FT)])
    ph("wg_mm")
    wsend[...] = mm(dcat[...], hcol[...]).astype(bf16)
    rows = wrecv.shape[1]
    cols = wrecv.shape[2]

    def piece(j, c):
        return (
            pl.ds(pl.multiple_of(j // gy * rows, 16), rows),
            pl.ds(pl.multiple_of(c * half_d + lax.rem(j, gy) * cols, 128), cols),
        )

    w_rs.mates(lambda j: wsend.at[piece(j, 0)], wrecv.at[chip])
    wrecv[chip] = wsend[piece(chip, 0)]
    ph("gap_wait")
    gl.wait(gapbuf.at[pl.ds(0, n - 1)])
    gap_all = jnp.sum(jnp.sum(gapbuf[...], axis=0), keepdims=True)
    inv = 1.0 / jnp.maximum(gap_all / (64.0 * tokens), gap_floor)
    dmd_ref[...] = dmd_ref[...] * inv
    put_dmd = load(dmd_ref, dmd_h.at[0])
    ph("w_wait")
    w_rs.wait(wrecv.at[pl.ds(0, chips - 1)])
    wsum = wrecv[0].astype(f32)
    for j in range(1, chips):
        wsum = wsum + wrecv[j].astype(f32)
    zbuf[mz] = (wsum * (inv / math.sqrt(nz * tokens))).astype(bf16)
    ph("w_z")
    for i in range(1, nz):
        w_z.to(zbuf.at[mz], zbuf.at[mz], lax.rem(mz + i, nz), "batch").start()
    if nz > 1:
        zview = zbuf.at[pl.ds(0, nz - 1)]
        zwait = w_z.to(zview, zview, lax.rem(mz + 1, nz), "batch")
        zwait.wait_recv()
        zwait.wait_send()
    whole = zbuf[0].astype(f32)
    for z in range(1, nz):
        whole = whole + zbuf[z].astype(f32)
    ph("w_ag")
    part = wg_ref.at[piece(chip, core)]
    part[...] = whole.astype(bf16)
    w_ag.mates(lambda j: part, part)
    w_ag.wait(wrecv.at[pl.ds(0, chips - 1)])
    ph("w_forward")
    w_fw.to(wg_ref.at[:, half_of(core)], wg_h.at[:, half_of(core)], other).start()
    put_wg = load(wg_ref.at[:, half_of(core)], wg_h.at[:, half_of(core)])
    put_dmd.wait()
    put_wg.wait()
    w_fw.to(wg_ref.at[:, half_of(core)], wg_h.at[:, half_of(1 - core)], other).wait_recv()
    w_fw.to(wg_ref.at[:, half_of(core)], wg_h.at[:, half_of(core)], other).wait_send()
    ph(None)


def per_device(
    hidden_states, gen_weight, noise_field, timesteps,
    embed_real, time_real, query_real, key_real, value_real, out_real, gain_real, proj_real,
    embed_fake, time_fake, query_fake, key_fake, value_fake, out_fake, gain_fake, proj_fake,
):
    n = lax.axis_size("tm")
    nz = lax.axis_size("batch")
    d = hidden_states.shape[2]
    tokens = n * FT
    blk = 512
    chips = n // 2
    rows = 64 // (n // GS)
    cols = d // GS
    fr = time_real.shape[0]
    hbm = pl.BlockSpec(memory_space=pl.ANY)
    sems = pltpu.SemaphoreType.DMA
    scratch = [
        pltpu.VMEM((64, FT), bf16),
        pltpu.VMEM((2, 2, HD), f32),
        pltpu.VMEM((2, 3, fr, d), bf16),
        pltpu.VMEM((FT, d), bf16),
        pltpu.VMEM((64, d), bf16),
        pltpu.VMEM((2, 128, d), bf16),
        pltpu.VMEM((2, 64, d), bf16),
        pltpu.VMEM((2, 128, d), bf16),
        pltpu.VMEM((2, d, 256), bf16),
        pltpu.VMEM((2, d, 128), bf16),
        pltpu.VMEM((n, 8, 128), f32),
        pltpu.VMEM((chips, 16, 128), bf16),
        pltpu.VMEM((n, 16, 128), bf16),
        pltpu.VMEM((chips, 16, 128), bf16),
        pltpu.VMEM((n, 8, 128), f32),
        pltpu.VMEM((chips, 2, 64, 128), bf16),
        pltpu.VMEM((128, tokens), bf16),
        pltpu.VMEM((64, 128), bf16),
        pltpu.VMEM((2, 128, 128), f32),
        pltpu.VMEM((2, 256, 128), bf16),
        pltpu.VMEM((2, 128, 128), bf16),
        pltpu.VMEM((2, 144, d), bf16),
        pltpu.VMEM((2, 144, 256), f32),
        pltpu.VMEM((2, 128, 1024), bf16),
        pltpu.VMEM((2, 128, 128), f32),
        pltpu.VMEM((2, 144, 128), f32),
        pltpu.VMEM((2, 8, tokens), f32),
        pltpu.VMEM((2, 128, tokens), f32),
        pltpu.VMEM((2, 128, tokens), f32),
        pltpu.VMEM((chips, 8, 128), f32),
        pltpu.VMEM((n, 8, 128), f32),
        pltpu.VMEM((chips, 8, 128), f32),
        pltpu.VMEM((2, 128, tokens), bf16),
        pltpu.VMEM((2, tokens, 128), bf16),
        pltpu.VMEM((2, 80, tokens), bf16),
        pltpu.VMEM((2, 8, blk), f32),
        pltpu.VMEM((2, 80, blk), f32),
        pltpu.VMEM((2, 2, blk, blk), f32),
        pltpu.VMEM((64, FT), f32),
        pltpu.VMEM((64, d), bf16),
        pltpu.VMEM((n, 128, 128), bf16),
        pltpu.VMEM((n, 128, 128), bf16),
        pltpu.VMEM((n, 1, 128), f32),
        pltpu.VMEM((2 * FT, d // 2), bf16),
        pltpu.VMEM((64, 2 * FT), bf16),
        pltpu.VMEM((64, d // 2), bf16),
        pltpu.VMEM((chips, rows, cols), bf16),
        pltpu.VMEM((nz, rows, cols), bf16),
        sems((22,)),
        sems((28,)),
    ]
    dmd, wg = pl.pallas_call(
        functools.partial(kernel, n, nz, blk),
        out_shape=(
            jax.ShapeDtypeStruct((1, 64, FT), f32),
            jax.ShapeDtypeStruct((64, d), bf16),
        ),
        in_specs=[pl.BlockSpec(memory_space=pltpu.SMEM)] + [hbm] * 19,
        out_specs=(hbm, hbm),
        scratch_shapes=scratch,
        compiler_params=pltpu.CompilerParams(
            collective_id=0, has_side_effects=True, vmem_limit_bytes=62 * 1024 * 1024
        ),
        name="dmd",
    )(
        timesteps, noise_field, gain_real, gain_fake,
        time_real.transpose(1, 0, 2), time_fake.transpose(1, 0, 2),
        hidden_states, gen_weight, embed_real, embed_fake, proj_real, proj_fake,
        out_real, out_fake,
        query_real, key_real, value_real, query_fake, key_fake, value_fake,
    )
    return dmd, wg.astype(f32)


def solution(mesh):
    in_specs = (
        P("batch", "tm", None), P(), P("batch", None, "tm"), P("batch"),
        P(), P("tm", None, None), P(None, "tm"), P(None, "tm"), P(None, "tm"),
        P("tm", None), P(None, "tm"), P(),
        P(), P("tm", None, None), P(None, "tm"), P(None, "tm"), P(None, "tm"),
        P("tm", None), P(None, "tm"), P(),
    )
    out_specs = (P("batch", None, "tm"), P())
    return jax.shard_map(
        per_device, mesh=mesh, in_specs=in_specs, out_specs=out_specs, check_vma=False
    )
```

```python
import functools
import math

import jax
import jax.numpy as jnp
from jax import lax
from jax.experimental import pallas as pl
from jax.experimental.pallas import tpu as pltpu
from jax.sharding import PartitionSpec as P

HD = 128
FREQ = 256
FT = 128
GS = 8
MESH = pl.DeviceIdType.MESH

norm_floor = 0.05
gap_floor = 0.25
highest = lax.Precision.HIGHEST
f32 = jnp.float32
bf16 = jnp.bfloat16


def split2(a):
    hi = a.astype(bf16)
    lo = (a - hi.astype(f32)).astype(bf16)
    return hi, lo


def stack2(a):
    hi, lo = split2(a)
    return jnp.concatenate([hi, lo], axis=0)


def mm(a, b):
    return jnp.dot(a, b, preferred_element_type=f32)


def mm_t(a, b):
    return lax.dot_general(a, b, (((1,), (1,)), ((), ())), preferred_element_type=f32)


class Phase:
    def __init__(self):
        self.now = None

    def __call__(self, name):
        if self.now is not None:
            self.now.__exit__(None, None, None)
        self.now = None
        if name:
            self.now = jax.named_scope(name)
            self.now.__enter__()


def attend_block(block, later, blk, qt_ref, k_ref, v_ref, m_ref, o_ref, s_ref):
    frames = blk // FT

    def score(net, k_block, q_block):
        k_at = pl.multiple_of(k_block * blk, blk)
        q_at = pl.multiple_of(q_block * blk, blk)
        return mm(k_ref[net, pl.ds(k_at, blk), :], qt_ref[net, :, pl.ds(q_at, blk)])

    if later is None:
        for net in range(2):
            s_ref[0, net] = score(net, block, block)
        return

    def advance(kb, last, first, src, dst):
        next_k = jnp.where(last, later, 0 if first else kb + 1)
        next_q = jnp.where(last, later, block)
        k_at = pl.multiple_of(kb * blk, blk)
        for net in range(2):
            s = s_ref[src, net]
            if first:
                rows = []
                for r in range(frames):
                    part = s[r * FT : (r + 1) * FT]
                    if r:
                        gone = jnp.full((FT, r * FT), -1e30, f32)
                        part = jnp.concatenate([gone, part[:, r * FT :]], axis=1)
                    rows.append(part)
                s = jnp.concatenate(rows, axis=0)
            top = jnp.max(s, axis=0, keepdims=True)
            if not first:
                old = m_ref[net, 0:1, :]
                top = jnp.maximum(old, top)
            p = jnp.exp2(s - top).astype(bf16)
            s_ref[dst, net] = score(net, next_k, next_q)
            o = mm(v_ref[net, :, pl.ds(k_at, blk)], p)
            if not first:
                o = o_ref[net] * jnp.exp2(old - top) + o
            o_ref[net] = o
            m_ref[net] = jnp.broadcast_to(top, (8, blk))

    odd = lax.rem(block, 2)

    @pl.when(odd == 0)
    def _():
        advance(block, block == 0, True, 0, 0)

    @pl.when(odd == 1)
    def _():
        advance(block, False, True, 0, 1)
        advance(0, block == 1, False, 1, 0)

    def pair(i, _):
        for u in range(2):
            kb = odd + i * 2 + u
            advance(kb, kb == block - 1, False, u, 1 - u)
        return 0

    lax.fori_loop(0, block // 2, pair, 0)


def block_at(s, me, per, blocks):
    home = me // per
    if blocks != 8:
        return lax.rem(home + 1 + s, blocks)
    dx = jnp.where(s < 2, 2, jnp.where((s == 2) | (s == 7), 0, 1 + 2 * lax.rem(s - 1, 2)))
    dy = jnp.where((s == 0) | ((s > 1) & (s < 5)), 1, 0)
    x = lax.rem(home // 2 + dx, 4)
    y = lax.rem(home + dy, 2)
    return x * 2 + y


def kernel(
    n, nz, blk,
    step_ref,
    noise_h, gain_rh, gain_fh, time_rh, time_fh, hidden_h, genw_h, emb_rh, emb_fh, proj_rh, proj_fh, out_rh, out_fh,
    wq_r, wk_r, wv_r, wq_f, wk_f, wv_f,
    dmd_h, wg_h,
    noise, gain, times, hid, genw, emb, proj, outw, wqk, wv,
    modbuf, modout, modin, modall, modfull, xg, xs, gen_s, mu_s, gmat, rmat,
    lhs, acc, lhs2, acc2, accv, rs_s, qraw, kraw, nbuf, nin, nfull,
    qt, kn, vt, m_s, o_s, s_s,
    dmd_ref, wg_ref, tsend, trecv, gapbuf, hcol, dcat, wsend, wrecv, zbuf,
    lsem, sem,
):
    me = lax.axis_index("tm")
    mz = lax.axis_index("batch")
    core = lax.rem(me, 2)
    chip = me // 2
    other = me + 1 - 2 * core
    chips = n // 2
    d = hid.shape[1]
    groups = d // 1024
    tokens = n * FT
    ph = Phase()
    loads = []

    def load(src, dst):
        c = pltpu.make_async_copy(src, dst, lsem.at[len(loads)])
        c.start()
        loads.append(c)
        return c

    ld_time = [load(time_rh, times.at[0]), load(time_fh, times.at[1])]
    ld_noise = load(noise_h.at[0], noise)
    ld_hid = load(hidden_h.at[0], hid)
    ld_gen = load(genw_h, genw)
    ld_emb = [load(emb_rh, emb.at[0]), load(emb_fh, emb.at[1])]
    ld_proj = [load(proj_rh, proj.at[0]), load(proj_fh, proj.at[1])]
    ld_qk = []
    for net, (a, b) in enumerate(((wq_r, wk_r), (wq_f, wk_f))):
        ld_qk.append(load(a, wqk.at[net, :, 0:HD]))
        ld_qk.append(load(b, wqk.at[net, :, HD : 2 * HD]))
    ld_v = [load(wv_r, wv.at[0]), load(wv_f, wv.at[1])]
    ld_out = [load(out_rh, outw.at[0]), load(out_fh, outw.at[1])]

    ld_gain = [load(gain_rh, gain.at[0]), load(gain_fh, gain.at[1])]

    barrier = pltpu.get_barrier_semaphore()

    def greet(i, _):
        pl.semaphore_signal(
            barrier, inc=1, device_id={"tm": lax.rem(me + i, n)}, device_id_type=MESH
        )
        return 0

    lax.fori_loop(1, n, greet, 0)
    for i in range(1, nz):
        pl.semaphore_signal(
            barrier, inc=1, device_id={"batch": lax.rem(mz + i, nz)}, device_id_type=MESH
        )

    used = [0]
    wide = chips // 4
    shifts = [(dx, dy) for dx in range(wide) for dy in range(4) if dx or dy]
    shifts.sort(key=lambda t: -min(t[0], wide - t[0]) - min(t[1], 4 - t[1]))
    far_first = [
        lax.rem(chip // 4 + dx, wide) * 4 + lax.rem(lax.rem(chip, 4) + dy, 4) for dx, dy in shifts
    ]

    class Lane:
        def __init__(self):
            self.send = sem.at[used[0]]
            self.recv = sem.at[used[0] + 1]
            used[0] += 2

        def to(self, src, dst, j, axis="tm"):
            return pltpu.make_async_remote_copy(
                src_ref=src, dst_ref=dst, send_sem=self.send, recv_sem=self.recv,
                device_id={axis: j}, device_id_type=MESH,
            )

        def all(self, src_of, dst):
            def body(i, _):
                j = lax.rem(me + i, n)
                self.to(src_of(j), dst, j).start()
                return 0

            lax.fori_loop(1, n, body, 0)

        def mates(self, src_of, dst):
            for j in far_first:
                self.to(src_of(j), dst, 2 * j + core).start()

        def wait(self, view):
            c = self.to(view, view, other)
            c.wait_recv()
            c.wait_send()

        def owners(self, src_of, dst, count):
            for j in far_first + [chip]:

                @pl.when(jnp.logical_and(j < count, 2 * j + 1 != me))
                def _():
                    self.to(src_of(j), dst, 2 * j + 1).start()

        def to_owner(self, whole, count, then):
            owner = jnp.logical_and(core == 1, chip < count)

            @pl.when(owner)
            def _():
                self.to(whole, whole, other).wait_recv()
                then()

                for j in far_first:
                    for c in range(2):
                        self.back.to(self.result, self.result, 2 * j + c).start()
                self.back.to(self.result, self.result, other).start()

            return owner

        def settle(self, owner, sent, fewer):
            @pl.when(owner)
            def _():
                self.to(fewer, fewer, other).wait_send()

            @pl.when(jnp.logical_not(owner))
            def _():
                self.to(sent, sent, other).wait_send()

        def gather(self, owner, whole, all_in, fewer):
            @pl.when(owner)
            def _():
                self.to(whole, whole, other).wait_send()
                self.to(fewer, fewer, other).wait_recv()

            @pl.when(jnp.logical_not(owner))
            def _():
                self.to(all_in, all_in, other).wait_recv()

    pieces = (6 * groups + 1) // 2
    mod_rs, mod_ag, xl, xf = Lane(), Lane(), Lane(), Lane()
    nrm_rs, nrm_ag, tl, gl = Lane(), Lane(), Lane(), Lane()
    hl, dl = Lane(), Lane()
    w_rs, w_z, w_ag, w_fw = [[Lane(), Lane()] for _ in range(4)]
    gy = GS // 2
    half_d = d // 2
    slot = pl.ds(pl.multiple_of(core * FT, FT), FT)

    def half_of(c):
        return pl.ds(pl.multiple_of(c * half_d, 128), half_d)


    ph("share")
    step = jnp.full((1, 128), step_ref[0], jnp.int32).astype(f32)
    raw = step / 1000.0
    sigma = 5.0 * raw / (1.0 + 4.0 * raw)
    freqs = times.shape[2]
    first = me * freqs + lax.broadcasted_iota(jnp.int32, (freqs, 128), 0)
    k = lax.rem(first, FREQ // 2).astype(f32)
    angle = step * jnp.exp(k * (-math.log(10000.0) / (FREQ // 2)))
    turns = jnp.floor(angle * (0.5 / math.pi) + 0.5)
    angle = (angle - turns * 6.28125) - turns * (2.0 * math.pi - 6.28125)
    wave = jnp.where(first < FREQ // 2, jnp.cos(angle), jnp.sin(angle)).astype(bf16).astype(f32)
    for p in range(6 * groups, 2 * pieces):
        modbuf[p] = jnp.zeros((8, 128), f32)
    for net in range(2):
        ld_time[net].wait()
        for c in range(3):
            for b in range(8 * groups):
                t = times[net, c, :, b * 128 : (b + 1) * 128].astype(f32)
                part = jnp.sum(t * wave, axis=0, keepdims=True)
                modbuf[(net * 3 + c) * groups + b // 8, b % 8 : b % 8 + 1, :] = part
    for j in range(pieces):
        pair = jnp.concatenate([modbuf[2 * j], modbuf[2 * j + 1]], axis=0)
        modout[j] = pair.astype(bf16)
    ph("generate")
    ld_hid.wait()
    ld_gen.wait()
    generated = mm_t(genw[...], hid[...]).astype(bf16)
    gen_s[...] = generated
    ld_noise.wait()
    mixed = (1.0 - sigma) * generated.astype(f32) + sigma * noise[...].astype(f32)
    xg[chip, core] = mixed.astype(bf16)
    ph("barrier")
    pl.semaphore_wait(barrier, n - 1 + nz - 1)
    mod_rs.owners(lambda j: modout.at[j], modin.at[me], pieces)

    mine = xg.at[chip, core]
    xl.mates(lambda j: mine, mine)

    ph("weights")
    ones_k = jnp.ones((1024, 128), bf16)

    def weight_terms(net):
        ld_emb[net].wait()
        ld_proj[net].wait()

        def gram(g, t):
            at = pl.multiple_of(g * 1024, 1024)
            e = emb[net, :, pl.ds(at, 1024)]
            return (
                t[0] + mm_t(e, e),
                t[1] + mm(e, ones_k),
                t[2] + mm_t(proj[net, :, pl.ds(at, 1024)], e),
            )

        zero = jnp.zeros((128, 128), f32)
        ee, mu, rr = lax.fori_loop(
            0, groups, gram, (zero, zero, jnp.zeros((64, 128), f32)), unroll=True
        )
        mu = mu / d
        mu_s[net] = mu
        gmat[net] = stack2(ee / d - mu * mu.T)
        rmat[net] = stack2(rr)

    weight_terms(0)
    ph("mod_rs")

    def add_mod():
        modin[me] = modout[chip]
        total = modin[0].astype(f32)
        for j in range(1, n):
            total = total + modin[j].astype(f32)
        modall[chip] = total.astype(bf16)

    mod_rs.back, mod_rs.result = mod_ag, modall.at[chip]
    mod_owner = mod_rs.to_owner(modin.at[pl.ds(0, n - 1)], pieces, add_mod)
    mod_rs.settle(mod_owner, modout.at[pl.ds(0, pieces)], modout.at[pl.ds(0, pieces - 1)])

    ph("weights1")
    weight_terms(1)
    hcol[slot, :] = hid[:, half_of(core)]

    ph("x_wait")
    xl.wait(xg.at[pl.ds(0, chips - 1), core])
    xf.to(xg.at[:, core], xg.at[:, core], other).start()
    xs[64:128, 0:FT] = jnp.zeros((64, FT), bf16)

    def place(parity, i):
        at = pl.multiple_of(i * (2 * FT) + parity * FT, FT)
        x = xg[i, parity]
        xs[0:64, pl.ds(at, FT)] = x
        return at, x

    def place_both(parity):
        def body(i, _):
            at, x = place(parity, i)
            xs[64:128, pl.ds(pl.multiple_of(at + FT, FT), FT)] = x
            return 0

        return body

    lax.fori_loop(0, chips - 1, place_both(core), 0, unroll=5)
    ph("x_fwait")
    xf.wait(xg.at[:, core])
    hl.to(hid.at[:, half_of(1 - core)], hcol.at[slot, :], other).start()

    ph("place_var")

    lax.fori_loop(0, chips - 1, place_both(1 - core), 0, unroll=5)
    at, x = place(0, chips - 1)
    xs[64:128, pl.ds(pl.multiple_of(at + FT, FT), FT)] = x
    place(1, chips - 1)

    width = blk

    def variances(t, _):
        at = pl.multiple_of(t * width, width)
        x = xs[:, pl.ds(at, width)]
        for net in range(2):
            y = mm(gmat[net], x)
            var = jnp.sum((y[0:128] + y[128:256]) * x.astype(f32), axis=0, keepdims=True)
            rs = lax.rsqrt(jnp.maximum(var, 0.0) + norm_floor)
            rs_s[net, :, pl.ds(at, width)] = jnp.broadcast_to(rs, (8, width))
        return 0

    lax.fori_loop(0, tokens // width, variances, 0, unroll=True)
    for c in ld_qk:
        c.wait()
    ph("mod_ag_wait")
    mod_ag.gather(
        mod_owner, modin.at[pl.ds(0, n - 1)], modall.at[pl.ds(0, pieces)],
        modall.at[pl.ds(0, pieces - 1)],
    )
    for j in range(pieces):
        both = modall[j].astype(f32)
        modfull[2 * j] = both[0:8]
        modfull[2 * j + 1] = both[8:16]

    ph("qk_fold")
    row = lax.broadcasted_iota(jnp.int32, (16, 128), 0)
    acc[...] = jnp.zeros_like(acc)

    def fold(g, _):
        at = pl.multiple_of(g * 1024, 1024)
        for net in range(2):
            shift8 = modfull[(net * 3 + 0) * groups + g]
            scale8 = modfull[(net * 3 + 1) * groups + g]
            for r in range(8):
                col = pl.multiple_of(at + r * 128, 128)
                e = emb[net, :, pl.ds(col, 128)].astype(f32) - mu_s[net]
                lhs[net, 0:128, pl.ds(col, 128)] = (e * (1.0 + scale8[r : r + 1, :])).astype(bf16)
                sh, sl = split2(shift8[r : r + 1, :])
                tail = jnp.where(
                    row == 0, sh.astype(f32), jnp.where(row == 1, sl.astype(f32), 0.0)
                )
                lhs[net, 128:144, pl.ds(col, 128)] = tail.astype(bf16)
            acc[net] += mm(lhs[net, :, pl.ds(at, 1024)], wqk[net, pl.ds(at, 1024), :])
        return 0

    lax.fori_loop(0, groups, fold, 0, unroll=True)
    ph("qk_project")
    mats = []
    for net in range(2):
        off = acc[net, 128:129, :] + acc[net, 129:130, :]
        for which in range(2):
            cols = slice(which * HD, (which + 1) * HD)
            mat = acc[net, 0:128, cols].T.astype(bf16)
            mats.append((mat, jnp.broadcast_to(off[:, cols], (128, 128)).T[:, 0:1]))

    def project(t, _):
        at = pl.multiple_of(t * width, width)
        x = xs[:, pl.ds(at, width)]
        for net in range(2):
            rs = rs_s[net, 0:1, pl.ds(at, width)]
            for which, dst in enumerate((qraw, kraw)):
                mat, off_c = mats[net * 2 + which]
                y = mm(mat, x) * rs + off_c
                dst[net, :, pl.ds(at, width)] = y
                sq = jnp.sum(y * y, axis=0, keepdims=True)
                for r in range(width // FT):
                    row = (r % 2) * 4 + net * 2 + which
                    nbuf[t * (width // FT // 2) + r // 2, row : row + 1, :] = sq[
                        :, r * FT : (r + 1) * FT
                    ]
        return 0

    lax.fori_loop(0, tokens // width, project, 0, unroll=True)

    ph("norm_send")
    nrm_rs.owners(lambda j: nbuf.at[j], nin.at[me], chips)

    ph("v_fold")
    for c in ld_v + ld_out:
        c.wait()
    accv[...] = jnp.zeros_like(accv)
    acc2[...] = jnp.zeros_like(acc2)

    def fold_v(g, _):
        at = pl.multiple_of(g * 1024, 1024)
        for net in range(2):
            gate8 = modfull[(net * 3 + 2) * groups + g]
            for r in range(8):
                col = pl.multiple_of(at + r * 128, 128)
                gated = proj[net, :, pl.ds(col, 128)].astype(f32) * gate8[r : r + 1, :]
                hi, lo = split2(gated)
                lhs2[net, 0:64, r * 128 : (r + 1) * 128] = hi
                lhs2[net, 64:128, r * 128 : (r + 1) * 128] = lo
            accv[net] += mm(lhs[net, :, pl.ds(at, 1024)], wv[net, pl.ds(at, 1024), :])
            acc2[net] += mm_t(lhs2[net], outw[net, :, pl.ds(at, 1024)])
        return 0

    lax.fori_loop(0, groups, fold_v, 0, unroll=True)

    ph("norm_rs_wait")

    def add_norm():
        nin[me] = nbuf[chip]
        nfull[chip] = lax.rsqrt(jnp.sum(nin[...], axis=0) / float(n * HD) + norm_floor)

    nrm_rs.back, nrm_rs.result = nrm_ag, nfull.at[chip]
    nrm_owner = nrm_rs.to_owner(nin.at[pl.ds(0, n - 1)], chips, add_norm)
    nrm_rs.settle(nrm_owner, nbuf.at[pl.ds(0, chips)], nbuf.at[pl.ds(0, chips - 1)])

    ph("values")
    vmats = []
    for net in range(2):
        a = accv[net, 0:128, :]
        off = accv[net, 128:129, :] + accv[net, 129:130, :]
        out_t = acc2[net, 0:64, :] + acc2[net, 64:128, :]
        b_mat = stack2(
            lax.dot_general(
                out_t, a, (((1,), (1,)), ((), ())), precision=highest, preferred_element_type=f32
            )
        )
        vmats.append((b_mat, jnp.sum(out_t * off, axis=1, keepdims=True)))
    ones = jnp.where(lax.broadcasted_iota(jnp.int32, (16, width), 0) == 0, 1.0, 0.0)

    def values(t, _):
        at = pl.multiple_of(t * width, width)
        x = xs[:, pl.ds(at, width)]
        for net in range(2):
            y = mm(vmats[net][0], x)
            y = (y[0:64] + y[64:128]) * rs_s[net, 0:1, pl.ds(at, width)] + vmats[net][1]
            vt[net, 0:64, pl.ds(at, width)] = y.astype(bf16)
            vt[net, 64:80, pl.ds(at, width)] = ones.astype(bf16)
        return 0

    lax.fori_loop(0, tokens // width, values, 0, unroll=4)
    gains = []
    for net in range(2):
        ld_gain[net].wait()
        both = gain[net, 0:1, :] * gain[net, 1:2, :] * (math.log2(math.e) / math.sqrt(HD))
        gains.append(jnp.broadcast_to(both, (128, 128)).T)

    def gained(t, _):
        at = pl.multiple_of(t * FT, FT)
        for net in range(2):
            qraw[net, :, pl.ds(at, FT)] = qraw[net, :, pl.ds(at, FT)] * gains[net]
        return 0

    lax.fori_loop(0, n, gained, 0, unroll=4)
    same = lax.broadcasted_iota(jnp.int32, (256, 256), 0) == lax.broadcasted_iota(
        jnp.int32, (256, 256), 1
    )
    eye = jnp.where(same, 1.0, 0.0).astype(bf16)
    ph("norm_ag_wait")
    nrm_ag.gather(
        nrm_owner, nin.at[pl.ds(0, n - 1)], nfull.at[pl.ds(0, chips)],
        nfull.at[pl.ds(0, chips - 1)],
    )

    ph("normalise")

    def normalise(t, _):
        at = pl.multiple_of(t * 256, 256)
        k_rows = []
        for net in range(2):
            k_cols = []
            for half in range(2):
                scales = nfull[t]
                to = pl.ds(pl.multiple_of(at + half * FT, FT), FT)
                at_row = half * 4 + net * 2
                sq = scales[at_row : at_row + 1, :]
                sk = scales[at_row + 1 : at_row + 2, :]
                qt[net, :, to] = (qraw[net, :, to] * sq).astype(bf16)
                k_cols.append((kraw[net, :, to] * sk).astype(bf16))
            k_rows.append(jnp.concatenate(k_cols, axis=1))
        turned = mm_t(eye, jnp.concatenate(k_rows, axis=0)).astype(bf16)
        for net in range(2):
            kn[net, pl.ds(at, 256), :] = turned[:, net * HD : (net + 1) * HD]
        return 0

    lax.fori_loop(0, tokens // 256, normalise, 0, unroll=True)

    ph("attend")
    blocks = tokens // blk
    per = blk // FT

    def one_block(s, _):
        block = block_at(s, me, per, blocks)
        later = block_at(lax.rem(s + 1, blocks), me, per, blocks)
        attend_block(block, later, blk, qt, kn, vt, m_s, o_s, s_s)
        for net in range(2):
            o = o_s[net]
            y = (o[0:64] / o[64:65]).astype(bf16)
            for r in range(per):
                tsend[block * per + r, net * 64 : (net + 1) * 64, :] = y[:, r * FT : (r + 1) * FT]
        for r in range(per):
            f = block * per + r

            @pl.when(f != me)
            def _():
                tl.to(tsend.at[f], trecv.at[me], f).start()

        return 0

    attend_block(block_at(0, me, per, blocks), None, blk, qt, kn, vt, m_s, o_s, s_s)
    lax.fori_loop(0, blocks, one_block, 0)
    ph("t_wait")
    x_own = xs[:, pl.ds(pl.multiple_of(me * FT, FT), FT)]
    base_r = mm(rmat[0], x_own)
    base_f = mm(rmat[1], x_own)
    noisy = x_own[0:64].astype(f32)
    trecv[me] = tsend[me]
    tl.wait(trecv.at[pl.ds(0, n - 1)])

    ph("finish")

    def add_up(s, t):
        return t + trecv[s].astype(f32)

    vel = lax.fori_loop(0, n, add_up, jnp.zeros((128, FT), f32), unroll=True)
    vel_r = vel[0:64] + base_r[0:64] + base_r[64:128]
    vel_f = vel[64:128] + base_f[0:64] + base_f[64:128]
    pred_r = noisy - sigma * vel_r
    pred_f = noisy - sigma * vel_f
    gap = jnp.abs(gen_s[...].astype(f32) - pred_r)
    gsum = gap[0:8]
    for r in range(1, 8):
        gsum = gsum + gap[r * 8 : (r + 1) * 8]
    gapbuf[me] = jnp.sum(gsum, axis=0, keepdims=True)
    diff = pred_f - pred_r
    own = dcat.at[:, slot]
    own[...] = diff.astype(bf16)
    dl.to(own, own, other).start()
    gl.all(lambda j: gapbuf.at[me], gapbuf.at[me])
    dmd_ref[...] = diff
    ph("h_wait")
    hl.wait(hcol.at[pl.ds(0, FT), :])
    ph("d_wait")
    dl.wait(dcat.at[:, pl.ds(0, FT)])
    ph("wg_mm")
    wsend[...] = mm(dcat[...], hcol[...]).astype(bf16)
    rows = wrecv.shape[1]
    cols = wrecv.shape[2]

    first_cols = (cols // 128 + 1) // 2 * 128
    parts = [(0, first_cols), (first_cols, cols - first_cols)]
    parts = [p for p in parts if p[1]]

    def piece(j, c, k):
        at, size = parts[k]
        return (
            pl.ds(pl.multiple_of(j // gy * rows, 16), rows),
            pl.ds(pl.multiple_of(c * half_d + lax.rem(j, gy) * cols + at, 128), size),
        )

    def inner(k):
        return pl.ds(*parts[k])

    some = pl.ds(0, chips - 1)
    for k in range(len(parts)):
        w_rs[k].mates(lambda j: wsend.at[piece(j, 0, k)], wrecv.at[chip, :, inner(k)])
        wrecv[chip, :, inner(k)] = wsend[piece(chip, 0, k)]
    ph("gap_wait")
    gl.wait(gapbuf.at[pl.ds(0, n - 1)])
    gap_all = jnp.sum(jnp.sum(gapbuf[...], axis=0), keepdims=True)
    inv = 1.0 / jnp.maximum(gap_all / (64.0 * tokens), gap_floor)
    dmd_ref[...] = dmd_ref[...] * inv
    put_dmd = load(dmd_ref, dmd_h.at[0])
    ph("w_wait")
    scale = inv / math.sqrt(nz * tokens)
    for k in range(len(parts)):
        w_rs[k].wait(wrecv.at[some, :, inner(k)])
        wsum = wrecv[0, :, inner(k)].astype(f32)
        for j in range(1, chips):
            wsum = wsum + wrecv[j, :, inner(k)].astype(f32)
        zbuf[mz, :, inner(k)] = (wsum * scale).astype(bf16)
        mine_z = zbuf.at[mz, :, inner(k)]
        for i in range(1, nz):
            w_z[k].to(mine_z, mine_z, lax.rem(mz + i, nz), "batch").start()
    ph("w_z")
    for k in range(len(parts)):
        if nz > 1:
            zview = zbuf.at[pl.ds(0, nz - 1), :, inner(k)]
            zwait = w_z[k].to(zview, zview, lax.rem(mz + 1, nz), "batch")
            zwait.wait_recv()
            zwait.wait_send()
        whole = zbuf[0, :, inner(k)].astype(f32)
        for z in range(1, nz):
            whole = whole + zbuf[z, :, inner(k)].astype(f32)
        part = wg_ref.at[piece(chip, core, k)]
        part[...] = whole.astype(bf16)
        w_ag[k].mates(lambda j: part, part)
    ph("w_ag")
    for k in range(len(parts)):
        at, size = parts[k]
        w_ag[k].wait(wrecv.at[some, :, inner(k)])
        for y in range(gy):
            col = pl.ds(pl.multiple_of(core * half_d + y * cols + at, 128), size)
            w_fw[k].to(wg_ref.at[:, col], wg_h.at[:, col], other).start()
    ph("w_forward")
    put_wg = load(wg_ref.at[:, half_of(core)], wg_h.at[:, half_of(core)])
    put_dmd.wait()
    put_wg.wait()
    for k in range(len(parts)):
        view = pl.ds(0, gy * parts[k][1])
        fwait = w_fw[k].to(wg_ref.at[:, view], wg_h.at[:, view], other)
        fwait.wait_recv()
        fwait.wait_send()
    ph(None)


def widen(a_h, b_h, a_out, b_out, a_v, b_v, c_v, sem):
    step = 1024
    parts = b_v.shape[1] // step
    ins = []
    outs = []
    for k in range(parts):
        cols = pl.ds(k * step, step)
        ins.append(pltpu.make_async_copy(b_h.at[:, cols], b_v.at[:, cols], sem.at[k]))
        outs.append(pltpu.make_async_copy(c_v.at[:, cols], b_out.at[:, cols], sem.at[parts + k]))
        ins[k].start()
    a_in = pltpu.make_async_copy(a_h, a_v, sem.at[2 * parts])
    a_go = pltpu.make_async_copy(a_v, a_out, sem.at[2 * parts + 1])
    a_in.start()
    for k in range(parts):
        cols = pl.ds(k * step, step)
        ins[k].wait()
        c_v[:, cols] = b_v[:, cols].astype(f32)
        outs[k].start()
    a_in.wait()
    a_go.start()
    for c in outs + [a_go]:
        c.wait()


def per_device(
    hidden_states, gen_weight, noise_field, timesteps,
    embed_real, time_real, query_real, key_real, value_real, out_real, gain_real, proj_real,
    embed_fake, time_fake, query_fake, key_fake, value_fake, out_fake, gain_fake, proj_fake,
):
    n = lax.axis_size("tm")
    nz = lax.axis_size("batch")
    d = hidden_states.shape[2]
    tokens = n * FT
    blk = 512
    chips = n // 2
    rows = 64 // (n // GS)
    cols = d // GS
    fr = time_real.shape[0]
    hbm = pl.BlockSpec(memory_space=pl.ANY)
    sems = pltpu.SemaphoreType.DMA
    scratch = [
        pltpu.VMEM((64, FT), bf16),
        pltpu.VMEM((2, 2, HD), f32),
        pltpu.VMEM((2, 3, fr, d), bf16),
        pltpu.VMEM((FT, d), bf16),
        pltpu.VMEM((64, d), bf16),
        pltpu.VMEM((2, 128, d), bf16),
        pltpu.VMEM((2, 64, d), bf16),
        pltpu.VMEM((2, 128, d), bf16),
        pltpu.VMEM((2, d, 256), bf16),
        pltpu.VMEM((2, d, 128), bf16),
        pltpu.VMEM((n, 8, 128), f32),
        pltpu.VMEM((chips, 16, 128), bf16),
        pltpu.VMEM((n, 16, 128), bf16),
        pltpu.VMEM((chips, 16, 128), bf16),
        pltpu.VMEM((n, 8, 128), f32),
        pltpu.VMEM((chips, 2, 64, 128), bf16),
        pltpu.VMEM((128, tokens), bf16),
        pltpu.VMEM((64, 128), bf16),
        pltpu.VMEM((2, 128, 128), f32),
        pltpu.VMEM((2, 256, 128), bf16),
        pltpu.VMEM((2, 128, 128), bf16),
        pltpu.VMEM((2, 144, d), bf16),
        pltpu.VMEM((2, 144, 256), f32),
        pltpu.VMEM((2, 128, 1024), bf16),
        pltpu.VMEM((2, 128, 128), f32),
        pltpu.VMEM((2, 144, 128), f32),
        pltpu.VMEM((2, 8, tokens), f32),
        pltpu.VMEM((2, 128, tokens), f32),
        pltpu.VMEM((2, 128, tokens), f32),
        pltpu.VMEM((chips, 8, 128), f32),
        pltpu.VMEM((n, 8, 128), f32),
        pltpu.VMEM((chips, 8, 128), f32),
        pltpu.VMEM((2, 128, tokens), bf16),
        pltpu.VMEM((2, tokens, 128), bf16),
        pltpu.VMEM((2, 80, tokens), bf16),
        pltpu.VMEM((2, 8, blk), f32),
        pltpu.VMEM((2, 80, blk), f32),
        pltpu.VMEM((2, 2, blk, blk), f32),
        pltpu.VMEM((64, FT), f32),
        pltpu.VMEM((64, d), bf16),
        pltpu.VMEM((n, 128, 128), bf16),
        pltpu.VMEM((n, 128, 128), bf16),
        pltpu.VMEM((n, 1, 128), f32),
        pltpu.VMEM((2 * FT, d // 2), bf16),
        pltpu.VMEM((64, 2 * FT), bf16),
        pltpu.VMEM((64, d // 2), bf16),
        pltpu.VMEM((chips, rows, cols), bf16),
        pltpu.VMEM((nz, rows, cols), bf16),
        sems((22,)),
        sems((36,)),
    ]
    dmd, wg = pl.pallas_call(
        functools.partial(kernel, n, nz, blk),
        out_shape=(
            jax.ShapeDtypeStruct((1, 64, FT), f32),
            jax.ShapeDtypeStruct((64, d), bf16),
        ),
        in_specs=[pl.BlockSpec(memory_space=pltpu.SMEM)] + [hbm] * 19,
        out_specs=(hbm, hbm),
        scratch_shapes=scratch,
        compiler_params=pltpu.CompilerParams(
            collective_id=0, has_side_effects=True, vmem_limit_bytes=62 * 1024 * 1024
        ),
        name="dmd",
    )(
        timesteps, noise_field, gain_real, gain_fake,
        time_real.transpose(1, 0, 2), time_fake.transpose(1, 0, 2),
        hidden_states, gen_weight, embed_real, embed_fake, proj_real, proj_fake,
        out_real, out_fake,
        query_real, key_real, value_real, query_fake, key_fake, value_fake,
    )
    return pl.pallas_call(
        widen,
        out_shape=(
            jax.ShapeDtypeStruct((1, 64, FT), f32),
            jax.ShapeDtypeStruct((64, d), f32),
        ),
        in_specs=[hbm, hbm],
        out_specs=(hbm, hbm),
        scratch_shapes=[
            pltpu.VMEM((1, 64, FT), f32),
            pltpu.VMEM((64, d), bf16),
            pltpu.VMEM((64, d), f32),
            sems((2 * (d // 1024) + 2,)),
        ],
        compiler_params=pltpu.CompilerParams(vmem_limit_bytes=62 * 1024 * 1024),
        name="widen",
    )(dmd, wg)


def solution(mesh):
    in_specs = (
        P("batch", "tm", None), P(), P("batch", None, "tm"), P("batch"),
        P(), P("tm", None, None), P(None, "tm"), P(None, "tm"), P(None, "tm"),
        P("tm", None), P(None, "tm"), P(),
        P(), P("tm", None, None), P(None, "tm"), P(None, "tm"), P(None, "tm"),
        P("tm", None), P(None, "tm"), P(),
    )
    out_specs = (P("batch", None, "tm"), P())
    return jax.shard_map(
        per_device, mesh=mesh, in_specs=in_specs, out_specs=out_specs, check_vma=False
    )
```
